32 devices in a mesh: dp: 4 (over y, z), tp: 8 (over x, core).
Axes of the slice: x: 4, y: 2, z: 2, core: 2. Of those that a mesh axis runs over, the one named last changes fastest.
The devices are a block of a 4x4x8 slice.
Arguments:
- hidden: bfloat16 [4, 256, 5120], P('dp', 'tp'), parts along dimension 0
- ln1_gain: float32 [5120], replicated
- ln1_bias: float32 [5120], replicated
- w_qkv: bfloat16 [5120, 3, 40, 128], P(None, None, 'tp')
- b_qkv: bfloat16 [3, 40, 128], P(None, 'tp')
- w_out: bfloat16 [40, 128, 5120], P('tp')
- b_out: bfloat16 [5120], replicated
- ln2_gain: float32 [5120], replicated
- ln2_bias: float32 [5120], replicated
- w_up: bfloat16 [5120, 20480], P(None, 'tp')
- b_up: bfloat16 [20480], P('tp')
- w_down: bfloat16 [20480, 5120], P('tp')
- b_down: bfloat16 [5120], replicated
Outputs:
- output: bfloat16 [4, 256, 5120], P('dp', 'tp'), parts along dimension 0
There are 4 independent parts. The reference program is written for one: setup_inputs(seed, part) draws one part's arguments, and reference() takes and returns one part's arrays. A program takes and returns all parts, laid end to end along the dimension named above; an argument that names none is the same for every part.
All inputs are finite; a program needn't handle non-finite values.
Results may differ from the reference program's by a relative error of at most 0.010208.
Values are sent between devices in bfloat16 or wider.
A program may use at most 768 MiB of HBM per device.

```python
import math
import jax
import jax.numpy as jnp
from jax import lax

N_BATCH = 1
SEQ_LEN = 256
D_MODEL = 5120
N_HEADS = 40

HEAD_DIM = D_MODEL // N_HEADS
FF_DIM = 4 * D_MODEL
LN_EPS = 1e-5


def layer_norm(inputs, gain_vec, shift_vec):
    as_f32 = inputs.astype(jnp.float32)
    row_mean = jnp.mean(as_f32, axis=-1, keepdims=True)
    centered = as_f32 - row_mean
    variance = jnp.mean(centered * centered, axis=-1, keepdims=True)
    return (centered * lax.rsqrt(variance + LN_EPS) * gain_vec + shift_vec).astype(jnp.bfloat16)


def setup_inputs(seed: int = 0, part: int = 0) -> dict:
    root_key = jax.random.key(seed)
    sub_keys = jax.random.split(root_key, 13)
    qk_gain = (0.5 * math.log(SEQ_LEN)) ** 0.25
    col_gain = jnp.array([qk_gain, qk_gain, 1.0], jnp.float32).reshape(1, 3, 1, 1)
    hidden = jax.random.normal(jax.random.fold_in(sub_keys[0], part), (N_BATCH, SEQ_LEN, D_MODEL), jnp.float32)
    w_qkv = jax.random.normal(sub_keys[3], (D_MODEL, 3, N_HEADS, HEAD_DIM), jnp.float32) * col_gain * D_MODEL ** -0.5
    return {
        "hidden": hidden.astype(jnp.bfloat16),
        "ln1_gain": 1.0 + 0.3 * jax.random.normal(sub_keys[1], (D_MODEL,), jnp.float32),
        "ln1_bias": 0.3 * jax.random.normal(sub_keys[2], (D_MODEL,), jnp.float32),
        "w_qkv": w_qkv.astype(jnp.bfloat16),
        "b_qkv": (0.5 * jax.random.normal(sub_keys[4], (3, N_HEADS, HEAD_DIM), jnp.float32)).astype(jnp.bfloat16),
        "w_out": (jax.random.normal(sub_keys[5], (N_HEADS, HEAD_DIM, D_MODEL), jnp.float32) * D_MODEL ** -0.5).astype(jnp.bfloat16),
        "b_out": (0.3 * jax.random.normal(sub_keys[6], (D_MODEL,), jnp.float32)).astype(jnp.bfloat16),
        "ln2_gain": 1.0 + 0.3 * jax.random.normal(sub_keys[7], (D_MODEL,), jnp.float32),
        "ln2_bias": 0.3 * jax.random.normal(sub_keys[8], (D_MODEL,), jnp.float32),
        "w_up": (jax.random.normal(sub_keys[9], (D_MODEL, FF_DIM), jnp.float32) * D_MODEL ** -0.5).astype(jnp.bfloat16),
        "b_up": (0.5 * jax.random.normal(sub_keys[10], (FF_DIM,), jnp.float32)).astype(jnp.bfloat16),
        "w_down": (jax.random.normal(sub_keys[11], (FF_DIM, D_MODEL), jnp.float32) * FF_DIM ** -0.5).astype(jnp.bfloat16),
        "b_down": (0.3 * jax.random.normal(sub_keys[12], (D_MODEL,), jnp.float32)).astype(jnp.bfloat16),
    }


def reference(hidden, ln1_gain, ln1_bias, w_qkv, b_qkv, w_out, b_out, ln2_gain, ln2_bias, w_up, b_up, w_down, b_down):
    normed = layer_norm(hidden, ln1_gain, ln1_bias).reshape(N_BATCH * SEQ_LEN, D_MODEL)
    qkv_acc = jnp.dot(normed, w_qkv.reshape(D_MODEL, 3 * D_MODEL), preferred_element_type=jnp.float32)
    qkv_all = (qkv_acc + b_qkv.reshape(3 * D_MODEL).astype(jnp.float32)).astype(jnp.bfloat16)
    head_major = jnp.transpose(qkv_all.reshape(N_BATCH, SEQ_LEN, 3, N_HEADS, HEAD_DIM), (2, 3, 0, 1, 4))
    positions = jnp.arange(SEQ_LEN)
    causal = positions[:, None] >= positions[None, :]

    def one_head(operands):
        queries, keys_all, values = operands
        logits = jnp.einsum("bqd,bkd->bqk", queries.astype(jnp.float32), keys_all.astype(jnp.float32)) * HEAD_DIM ** -0.5
        logits = jnp.where(causal, logits, -1e30)
        row_max = jnp.max(logits, axis=-1, keepdims=True)
        exp_vals = jnp.exp(logits - row_max)
        weights_bf = (exp_vals / jnp.sum(exp_vals, axis=-1, keepdims=True)).astype(jnp.bfloat16)
        return jnp.einsum("bqk,bkd->bqd", weights_bf.astype(jnp.float32), values.astype(jnp.float32)).astype(jnp.bfloat16)

    context = lax.map(one_head, (head_major[0], head_major[1], head_major[2]))
    attn_sum = jnp.einsum("hbsd,hde->bse", context.astype(jnp.float32), w_out.astype(jnp.float32))
    resid_mid = (hidden.astype(jnp.float32) + (attn_sum + b_out.astype(jnp.float32))).astype(jnp.bfloat16)
    normed_mid = layer_norm(resid_mid, ln2_gain, ln2_bias).reshape(N_BATCH * SEQ_LEN, D_MODEL)
    up_proj = jnp.dot(normed_mid, w_up, preferred_element_type=jnp.float32) + b_up.astype(jnp.float32)
    gelu_out = jax.nn.gelu(up_proj, approximate=True).astype(jnp.bfloat16)
    down_sum = jnp.dot(gelu_out, w_down, preferred_element_type=jnp.float32) + b_down.astype(jnp.float32)
    return (resid_mid.astype(jnp.float32) + down_sum.reshape(N_BATCH, SEQ_LEN, D_MODEL)).astype(jnp.bfloat16)
```

```python
import functools

import jax
import jax.numpy as jnp
from jax import lax
from jax.experimental import pallas as pl
from jax.experimental.pallas import tpu as pltpu
from jax.sharding import PartitionSpec as P

LN_EPS = 1e-5
MESH = pl.DeviceIdType.MESH
CH = 512
LOOK = 4
LAG_B, LAG_C = 2, 3
LAG_P, LAG_H, LAG_F = 1, 3, 5
N_WD = 6


def f32(v):
    return v.astype(jnp.float32)


def dot(a, b):
    return jnp.dot(a, b, preferred_element_type=jnp.float32)


def layer_kernel(
    n_dev,
    x_ref, g1_ref, s1_ref, wqkv, bqkv_ref, wo, bo_ref, g2_ref, s2_ref, wu, bu_ref, wd, bd_ref,
    out_ref,
    h_all, u_w, d_w, o_w, acc, qkv, ctx, act, psend, precv,
    hop_s, hop_r, fin_s, fin_r, x1,
    usem, osem, dsem, ag_send, ag_l, ag_r, ag_l2, ag_r2, ag_p,
    rs_send, rs_p, rs_hl, rs_hr, rs_fl, rs_fr,
):
    n_chips = n_dev // 2
    rows, dim = x_ref.shape
    nch = dim // CH
    half = rows // 2
    side = rows * n_chips
    n_tok = 2 * side
    n_slab = wqkv.shape[0]
    hd = wqkv.shape[2]
    heads = n_slab // 3
    qw = n_slab * hd
    ff = wu.shape[1]
    me = lax.axis_index("tp")
    chip, core = me // 2, me % 2
    right = {"tp": ((chip + 1) % n_chips) * 2 + core}
    left = {"tp": ((chip + n_chips - 1) % n_chips) * 2 + core}
    mate = {"tp": chip * 2 + (1 - core)}

    def push(src, dst, ssem, rsem, dev):
        return pltpu.make_async_remote_copy(
            src_ref=src, dst_ref=dst, send_sem=ssem, recv_sem=rsem, device_id=dev, device_id_type=MESH)

    barrier = pltpu.get_barrier_semaphore()
    for dev in (left, right, mate):
        pl.semaphore_signal(barrier, inc=1, device_id=dev, device_id_type=MESH)

    def load_qkv(j):
        for s in range(n_slab):
            pltpu.make_async_copy(
                wqkv.at[s, pl.ds(pl.multiple_of(j * CH, CH), CH), :],
                u_w.at[j, :, pl.ds(s * hd, hd)], usem.at[j]).start()

    def load_up(j):
        return pltpu.make_async_copy(
            wu.at[pl.ds(pl.multiple_of(j * CH, CH), CH), :], u_w.at[j], usem.at[j])

    def load_down(j):
        slot = j % N_WD
        return pltpu.make_async_copy(
            wd.at[:, pl.ds(pl.multiple_of(j * CH, CH), CH)], d_w.at[slot], dsem.at[slot])

    def init_loads(j, c):
        load_qkv(j)
        return c

    lax.fori_loop(0, nch, init_loads, 0)
    out_load = pltpu.make_async_copy(wo, o_w, osem)
    out_load.start()
    for j in range(N_WD):
        load_down(j).start()

    def norm(get, gain_ref, shift_ref):
        tot = jnp.zeros((rows, CH), jnp.float32)
        for j in range(nch):
            tot += get(j)
        mean = jnp.sum(tot, axis=1, keepdims=True) * (1.0 / dim)
        tot = jnp.zeros((rows, CH), jnp.float32)
        for j in range(nch):
            cen = get(j) - mean
            tot += cen * cen
        var = jnp.sum(tot, axis=1, keepdims=True) * (1.0 / dim)
        inv = lax.rsqrt(var + LN_EPS)
        for j in range(nch):
            cols = slice(j * CH, (j + 1) * CH)
            y = (get(j) - mean) * inv * gain_ref[:, cols] + shift_ref[:, cols]
            h_all[j, 0:rows, :] = y.astype(jnp.bfloat16)

    norm(lambda j: f32(x_ref[:, j * CH:(j + 1) * CH]), g1_ref, s1_ref)
    acc[...] = jnp.zeros_like(acc)
    pl.semaphore_wait(barrier, 3)

    def at(j, s, r, lo=0, n=rows):
        return h_all.at[j, pl.ds(s * side + r * rows + lo, n), :]

    def gather(consume):
        def own(j):
            push(at(j, 0, 0), at(j, 0, n_chips - 1), ag_send, ag_l.at[j], right).start()
            push(at(j, 0, 0), at(j, 0, 1), ag_send, ag_r.at[j], left).start()
            push(at(j, 0, 0), at(j, 1, 0), ag_send, ag_p.at[j], mate).start()

        for j in range(LOOK):
            own(j)

        def step(i, c):
            @pl.when(i + LOOK < nch)
            def _():
                own(i + LOOK)

            @pl.when(i < nch)
            def _():
                push(at(i, 0, 0), at(i, 0, 3), ag_send, ag_l.at[i], right).wait_recv()
                push(at(i, 0, 3, 0, half), at(i, 0, 2, 0, half), ag_send, ag_l2.at[i], right).start()
                push(at(i, 0, 3), at(i, 1, 3), ag_send, ag_p.at[i], mate).start()
                push(at(i, 0, 0), at(i, 0, 1), ag_send, ag_r.at[i], left).wait_recv()
                push(at(i, 0, 1, half, half), at(i, 0, 2, half, half), ag_send, ag_r2.at[i], left).start()
                push(at(i, 0, 1), at(i, 1, 1), ag_send, ag_p.at[i], mate).start()

            @pl.when((i >= LAG_B) & (i < nch + LAG_B))
            def _():
                j = i - LAG_B
                push(at(j, 0, 3, 0, half), at(j, 0, 2, 0, half), ag_send, ag_l2.at[j], right).wait_recv()
                push(at(j, 0, 1, half, half), at(j, 0, 2, half, half), ag_send, ag_r2.at[j], left).wait_recv()
                push(at(j, 0, 2), at(j, 1, 2), ag_send, ag_p.at[j], mate).start()

            @pl.when(i >= LAG_C)
            def _():
                j = i - LAG_C
                push(at(j, 0, 0, 0, side), at(j, 1, 0, 0, side), ag_send, ag_p.at[j], mate).wait_recv()
                consume(j)
            return c

        lax.fori_loop(0, nch + LAG_C, step, 0)

    def gather_drain():
        sent = h_all.at[:, pl.ds(0, 7 * rows), :]
        push(sent, sent, ag_send, ag_p.at[0], mate).wait_send()

    def own_part(j, r, lo=0, n=rows):
        return acc.at[j // 2, pl.ds((j % 2) * side + r * rows + lo, n), :]

    def scatter(partial, finish):
        def step(i, c):
            @pl.when(i < nch)
            def _():
                p = partial(i)
                acc[i // 2, pl.ds(pl.multiple_of((i % 2) * side, side), side), :] = p[0:side]
                psend[i] = p[side:].astype(jnp.bfloat16)
                push(psend.at[i], precv.at[i], rs_send, rs_p.at[i], mate).start()

            @pl.when((i >= LAG_P) & (i < nch + LAG_P))
            def _():
                j = i - LAG_P
                base = pl.multiple_of((j % 2) * side, side)
                push(psend.at[j], precv.at[j], rs_send, rs_p.at[j], mate).wait_recv()
                s = acc[j // 2, pl.ds(base, side), :] + f32(precv[j])
                hop_s[0, j] = s[2 * rows:2 * rows + half].astype(jnp.bfloat16)
                hop_s[1, j] = s[2 * rows + half:3 * rows].astype(jnp.bfloat16)
                push(hop_s.at[0, j], hop_r.at[0, j], rs_send, rs_hl.at[j], right).start()
                push(hop_s.at[1, j], hop_r.at[1, j], rs_send, rs_hr.at[j], left).start()
                acc[j // 2, pl.ds(base, side), :] = s

            @pl.when((i >= LAG_H) & (i < nch + LAG_H))
            def _():
                j = i - LAG_H
                base = pl.multiple_of((j % 2) * side, side)
                push(hop_s.at[0, j], hop_r.at[0, j], rs_send, rs_hl.at[j], right).wait_recv()
                one = acc[j // 2, pl.ds(base + rows, rows), :]
                fin_s[0, j, 0:half] = (one[0:half] + f32(hop_r[0, j])).astype(jnp.bfloat16)
                fin_s[0, j, half:] = one[half:].astype(jnp.bfloat16)
                push(fin_s.at[0, j], fin_r.at[0, j], rs_send, rs_fl.at[j], right).start()
                push(hop_s.at[1, j], hop_r.at[1, j], rs_send, rs_hr.at[j], left).wait_recv()
                three = acc[j // 2, pl.ds(base + 3 * rows, rows), :]
                fin_s[1, j, 0:half] = three[0:half].astype(jnp.bfloat16)
                fin_s[1, j, half:] = (three[half:] + f32(hop_r[1, j])).astype(jnp.bfloat16)
                push(fin_s.at[1, j], fin_r.at[1, j], rs_send, rs_fr.at[j], left).start()

            @pl.when(i >= LAG_F)
            def _():
                j = i - LAG_F
                base = pl.multiple_of((j % 2) * side, side)
                push(fin_s.at[0, j], fin_r.at[0, j], rs_send, rs_fl.at[j], right).wait_recv()
                push(fin_s.at[1, j], fin_r.at[1, j], rs_send, rs_fr.at[j], left).wait_recv()
                finish(j, acc[j // 2, pl.ds(base, rows), :] + f32(fin_r[0, j]) + f32(fin_r[1, j]))
            return c

        lax.fori_loop(0, nch + LAG_F, step, 0)

    def scatter_drain():
        push(psend, precv, rs_send, rs_p.at[0], mate).wait_send()
        push(hop_s, hop_r, rs_send, rs_p.at[0], mate).wait_send()
        push(fin_s, fin_r, rs_send, rs_p.at[0], mate).wait_send()

    tiles = [(t, min(CH, qw - t * CH)) for t in range((qw + CH - 1) // CH)]

    def use_qkv(j):
        pltpu.make_async_copy(u_w.at[j, :, pl.ds(0, qw)], u_w.at[j, :, pl.ds(0, qw)], usem.at[j]).wait()
        for t, n in tiles:
            acc[t, :, 0:n] += dot(h_all[j], u_w[j, :, t * CH:t * CH + n])
        load_up(j).start()

    gather(use_qkv)
    for t, n in tiles:
        cols = slice(t * CH, t * CH + n)
        qkv[:, cols] = (acc[t, :, 0:n] + f32(bqkv_ref[:, cols])).astype(jnp.bfloat16)

    def position(i):
        s, r, w = i // side, (i // rows) % n_chips, i % rows
        return ((chip + r) % n_chips) * (2 * rows) + (core + s - 2 * core * s) * rows + w

    qpos = position(lax.broadcasted_iota(jnp.int32, (n_tok, n_tok), 0))
    kpos = position(lax.broadcasted_iota(jnp.int32, (n_tok, n_tok), 1))
    keep = qpos >= kpos
    for h in range(heads):
        q = qkv[:, h * hd:(h + 1) * hd]
        k = qkv[:, (heads + h) * hd:(heads + h + 1) * hd]
        v = qkv[:, (2 * heads + h) * hd:(2 * heads + h + 1) * hd]
        logits = lax.dot_general(q, k, (((1,), (1,)), ((), ())), preferred_element_type=jnp.float32) * hd ** -0.5
        logits = jnp.where(keep, logits, -1e30)
        e = jnp.exp(logits - jnp.max(logits, axis=1, keepdims=True))
        p = (e / jnp.sum(e, axis=1, keepdims=True)).astype(jnp.bfloat16)
        ctx[:, h * hd:(h + 1) * hd] = dot(p, v).astype(jnp.bfloat16)

    gather_drain()
    out_load.wait()

    def out_part(j):
        return dot(ctx[...], o_w[:, pl.ds(pl.multiple_of(j * CH, CH), CH)])

    def out_finish(j, total):
        cols = pl.ds(pl.multiple_of(j * CH, CH), CH)
        x1[j] = (f32(x_ref[:, cols]) + (total + f32(bo_ref[:, cols]))).astype(jnp.bfloat16)

    scatter(out_part, out_finish)

    norm(lambda j: f32(x1[j]), g2_ref, s2_ref)
    acc[...] = jnp.zeros_like(acc)

    def use_up(j):
        load_up(j).wait()
        for t in range(ff // CH):
            acc[t] += dot(h_all[j], u_w[j, :, t * CH:(t + 1) * CH])

    gather(use_up)
    for t in range(ff // CH):
        cols = slice(t * CH, (t + 1) * CH)
        a = acc[t] + f32(bu_ref[:, cols])
        act[:, cols] = jax.nn.gelu(a, approximate=True).astype(jnp.bfloat16)
    scatter_drain()
    gather_drain()

    def down_part(j):
        load_down(j).wait()
        p = dot(act[...], d_w[j % N_WD])

        @pl.when(j + N_WD < nch)
        def _():
            load_down(j + N_WD).start()
        return p

    def down_finish(j, total):
        cols = pl.ds(pl.multiple_of(j * CH, CH), CH)
        out_ref[:, cols] = (f32(x1[j]) + (total + f32(bd_ref[:, cols]))).astype(jnp.bfloat16)

    scatter(down_part, down_finish)
    scatter_drain()


def solution(mesh):
    n_dev = mesh.shape["tp"]

    def body(hidden, g1, s1, w_qkv, b_qkv, w_out, b_out, g2, s2, w_up, b_up, w_down, b_down):
        _, rows, dim = hidden.shape
        _, three, heads, hd = w_qkv.shape
        ff = w_up.shape[1]
        nch = dim // CH
        n_tok, side, half = rows * n_dev, rows * n_dev // 2, rows // 2
        bf, fl = jnp.bfloat16, jnp.float32
        row = lambda v: v.reshape(1, -1)
        vmem = pl.BlockSpec(memory_space=pltpu.VMEM)
        hbm = pl.BlockSpec(memory_space=pl.ANY)
        dma = pltpu.SemaphoreType.DMA
        out = pl.pallas_call(
            functools.partial(layer_kernel, n_dev),
            out_shape=jax.ShapeDtypeStruct((rows, dim), bf),
            in_specs=[vmem, vmem, vmem, hbm, vmem, hbm, vmem, vmem, vmem, hbm, vmem, hbm, vmem],
            out_specs=vmem,
            scratch_shapes=[
                pltpu.VMEM((nch, n_tok, CH), bf),
                pltpu.VMEM((nch, CH, ff), bf),
                pltpu.VMEM((N_WD, ff, CH), bf),
                pltpu.VMEM((heads * hd, dim), bf),
                pltpu.VMEM((nch // 2, n_tok, CH), fl),
                pltpu.VMEM((n_tok, three * heads * hd), bf),
                pltpu.VMEM((n_tok, heads * hd), bf),
                pltpu.VMEM((n_tok, ff), bf),
                pltpu.VMEM((nch, side, CH), bf),
                pltpu.VMEM((nch, side, CH), bf),
                pltpu.VMEM((2, nch, half, CH), bf),
                pltpu.VMEM((2, nch, half, CH), bf),
                pltpu.VMEM((2, nch, rows, CH), bf),
                pltpu.VMEM((2, nch, rows, CH), bf),
                pltpu.VMEM((nch, rows, CH), bf),
                dma((nch,)), dma(()), dma((N_WD,)),
                dma(()), dma((nch,)), dma((nch,)), dma((nch,)), dma((nch,)), dma((nch,)),
                dma(()), dma((nch,)), dma((nch,)), dma((nch,)), dma((nch,)), dma((nch,)),
            ],
            compiler_params=pltpu.CompilerParams(
                collective_id=0, has_side_effects=True, vmem_limit_bytes=67043328),
            name="decoder_layer",
        )(
            hidden[0], row(g1), row(s1),
            jnp.transpose(w_qkv, (1, 2, 0, 3)).reshape(three * heads, dim, hd), row(b_qkv),
            w_out.reshape(heads * hd, dim), row(b_out), row(g2), row(s2), w_up, row(b_up), w_down, row(b_down),
        )
        return out[None]

    specs = (P("dp", "tp", None), P(), P(), P(None, None, "tp", None), P(None, "tp", None),
             P("tp", None, None), P(), P(), P(), P(None, "tp"), P("tp"), P("tp", None), P())
    return jax.shard_map(body, mesh=mesh, in_specs=specs, out_specs=P("dp", "tp", None), check_vma=False)
```

```python
import functools

import jax
import jax.numpy as jnp
from jax import lax
from jax.experimental import pallas as pl
from jax.experimental.pallas import tpu as pltpu
from jax.sharding import PartitionSpec as P

LN_EPS = 1e-5
MESH = pl.DeviceIdType.MESH
CH = 512
LOOK = 5
LAG_B, LAG_C = 5, 6
LAGS_OUT = (2, 8, 12)
LAGS_DOWN = (2, 5, 9)
N_WD = 6


def f32(v):
    return v.astype(jnp.float32)


def dot(a, b):
    return jnp.dot(a, b, preferred_element_type=jnp.float32)


def layer_kernel(
    n_dev,
    x_hbm, g1_hbm, s1_hbm, wqkv, bqkv_hbm, wo, bo_hbm, g2_hbm, s2_hbm, wu, bu_hbm, wd, bd_hbm,
    out_hbm,
    x_ref, g1_ref, s1_ref, g2_ref, s2_ref, bqkv_ref, bo_ref, bu_ref, bd_ref,
    xb, h_all, u_w, d_w, o_w, acc, qkv, ctx, act, psend, precv,
    hop_s, hop_r, fin_s, fin_r, x1,
    xsem, psem, usem, osem, dsem, outsem, ag_send, ag_l, ag_r, ag_l2, ag_r2, ag_p,
    rs_send, rs_p, rs_hl, rs_hr, rs_fl, rs_fr,
):
    small = [pltpu.make_async_copy(a, b, xsem.at[i]) for i, (a, b) in enumerate(
        ((x_hbm, x_ref), (g1_hbm, g1_ref), (s1_hbm, s1_ref)))]
    late = [pltpu.make_async_copy(a, b, psem.at[i]) for i, (a, b) in enumerate(
        ((bqkv_hbm, bqkv_ref), (bo_hbm, bo_ref), (g2_hbm, g2_ref), (s2_hbm, s2_ref), (bu_hbm, bu_ref), (bd_hbm, bd_ref)))]
    for copy in small:
        copy.start()
    n_chips = n_dev // 2
    rows, dim = x_ref.shape
    nch = dim // CH
    half = rows // 2
    side = rows * n_chips
    n_tok = 2 * side
    n_slab = wqkv.shape[0]
    hd = wqkv.shape[2]
    heads = n_slab // 3
    qw = n_slab * hd
    ff = wu.shape[1]
    me = lax.axis_index("tp")
    chip, core = me // 2, me % 2
    right = {"tp": ((chip + 1) % n_chips) * 2 + core}
    left = {"tp": ((chip + n_chips - 1) % n_chips) * 2 + core}
    mate = {"tp": chip * 2 + (1 - core)}

    def push(src, dst, ssem, rsem, dev):
        return pltpu.make_async_remote_copy(
            src_ref=src, dst_ref=dst, send_sem=ssem, recv_sem=rsem, device_id=dev, device_id_type=MESH)

    barrier = pltpu.get_barrier_semaphore()
    for dev in (left, right, mate):
        pl.semaphore_signal(barrier, inc=1, device_id=dev, device_id_type=MESH)

    def load_qkv(j):
        for s in range(n_slab):
            pltpu.make_async_copy(
                wqkv.at[s, pl.ds(pl.multiple_of(j * CH, CH), CH), :],
                u_w.at[j, :, pl.ds(s * hd, hd)], usem.at[j]).start()

    def load_up(j):
        return pltpu.make_async_copy(
            wu.at[pl.ds(pl.multiple_of(j * CH, CH), CH), :], u_w.at[j], usem.at[j])

    def load_down(j):
        slot = j % N_WD
        return pltpu.make_async_copy(
            wd.at[:, pl.ds(pl.multiple_of(j * CH, CH), CH)], d_w.at[slot], dsem.at[slot])

    def init_loads(j, c):
        load_qkv(j)
        return c

    lax.fori_loop(0, nch, init_loads, 0)
    for copy in late:
        copy.start()
    out_load = pltpu.make_async_copy(wo, o_w, osem)
    out_load.start()
    for j in range(N_WD):
        load_down(j).start()

    def norm(get, gain_ref, shift_ref):
        tot = jnp.zeros((rows, CH), jnp.float32)
        for j in range(nch):
            tot += get(j)
        mean = jnp.sum(tot, axis=1, keepdims=True) * (1.0 / dim)
        tot = jnp.zeros((rows, CH), jnp.float32)
        for j in range(nch):
            cen = get(j) - mean
            tot += cen * cen
        var = jnp.sum(tot, axis=1, keepdims=True) * (1.0 / dim)
        inv = lax.rsqrt(var + LN_EPS)
        for j in range(nch):
            cols = slice(j * CH, (j + 1) * CH)
            y = (get(j) - mean) * inv * gain_ref[:, cols] + shift_ref[:, cols]
            h_all[j, 0:rows, :] = y.astype(jnp.bfloat16)

    for copy in small:
        copy.wait()
    norm(lambda j: f32(x_ref[:, j * CH:(j + 1) * CH]), g1_ref, s1_ref)
    acc[...] = jnp.zeros_like(acc)
    pl.semaphore_wait(barrier, 3)

    def at(j, s, r, lo=0, n=rows):
        return h_all.at[j, pl.ds(s * side + r * rows + lo, n), :]

    def gather(consume):
        def own(j):
            push(at(j, 0, 0), at(j, 0, n_chips - 1), ag_send, ag_l.at[j], right).start()
            push(at(j, 0, 0), at(j, 0, 1), ag_send, ag_r.at[j], left).start()
            push(at(j, 0, 0), at(j, 1, 0), ag_send, ag_p.at[j], mate).start()

        for j in range(LOOK):
            own(j)

        def step(i, c):
            @pl.when(i + LOOK < nch)
            def _():
                own(i + LOOK)

            @pl.when(i < nch)
            def _():
                push(at(i, 0, 0), at(i, 0, 3), ag_send, ag_l.at[i], right).wait_recv()
                push(at(i, 0, 3, 0, half), at(i, 0, 2, 0, half), ag_send, ag_l2.at[i], right).start()
                push(at(i, 0, 3), at(i, 1, 3), ag_send, ag_p.at[i], mate).start()
                push(at(i, 0, 0), at(i, 0, 1), ag_send, ag_r.at[i], left).wait_recv()
                push(at(i, 0, 1, half, half), at(i, 0, 2, half, half), ag_send, ag_r2.at[i], left).start()
                push(at(i, 0, 1), at(i, 1, 1), ag_send, ag_p.at[i], mate).start()

            @pl.when((i >= LAG_B) & (i < nch + LAG_B))
            def _():
                j = i - LAG_B
                push(at(j, 0, 3, 0, half), at(j, 0, 2, 0, half), ag_send, ag_l2.at[j], right).wait_recv()
                push(at(j, 0, 1, half, half), at(j, 0, 2, half, half), ag_send, ag_r2.at[j], left).wait_recv()
                push(at(j, 0, 2), at(j, 1, 2), ag_send, ag_p.at[j], mate).start()

            @pl.when(i >= LAG_C)
            def _():
                j = i - LAG_C
                push(at(j, 0, 0, 0, side), at(j, 1, 0, 0, side), ag_send, ag_p.at[j], mate).wait_recv()
                consume(j)
            return c

        lax.fori_loop(0, nch + LAG_C, step, 0)

    def gather_drain():
        sent = h_all.at[:, pl.ds(0, 7 * rows), :]
        push(sent, sent, ag_send, ag_p.at[0], mate).wait_send()

    def own_part(j, r, lo=0, n=rows):
        return acc.at[j // 2, pl.ds((j % 2) * side + r * rows + lo, n), :]

    def scatter(partial, finish, lags):
        lag_p, lag_h, lag_f = lags

        def step(i, c):
            @pl.when(i < nch)
            def _():
                p = partial(i)
                acc[i // 2, pl.ds(pl.multiple_of((i % 2) * side, side), side), :] = p[0:side]
                psend[i] = p[side:].astype(jnp.bfloat16)
                push(psend.at[i], precv.at[i], rs_send, rs_p.at[i], mate).start()

            @pl.when((i >= lag_p) & (i < nch + lag_p))
            def _():
                j = i - lag_p
                base = pl.multiple_of((j % 2) * side, side)
                push(psend.at[j], precv.at[j], rs_send, rs_p.at[j], mate).wait_recv()
                s = acc[j // 2, pl.ds(base, side), :] + f32(precv[j])
                hop_s[0, j] = s[2 * rows:2 * rows + half].astype(jnp.bfloat16)
                hop_s[1, j] = s[2 * rows + half:3 * rows].astype(jnp.bfloat16)
                push(hop_s.at[0, j], hop_r.at[0, j], rs_send, rs_hl.at[j], right).start()
                push(hop_s.at[1, j], hop_r.at[1, j], rs_send, rs_hr.at[j], left).start()
                acc[j // 2, pl.ds(base, side), :] = s

            @pl.when((i >= lag_h) & (i < nch + lag_h))
            def _():
                j = i - lag_h
                base = pl.multiple_of((j % 2) * side, side)
                push(hop_s.at[0, j], hop_r.at[0, j], rs_send, rs_hl.at[j], right).wait_recv()
                one = acc[j // 2, pl.ds(base + rows, rows), :]
                fin_s[0, j, 0:half] = (one[0:half] + f32(hop_r[0, j])).astype(jnp.bfloat16)
                fin_s[0, j, half:] = one[half:].astype(jnp.bfloat16)
                push(fin_s.at[0, j], fin_r.at[0, j], rs_send, rs_fl.at[j], right).start()
                push(hop_s.at[1, j], hop_r.at[1, j], rs_send, rs_hr.at[j], left).wait_recv()
                three = acc[j // 2, pl.ds(base + 3 * rows, rows), :]
                fin_s[1, j, 0:half] = three[0:half].astype(jnp.bfloat16)
                fin_s[1, j, half:] = (three[half:] + f32(hop_r[1, j])).astype(jnp.bfloat16)
                push(fin_s.at[1, j], fin_r.at[1, j], rs_send, rs_fr.at[j], left).start()

            @pl.when(i >= lag_f)
            def _():
                j = i - lag_f
                base = pl.multiple_of((j % 2) * side, side)
                push(fin_s.at[0, j], fin_r.at[0, j], rs_send, rs_fl.at[j], right).wait_recv()
                push(fin_s.at[1, j], fin_r.at[1, j], rs_send, rs_fr.at[j], left).wait_recv()
                finish(j, acc[j // 2, pl.ds(base, rows), :] + f32(fin_r[0, j]) + f32(fin_r[1, j]))
            return c

        lax.fori_loop(0, nch + lag_f, step, 0)

    def scatter_drain():
        push(psend, precv, rs_send, rs_p.at[0], mate).wait_send()
        push(hop_s, hop_r, rs_send, rs_p.at[0], mate).wait_send()
        push(fin_s, fin_r, rs_send, rs_p.at[0], mate).wait_send()

    tiles = [(t, min(CH, qw - t * CH)) for t in range((qw + CH - 1) // CH)]

    def use_qkv(j):
        pltpu.make_async_copy(u_w.at[j, :, pl.ds(0, qw)], u_w.at[j, :, pl.ds(0, qw)], usem.at[j]).wait()
        for t, n in tiles:
            acc[t, :, 0:n] += dot(h_all[j], u_w[j, :, t * CH:t * CH + n])
        load_up(j).start()

    gather(use_qkv)
    for copy in late:
        copy.wait()
    for s in range(n_slab):
        lo = s * hd
        part = acc[lo // CH, :, lo % CH:lo % CH + hd]
        qkv[:, lo:lo + hd] = (part + f32(bqkv_ref[s % heads, s // heads:s // heads + 1, :])).astype(jnp.bfloat16)

    def position(i):
        s, r, w = i // side, (i // rows) % n_chips, i % rows
        return ((chip + r) % n_chips) * (2 * rows) + (core + s - 2 * core * s) * rows + w

    qpos = position(lax.broadcasted_iota(jnp.int32, (n_tok, n_tok), 0))
    kpos = position(lax.broadcasted_iota(jnp.int32, (n_tok, n_tok), 1))
    keep = qpos >= kpos
    for h in range(heads):
        q = qkv[:, h * hd:(h + 1) * hd]
        k = qkv[:, (heads + h) * hd:(heads + h + 1) * hd]
        v = qkv[:, (2 * heads + h) * hd:(2 * heads + h + 1) * hd]
        logits = lax.dot_general(q, k, (((1,), (1,)), ((), ())), preferred_element_type=jnp.float32) * hd ** -0.5
        logits = jnp.where(keep, logits, -1e30)
        e = jnp.exp(logits - jnp.max(logits, axis=1, keepdims=True))
        p = (e / jnp.sum(e, axis=1, keepdims=True)).astype(jnp.bfloat16)
        ctx[:, h * hd:(h + 1) * hd] = dot(p, v).astype(jnp.bfloat16)

    gather_drain()
    out_load.wait()

    bo = f32(bo_ref[...]).reshape(1, dim)
    for j in range(nch):
        cols = slice(j * CH, (j + 1) * CH)
        xb[j] = f32(x_ref[:, cols]) + bo[:, cols]

    def out_part(j):
        return dot(ctx[...], o_w[:, pl.ds(pl.multiple_of(j * CH, CH), CH)])

    def out_finish(j, total):
        x1[j] = (xb[j] + total).astype(jnp.bfloat16)

    scatter(out_part, out_finish, LAGS_OUT)

    norm(lambda j: f32(x1[j]), g2_ref, s2_ref)
    acc[...] = jnp.zeros_like(acc)

    def use_up(j):
        load_up(j).wait()
        for t in range(ff // CH):
            acc[t] += dot(h_all[j], u_w[j, :, t * CH:(t + 1) * CH])

    gather(use_up)
    bu = f32(bu_ref[...]).reshape(1, ff)
    for t in range(ff // CH):
        cols = slice(t * CH, (t + 1) * CH)
        a = acc[t] + bu[:, cols]
        act[:, cols] = jax.nn.gelu(a, approximate=True).astype(jnp.bfloat16)
    scatter_drain()
    gather_drain()

    bd = f32(bd_ref[...]).reshape(1, dim)
    for j in range(nch):
        xb[j] = f32(x1[j]) + bd[:, j * CH:(j + 1) * CH]

    def down_part(j):
        load_down(j).wait()
        p = dot(act[...], d_w[j % N_WD])

        @pl.when(j + N_WD < nch)
        def _():
            load_down(j + N_WD).start()
        return p

    def store(j):
        return pltpu.make_async_copy(x1.at[j], out_hbm.at[:, pl.ds(pl.multiple_of(j * CH, CH), CH)], outsem.at[j])

    def down_finish(j, total):
        x1[j] = (xb[j] + total).astype(jnp.bfloat16)
        store(j).start()

    scatter(down_part, down_finish, LAGS_DOWN)
    scatter_drain()
    for j in range(nch):
        store(j).wait()


def solution(mesh):
    n_dev = mesh.shape["tp"]

    def body(hidden, g1, s1, w_qkv, b_qkv, w_out, b_out, g2, s2, w_up, b_up, w_down, b_down):
        _, rows, dim = hidden.shape
        _, three, heads, hd = w_qkv.shape
        ff = w_up.shape[1]
        nch = dim // CH
        n_tok, side, half = rows * n_dev, rows * n_dev // 2, rows // 2
        bf, fl = jnp.bfloat16, jnp.float32
        row = lambda v: v.reshape(1, -1)
        hbm = pl.BlockSpec(memory_space=pl.ANY)
        dma = pltpu.SemaphoreType.DMA
        out = pl.pallas_call(
            functools.partial(layer_kernel, n_dev),
            out_shape=jax.ShapeDtypeStruct((rows, dim), bf),
            in_specs=[hbm] * 13,
            out_specs=hbm,
            scratch_shapes=[
                pltpu.VMEM((rows, dim), bf),
                pltpu.VMEM((1, dim), fl), pltpu.VMEM((1, dim), fl),
                pltpu.VMEM((1, dim), fl), pltpu.VMEM((1, dim), fl),
                pltpu.VMEM((heads, three, hd), bf), pltpu.VMEM((dim,), bf),
                pltpu.VMEM((ff,), bf), pltpu.VMEM((dim,), bf),
                pltpu.VMEM((nch, rows, CH), fl),
                pltpu.VMEM((nch, n_tok, CH), bf),
                pltpu.VMEM((nch, CH, ff), bf),
                pltpu.VMEM((N_WD, ff, CH), bf),
                pltpu.VMEM((heads * hd, dim), bf),
                pltpu.VMEM((nch // 2, n_tok, CH), fl),
                pltpu.VMEM((n_tok, three * heads * hd), bf),
                pltpu.VMEM((n_tok, heads * hd), bf),
                pltpu.VMEM((n_tok, ff), bf),
                pltpu.VMEM((nch, side, CH), bf),
                pltpu.VMEM((nch, side, CH), bf),
                pltpu.VMEM((2, nch, half, CH), bf),
                pltpu.VMEM((2, nch, half, CH), bf),
                pltpu.VMEM((2, nch, rows, CH), bf),
                pltpu.VMEM((2, nch, rows, CH), bf),
                pltpu.VMEM((nch, rows, CH), bf),
                dma((3,)), dma((6,)), dma((nch,)), dma(()), dma((N_WD,)), dma((nch,)),
                dma(()), dma((nch,)), dma((nch,)), dma((nch,)), dma((nch,)), dma((nch,)),
                dma(()), dma((nch,)), dma((nch,)), dma((nch,)), dma((nch,)), dma((nch,)),
            ],
            compiler_params=pltpu.CompilerParams(
                collective_id=0, has_side_effects=True, vmem_limit_bytes=67043328),
            name="decoder_layer",
        )(
            hidden[0], row(g1), row(s1),
            jnp.transpose(w_qkv, (1, 2, 0, 3)).reshape(three * heads, dim, hd),
            jnp.transpose(b_qkv, (1, 0, 2)),
            w_out.reshape(heads * hd, dim), b_out, row(g2), row(s2), w_up, b_up, w_down, b_down,
        )
        return out[None]

    specs = (P("dp", "tp", None), P(), P(), P(None, None, "tp", None), P(None, "tp", None),
             P("tp", None, None), P(), P(), P(), P(None, "tp"), P("tp"), P("tp", None), P())
    return jax.shard_map(body, mesh=mesh, in_specs=specs, out_specs=P("dp", "tp", None), check_vma=False)
```

```python
import functools

import jax
import jax.numpy as jnp
from jax import lax
from jax.experimental import pallas as pl
from jax.experimental.pallas import tpu as pltpu
from jax.sharding import PartitionSpec as P

LN_EPS = 1e-5
MESH = pl.DeviceIdType.MESH
CH = 512
LOOK = 5
LAG_B, LAG_C = 5, 6
LAGS_OUT = (2, 6, 11)
LAGS_DOWN = (2, 6, 10)
N_WD = 3


def f32(v):
    return v.astype(jnp.float32)


def bf16(v):
    return v.astype(jnp.bfloat16)


def dot(a, b):
    return jnp.dot(a, b, preferred_element_type=jnp.float32)


def layer_kernel(
    n_dev,
    x_hbm, g1_hbm, s1_hbm, wqkv, bqkv_hbm, wo, bo_hbm, g2_hbm, s2_hbm, wu, bu_hbm, wd, bd_hbm,
    out_hbm,
    x_ref, g1_ref, s1_ref, g2_ref, s2_ref, bqkv_ref, bo_ref, bu_ref, bd_ref,
    xb, h_all, u_w, d_w, o_w, acc, qkv, ctx, act, psend, precv,
    hop_s, hop_r, fin_s, fin_r, x1,
    xsem, psem, usem, osem, dsem, outsem, ag_send, ag_l, ag_r, ag_l2, ag_r2, ag_p,
    rs_send, rs_p, rs_hl, rs_hr, rs_fl, rs_fr,
):
    small = [pltpu.make_async_copy(a, b, xsem.at[i]) for i, (a, b) in enumerate(
        ((x_hbm, x_ref), (g1_hbm, g1_ref), (s1_hbm, s1_ref)))]
    late = [pltpu.make_async_copy(a, b, psem.at[i]) for i, (a, b) in enumerate(
        ((bqkv_hbm, bqkv_ref), (bo_hbm, bo_ref), (g2_hbm, g2_ref), (s2_hbm, s2_ref), (bu_hbm, bu_ref), (bd_hbm, bd_ref)))]
    for copy in small:
        copy.start()
    n_chips = n_dev // 2
    rows, dim = x_ref.shape
    nch = dim // CH
    ng = nch // 2
    hr = rows // 2
    side = hr * n_chips
    st_rows = 2 * side
    n_tok = 2 * st_rows
    hc = CH // 2
    n_slab = wqkv.shape[0]
    hd = wqkv.shape[2]
    heads = n_slab // 3
    qw = n_slab * hd
    ff = wu.shape[1]
    nt = ff // CH
    me = lax.axis_index("tp")
    chip, core = me // 2, me % 2
    right = {"tp": ((chip + 1) % n_chips) * 2 + core}
    left = {"tp": ((chip + n_chips - 1) % n_chips) * 2 + core}
    mate = {"tp": chip * 2 + (1 - core)}

    def push(src, dst, ssem, rsem, dev):
        return pltpu.make_async_remote_copy(
            src_ref=src, dst_ref=dst, send_sem=ssem, recv_sem=rsem, device_id=dev, device_id_type=MESH)

    barrier = pltpu.get_barrier_semaphore()
    for dev in (left, right, mate):
        pl.semaphore_signal(barrier, inc=1, device_id=dev, device_id_type=MESH)

    def load_qkv(j):
        for s in range(n_slab):
            pltpu.make_async_copy(
                wqkv.at[s, pl.ds(pl.multiple_of(j * CH, CH), CH), :],
                u_w.at[j, :, pl.ds(s * hd, hd)], usem.at[j]).start()

    def load_up(j):
        return pltpu.make_async_copy(
            wu.at[pl.ds(pl.multiple_of(j * CH, CH), CH), :], u_w.at[j], usem.at[j])

    def load_down(q):
        g, slot = q % ng, q % N_WD
        return pltpu.make_async_copy(
            wd.at[:, pl.ds(pl.multiple_of(g * 2 * CH, 2 * CH), 2 * CH)], d_w.at[slot], dsem.at[slot])

    def init_loads(j, c):
        load_qkv(j)
        return c

    lax.fori_loop(0, nch, init_loads, 0)
    for copy in late:
        copy.start()
    out_load = pltpu.make_async_copy(wo, o_w, osem)
    out_load.start()
    for q in range(N_WD):
        load_down(q).start()

    def norm(get, put, n, gain_ref, shift_ref):
        tot = jnp.zeros((n, CH), jnp.float32)
        for j in range(nch):
            tot += get(j)
        mean = jnp.sum(tot, axis=1, keepdims=True) * (1.0 / dim)
        tot = jnp.zeros((n, CH), jnp.float32)
        for j in range(nch):
            cen = get(j) - mean
            tot += cen * cen
        var = jnp.sum(tot, axis=1, keepdims=True) * (1.0 / dim)
        inv = lax.rsqrt(var + LN_EPS)
        for j in range(nch):
            cols = slice(j * CH, (j + 1) * CH)
            put(j, bf16((get(j) - mean) * inv * gain_ref[:, cols] + shift_ref[:, cols]))

    def put_both(j, y):
        h_all[j, 0, 0:hr, :] = y[0:hr]
        h_all[j, 1, 0:hr, :] = y[hr:]

    def put_stream(st):
        def put(j, y):
            h_all[j, st, 0:hr, :] = y
        return put

    for copy in small:
        copy.wait()
    norm(lambda j: f32(x_ref[:, j * CH:(j + 1) * CH]), put_both, rows, g1_ref, s1_ref)
    acc[...] = jnp.zeros_like(acc)
    pl.semaphore_wait(barrier, 3)

    def piece_both(v, s, r, lo=0, n=CH):
        return h_all.at[v, :, pl.ds(s * side + r * hr, hr), pl.ds(lo, n)]

    def all_both(v, s):
        return h_all.at[v, :, pl.ds(s * side, side), :]

    def piece_stream(v, s, r, lo=0, n=CH):
        return h_all.at[pl.ds((v % ng) * 2, 2), v // ng, pl.ds(s * side + r * hr, hr), pl.ds(lo, n)]

    def all_stream(v, s):
        return h_all.at[pl.ds((v % ng) * 2, 2), v // ng, pl.ds(s * side, side), :]

    def send_own(at, v):
        push(at(v, 0, 0), at(v, 0, 3), ag_send, ag_l.at[v], right).start()
        push(at(v, 0, 0), at(v, 0, 1), ag_send, ag_r.at[v], left).start()
        push(at(v, 0, 0), at(v, 1, 0), ag_send, ag_p.at[v], mate).start()

    def wait_mate(whole, v):
        push(whole(v, 0), whole(v, 1), ag_send, ag_p.at[v], mate).wait_recv()

    def gather(at, whole, n_use, consume, steps):
        def step(i, c):
            @pl.when(i + LOOK < nch)
            def _():
                send_own(at, i + LOOK)

            @pl.when(i < nch)
            def _():
                with jax.named_scope("gw1l"):
                    push(at(i, 0, 0), at(i, 0, 3), ag_send, ag_l.at[i], right).wait_recv()
                push(at(i, 0, 3, 0, hc), at(i, 0, 2, 0, hc), ag_send, ag_l2.at[i], right).start()
                push(at(i, 0, 3), at(i, 1, 3), ag_send, ag_p.at[i], mate).start()
                with jax.named_scope("gw1r"):
                    push(at(i, 0, 0), at(i, 0, 1), ag_send, ag_r.at[i], left).wait_recv()
                push(at(i, 0, 1, hc, hc), at(i, 0, 2, hc, hc), ag_send, ag_r2.at[i], left).start()
                push(at(i, 0, 1), at(i, 1, 1), ag_send, ag_p.at[i], mate).start()

            @pl.when((i >= LAG_B) & (i < nch + LAG_B))
            def _():
                j = i - LAG_B
                with jax.named_scope("gw2"):
                    push(at(j, 0, 3, 0, hc), at(j, 0, 2, 0, hc), ag_send, ag_l2.at[j], right).wait_recv()
                    push(at(j, 0, 1, hc, hc), at(j, 0, 2, hc, hc), ag_send, ag_r2.at[j], left).wait_recv()
                push(at(j, 0, 2), at(j, 1, 2), ag_send, ag_p.at[j], mate).start()

            @pl.when((i >= LAG_C) & (i < n_use + LAG_C))
            def _():
                j = i - LAG_C
                with jax.named_scope("gwp"):
                    wait_mate(whole, j)
                with jax.named_scope("guse"):
                    consume(j)
            return c

        lax.fori_loop(0, steps, step, 0)

    def gather_drain():
        sent = h_all.at[:, :, pl.ds(0, 7 * hr), :]
        push(sent, sent, ag_send, ag_p.at[0], mate).wait_send()

    tiles = [(t, min(CH, qw - t * CH)) for t in range((qw + CH - 1) // CH)]

    def use_qkv(j):
        pltpu.make_async_copy(u_w.at[j, :, pl.ds(0, qw)], u_w.at[j, :, pl.ds(0, qw)], usem.at[j]).wait()
        h = h_all[j].reshape(n_tok, CH)
        for t, n in tiles:
            p = dot(h, u_w[j, :, t * CH:t * CH + n])
            acc[2 * t, :, 0:n] += p[0:st_rows]
            acc[2 * t + 1, :, 0:n] += p[st_rows:]
        load_up(j).start()

    for v in range(LOOK):
        send_own(piece_both, v)
    with jax.named_scope("gather1"):
        gather(piece_both, all_both, nch, use_qkv, nch + LAG_C)
    for copy in late:
        copy.wait()
    for s in range(n_slab):
        lo = s * hd
        for st in range(2):
            part = acc[2 * (lo // CH) + st, :, lo % CH:lo % CH + hd]
            qkv[st * st_rows:(st + 1) * st_rows, lo:lo + hd] = bf16(
                part + f32(bqkv_ref[s % heads, s // heads:s // heads + 1, :]))

    def position(i):
        st, s, r, w = i // st_rows, (i // side) % 2, (i // hr) % n_chips, i % hr
        return ((chip + r) % n_chips) * (2 * rows) + (core + s - 2 * core * s) * rows + st * hr + w

    qpos = position(lax.broadcasted_iota(jnp.int32, (n_tok, n_tok), 0))
    kpos = position(lax.broadcasted_iota(jnp.int32, (n_tok, n_tok), 1))
    keep = qpos >= kpos
    for h in range(heads):
        q = qkv[:, h * hd:(h + 1) * hd]
        k = qkv[:, (heads + h) * hd:(heads + h + 1) * hd]
        v = qkv[:, (2 * heads + h) * hd:(2 * heads + h + 1) * hd]
        logits = lax.dot_general(q, k, (((1,), (1,)), ((), ())), preferred_element_type=jnp.float32) * hd ** -0.5
        logits = jnp.where(keep, logits, -1e30)
        e = jnp.exp(logits - jnp.max(logits, axis=1, keepdims=True))
        p = bf16(e / jnp.sum(e, axis=1, keepdims=True))
        ctx[:, h * hd:(h + 1) * hd] = bf16(dot(p, v))

    gather_drain()
    out_load.wait()

    def pair_sum(v, st, g):
        for c in range(2):
            j = 2 * g + c
            s = acc[v, c * side:(c + 1) * side, :] + f32(precv[st, j])
            two = bf16(s[2 * hr:3 * hr])
            hop_s[0, st, j] = two[:, 0:hc]
            hop_s[1, st, j] = two[:, hc:]
            acc[v, c * side:(c + 1) * side, :] = s

    def middle_sum(v, st, g):
        for c in range(2):
            j = 2 * g + c
            one = acc[v, c * side + hr:c * side + 2 * hr, :]
            fin_s[0, st, j, :, 0:hc] = bf16(one[:, 0:hc] + f32(hop_r[0, st, j]))
            fin_s[0, st, j, :, hc:] = bf16(one[:, hc:])
            three = acc[v, c * side + 3 * hr:(c + 1) * side, :]
            fin_s[1, st, j, :, 0:hc] = bf16(three[:, 0:hc])
            fin_s[1, st, j, :, hc:] = bf16(three[:, hc:] + f32(hop_r[1, st, j]))

    def fins(st, g, v):
        pair = pl.ds(2 * g, 2)
        return (push(fin_s.at[0, st, pair], fin_r.at[0, st, pair], rs_send, rs_fl.at[v], right),
                push(fin_s.at[1, st, pair], fin_r.at[1, st, pair], rs_send, rs_fr.at[v], left))

    def last_sum(v, st, g):
        for copy in fins(st, g, v):
            copy.wait_recv()
        for c in range(2):
            j = 2 * g + c
            total = acc[v, c * side:c * side + hr, :] + f32(fin_r[0, st, j]) + f32(fin_r[1, st, j])
            x1[st, j] = bf16(xb[st, j] + total)

    def scatter_drain():
        push(psend, precv, rs_send, rs_p.at[0], mate).wait_send()
        push(hop_s, hop_r, rs_send, rs_p.at[0], mate).wait_send()
        push(fin_s, fin_r, rs_send, rs_p.at[0], mate).wait_send()

    bo = f32(bo_ref[...]).reshape(1, dim)
    for j in range(nch):
        cols = slice(j * CH, (j + 1) * CH)
        y = f32(x_ref[:, cols]) + bo[:, cols]
        xb[0, j] = y[0:hr]
        xb[1, j] = y[hr:]

    def pairs_out(g):
        two = pl.ds(2 * g, 2)
        return push(psend.at[:, two], precv.at[:, two], rs_send, rs_p.at[g], mate)

    def hops_out(g):
        two = pl.ds(2 * g, 2)
        return (push(hop_s.at[0, :, two], hop_r.at[0, :, two], rs_send, rs_hl.at[g], right),
                push(hop_s.at[1, :, two], hop_r.at[1, :, two], rs_send, rs_hr.at[g], left))

    lag_p, lag_h, lag_f = LAGS_OUT

    def out_step(i, carry):
        @pl.when(i < ng)
        def _():
            with jax.named_scope("spart"):
                for c in range(2):
                    j = 2 * i + c
                    p = dot(ctx[...], o_w[:, pl.ds(pl.multiple_of(j * CH, CH), CH)])
                    for st in range(2):
                        acc[st * ng + i, c * side:(c + 1) * side, :] = p[st * st_rows:st * st_rows + side]
                        psend[st, j] = bf16(p[st * st_rows + side:(st + 1) * st_rows])
            pairs_out(i).start()

        @pl.when((i >= lag_p) & (i < ng + lag_p))
        def _():
            g = i - lag_p
            with jax.named_scope("swp"):
                pairs_out(g).wait_recv()
            for st in range(2):
                pair_sum(st * ng + g, st, g)
            for copy in hops_out(g):
                copy.start()

        @pl.when((i >= lag_h) & (i < ng + lag_h))
        def _():
            g = i - lag_h
            with jax.named_scope("swh"):
                for copy in hops_out(g):
                    copy.wait_recv()
            for st in range(2):
                middle_sum(st * ng + g, st, g)
            for copy in fins(0, g, g):
                copy.start()

        @pl.when(i == ng + lag_h - 1)
        def _():
            for g in range(ng):
                for copy in fins(1, g, ng + g):
                    copy.start()

        @pl.when(i >= lag_f)
        def _():
            g = i - lag_f
            with jax.named_scope("swf"):
                last_sum(g, 0, g)
        return carry

    with jax.named_scope("scatter1"):
        lax.fori_loop(0, ng + lag_f, out_step, 0)

    with jax.named_scope("ln2a"):
        norm(lambda j: f32(x1[0, j]), put_stream(0), hr, g2_ref, s2_ref)
    for v in range(LOOK):
        send_own(piece_stream, v)

    def last_out(g, carry):
        last_sum(ng + g, 1, g)
        return carry

    with jax.named_scope("last1"):
        lax.fori_loop(0, ng, last_out, 0)
    with jax.named_scope("ln2b"):
        norm(lambda j: f32(x1[1, j]), put_stream(1), hr, g2_ref, s2_ref)
    acc[ng:2 * ng] = jnp.zeros((ng, st_rows, CH), jnp.float32)
    bd = f32(bd_ref[...]).reshape(1, dim)
    for j in range(nch):
        for st in range(2):
            xb[st, j] = f32(x1[st, j]) + bd[:, j * CH:(j + 1) * CH]
    for j in range(nch):
        load_up(j).wait()

    def use_up(v):
        st, g = v // ng, v % ng
        h = jnp.concatenate([h_all[2 * g, st], h_all[2 * g + 1, st]], axis=1)
        for t in range(nt):
            w = u_w[pl.ds(2 * g, 2), :, t * CH:(t + 1) * CH].reshape(2 * CH, CH)
            acc[ng + t] += dot(h, w)

    with jax.named_scope("gather2"):
        gather(piece_stream, all_stream, ng, use_up, nch + LAG_B)
    scatter_drain()

    bu = f32(bu_ref[...]).reshape(1, ff)

    def activate(st):
        for t in range(nt):
            cols = slice(t * CH, (t + 1) * CH)
            act[st, :, cols] = bf16(jax.nn.gelu(acc[ng + t] + bu[:, cols], approximate=True))
            acc[ng + t] = jnp.zeros((st_rows, CH), jnp.float32)

    def store(st, j):
        return pltpu.make_async_copy(
            x1.at[st, j],
            out_hbm.at[pl.ds(pl.multiple_of(st * hr, hr), hr), pl.ds(pl.multiple_of(j * CH, CH), CH)], outsem)

    def pairs_down(v, st, g):
        two = pl.ds(2 * g, 2)
        return push(psend.at[st, two], precv.at[st, two], rs_send, rs_p.at[v], mate)

    def hops_down(v, st, g):
        two = pl.ds(2 * g, 2)
        return (push(hop_s.at[0, st, two], hop_r.at[0, st, two], rs_send, rs_hl.at[v], right),
                push(hop_s.at[1, st, two], hop_r.at[1, st, two], rs_send, rs_hr.at[v], left))

    def when_group(k, fn):
        @pl.when(((k >= 0) & (k < ng)) | ((k >= 2 * ng) & (k < 3 * ng)))
        def _():
            st = k // (2 * ng)
            g = k - st * 2 * ng
            fn(st * ng + g, st, g)

    lag_p2, lag_h2, lag_f2 = LAGS_DOWN

    def down_part(v, st, g):
        load_down(v).wait()
        slot = v % N_WD
        with jax.named_scope("dpart"):
            for c in range(2):
                j = 2 * g + c
                p = dot(act[st], d_w[slot, :, c * CH:(c + 1) * CH])
                acc[v, c * side:(c + 1) * side, :] = p[0:side]
                psend[st, j] = bf16(p[side:])

        @pl.when(v + N_WD < 2 * ng)
        def _():
            load_down(v + N_WD).start()
        pairs_down(v, st, g).start()

    def down_pair(v, st, g):
        with jax.named_scope("dwp"):
            pairs_down(v, st, g).wait_recv()
        pair_sum(v, st, g)
        for copy in hops_down(v, st, g):
            copy.start()

    def down_middle(v, st, g):
        with jax.named_scope("dwh"):
            for copy in hops_down(v, st, g):
                copy.wait_recv()
        middle_sum(v, st, g)
        for copy in fins(st, g, v):
            copy.start()

    def down_last(v, st, g):
        with jax.named_scope("dwf"):
            last_sum(v, st, g)
        for c in range(2):
            store(st, 2 * g + c).start()

    def mlp_step(w, carry):
        @pl.when((w == 0) | (w == 2 * ng))
        def _():
            with jax.named_scope("gelu"):
                activate(w // (2 * ng))

        when_group(w, down_part)

        @pl.when((w >= ng) & (w < 2 * ng))
        def _():
            with jax.named_scope("mwp"):
                wait_mate(all_stream, w)
            with jax.named_scope("muse"):
                use_up(w)

        when_group(w - lag_p2, down_pair)
        when_group(w - lag_h2, down_middle)
        when_group(w - lag_f2, down_last)
        return carry

    with jax.named_scope("mlp"):
        lax.fori_loop(0, 3 * ng + lag_f2, mlp_step, 0)
    scatter_drain()
    gather_drain()
    pltpu.make_async_copy(x1, x1, outsem).wait()


def solution(mesh):
    n_dev = mesh.shape["tp"]

    def body(hidden, g1, s1, w_qkv, b_qkv, w_out, b_out, g2, s2, w_up, b_up, w_down, b_down):
        _, rows, dim = hidden.shape
        _, three, heads, hd = w_qkv.shape
        ff = w_up.shape[1]
        nch = dim // CH
        n_tok, hr = rows * n_dev, rows // 2
        st_rows, side = n_tok // 2, n_tok // 4
        bf, fl = jnp.bfloat16, jnp.float32
        row = lambda v: v.reshape(1, -1)
        hbm = pl.BlockSpec(memory_space=pl.ANY)
        dma = pltpu.SemaphoreType.DMA
        out = pl.pallas_call(
            functools.partial(layer_kernel, n_dev),
            out_shape=jax.ShapeDtypeStruct((rows, dim), bf),
            in_specs=[hbm] * 13,
            out_specs=hbm,
            scratch_shapes=[
                pltpu.VMEM((rows, dim), bf),
                pltpu.VMEM((1, dim), fl), pltpu.VMEM((1, dim), fl),
                pltpu.VMEM((1, dim), fl), pltpu.VMEM((1, dim), fl),
                pltpu.VMEM((heads, three, hd), bf), pltpu.VMEM((dim,), bf),
                pltpu.VMEM((ff,), bf), pltpu.VMEM((dim,), bf),
                pltpu.VMEM((2, nch, hr, CH), fl),
                pltpu.VMEM((nch, 2, st_rows, CH), bf),
                pltpu.VMEM((nch, CH, ff), bf),
                pltpu.VMEM((N_WD, ff, 2 * CH), bf),
                pltpu.VMEM((heads * hd, dim), bf),
                pltpu.VMEM((nch, st_rows, CH), fl),
                pltpu.VMEM((n_tok, three * heads * hd), bf),
                pltpu.VMEM((n_tok, heads * hd), bf),
                pltpu.VMEM((2, st_rows, ff), bf),
                pltpu.VMEM((2, nch, side, CH), bf),
                pltpu.VMEM((2, nch, side, CH), bf),
                pltpu.VMEM((2, 2, nch, hr, CH // 2), bf),
                pltpu.VMEM((2, 2, nch, hr, CH // 2), bf),
                pltpu.VMEM((2, 2, nch, hr, CH), bf),
                pltpu.VMEM((2, 2, nch, hr, CH), bf),
                pltpu.VMEM((2, nch, hr, CH), bf),
                dma((3,)), dma((6,)), dma((nch,)), dma(()), dma((N_WD,)), dma(()),
                dma(()), dma((nch,)), dma((nch,)), dma((nch,)), dma((nch,)), dma((nch,)),
                dma(()), dma((nch,)), dma((nch,)), dma((nch,)), dma((nch,)), dma((nch,)),
            ],
            compiler_params=pltpu.CompilerParams(
                collective_id=0, has_side_effects=True, vmem_limit_bytes=67043328),
            name="decoder_layer",
        )(
            hidden[0], row(g1), row(s1),
            jnp.transpose(w_qkv, (1, 2, 0, 3)).reshape(three * heads, dim, hd),
            jnp.transpose(b_qkv, (1, 0, 2)),
            w_out.reshape(heads * hd, dim), b_out, row(g2), row(s2), w_up, b_up, w_down, b_down,
        )
        return out[None]

    specs = (P("dp", "tp", None), P(), P(), P(None, None, "tp", None), P(None, "tp", None),
             P("tp", None, None), P(), P(), P(), P(None, "tp"), P("tp"), P("tp", None), P())
    return jax.shard_map(body, mesh=mesh, in_specs=specs, out_specs=P("dp", "tp", None), check_vma=False)
```

```python
import functools

import jax
import jax.numpy as jnp
from jax import lax
from jax.experimental import pallas as pl
from jax.experimental.pallas import tpu as pltpu
from jax.sharding import PartitionSpec as P

LN_EPS = 1e-5
MESH = pl.DeviceIdType.MESH
CH = 512
GATHER_QKV = (6, 5, 6)
GATHER_UP = (5, 4, 5)
LAGS_OUT = (2, 6, 11)
LAGS_DOWN = (2, 6, 10)
N_WD = 4


def f32(v):
    return v.astype(jnp.float32)


def bf16(v):
    return v.astype(jnp.bfloat16)


def dot(a, b):
    return jnp.dot(a, b, preferred_element_type=jnp.float32)


def layer_kernel(
    n_dev,
    x_hbm, g1_hbm, s1_hbm, wqkv, bqkv_hbm, wo, bo_hbm, g2_hbm, s2_hbm, wu, bu_hbm, wd, bd_hbm,
    out_ref,
    x_ref, g1_ref, s1_ref, g2_ref, s2_ref, bqkv_ref, bo_ref, bu_ref, bd_ref,
    xb, h_all, u_w, pool, acc, qkv, ctx, act, psend, precv,
    hop_s, hop_r, fin_s, fin_r, x1,
    xsem, psem, usem, osem, dsem, ag_send, ag_l, ag_r, ag_l2, ag_r2, ag_p,
    rs_send, rs_p, rs_hl, rs_hr, rs_fl, rs_fr,
):
    small = [pltpu.make_async_copy(a, b, xsem.at[i]) for i, (a, b) in enumerate(
        ((x_hbm, x_ref), (g1_hbm, g1_ref), (s1_hbm, s1_ref)))]
    late = [pltpu.make_async_copy(a, b, psem.at[i]) for i, (a, b) in enumerate(
        ((bqkv_hbm, bqkv_ref), (bo_hbm, bo_ref), (g2_hbm, g2_ref), (s2_hbm, s2_ref), (bu_hbm, bu_ref), (bd_hbm, bd_ref)))]
    for copy in small:
        copy.start()
    n_chips = n_dev // 2
    rows, dim = x_ref.shape
    nch = dim // CH
    ng = nch // 2
    hr = rows // 2
    side = hr * n_chips
    st_rows = 2 * side
    n_tok = 2 * st_rows
    hc = CH // 2
    n_slab = wqkv.shape[0]
    hd = wqkv.shape[2]
    heads = n_slab // 3
    qw = n_slab * hd
    ff = wu.shape[1]
    nt = ff // CH
    me = lax.axis_index("tp")
    chip, core = me // 2, me % 2
    right = {"tp": ((chip + 1) % n_chips) * 2 + core}
    left = {"tp": ((chip + n_chips - 1) % n_chips) * 2 + core}
    mate = {"tp": chip * 2 + (1 - core)}

    def push(src, dst, ssem, rsem, dev):
        return pltpu.make_async_remote_copy(
            src_ref=src, dst_ref=dst, send_sem=ssem, recv_sem=rsem, device_id=dev, device_id_type=MESH)

    barrier = pltpu.get_barrier_semaphore()
    for dev in (left, right, mate):
        pl.semaphore_signal(barrier, inc=1, device_id=dev, device_id_type=MESH)

    def load_qkv(j):
        for s in range(n_slab):
            pltpu.make_async_copy(
                wqkv.at[s, pl.ds(pl.multiple_of(j * CH, CH), CH), :],
                u_w.at[j, :, pl.ds(s * hd, hd)], usem.at[j]).start()

    def load_up(j):
        return pltpu.make_async_copy(
            wu.at[pl.ds(pl.multiple_of(j * CH, CH), CH), :], u_w.at[j], usem.at[j])

    kt = heads * hd
    nk = ff // kt
    o_base = (N_WD - 1) * nk

    def load_down(q):
        g, slot = q % ng, q % N_WD
        for k in range(nk):
            pltpu.make_async_copy(
                wd.at[pl.ds(k * kt, kt), pl.ds(pl.multiple_of(g * 2 * CH, 2 * CH), 2 * CH)],
                pool.at[slot * nk + k], dsem.at[slot]).start()

    def wait_down(q):
        slot = q % N_WD
        pltpu.make_async_copy(pool.at[pl.ds(slot * nk, nk)], pool.at[pl.ds(slot * nk, nk)], dsem.at[slot]).wait()

    def init_loads(j, c):
        load_qkv(j)
        return c

    lax.fori_loop(0, nch, init_loads, 0)
    for copy in late:
        copy.start()
    for g in range(ng):
        pltpu.make_async_copy(wo.at[:, pl.ds(g * 2 * CH, 2 * CH)], pool.at[o_base + g], osem).start()
    for q in range(N_WD - 1):
        load_down(q)

    def norm(get, put, n, gain_ref, shift_ref):
        tot = jnp.zeros((n, CH), jnp.float32)
        for j in range(nch):
            tot += get(j)
        mean = jnp.sum(tot, axis=1, keepdims=True) * (1.0 / dim)
        tot = jnp.zeros((n, CH), jnp.float32)
        for j in range(nch):
            cen = get(j) - mean
            tot += cen * cen
        var = jnp.sum(tot, axis=1, keepdims=True) * (1.0 / dim)
        inv = lax.rsqrt(var + LN_EPS)
        for j in range(nch):
            cols = slice(j * CH, (j + 1) * CH)
            put(j, bf16((get(j) - mean) * inv * gain_ref[:, cols] + shift_ref[:, cols]))

    def put_both(j, y):
        h_all[j, 0, 0:hr, :] = y[0:hr]
        h_all[j, 1, 0:hr, :] = y[hr:]

    def put_stream(st):
        def put(j, y):
            h_all[j, st, 0:hr, :] = y
        return put

    for copy in small:
        copy.wait()
    norm(lambda j: f32(x_ref[:, j * CH:(j + 1) * CH]), put_both, rows, g1_ref, s1_ref)
    acc[...] = jnp.zeros_like(acc)
    pl.semaphore_wait(barrier, 3)

    def piece_both(v, s, r, lo=0, n=CH):
        return h_all.at[v, :, pl.ds(s * side + r * hr, hr), pl.ds(lo, n)]

    def all_both(v, s):
        return h_all.at[v, :, pl.ds(s * side, side), :]

    def piece_stream(v, s, r, lo=0, n=CH):
        return h_all.at[pl.ds((v % ng) * 2, 2), v // ng, pl.ds(s * side + r * hr, hr), pl.ds(lo, n)]

    def all_stream(v, s):
        return h_all.at[pl.ds((v % ng) * 2, 2), v // ng, pl.ds(s * side, side), :]

    def send_own(at, v):
        push(at(v, 0, 0), at(v, 0, 3), ag_send, ag_l.at[v], right).start()
        push(at(v, 0, 0), at(v, 0, 1), ag_send, ag_r.at[v], left).start()
        push(at(v, 0, 0), at(v, 1, 0), ag_send, ag_p.at[v], mate).start()

    def wait_mate(whole, v):
        push(whole(v, 0), whole(v, 1), ag_send, ag_p.at[v], mate).wait_recv()

    def forward_one(at, i):
        with jax.named_scope("gw1l"):
            push(at(i, 0, 0), at(i, 0, 3), ag_send, ag_l.at[i], right).wait_recv()
        push(at(i, 0, 3, 0, hc), at(i, 0, 2, 0, hc), ag_send, ag_l2.at[i], right).start()
        with jax.named_scope("gw1r"):
            push(at(i, 0, 0), at(i, 0, 1), ag_send, ag_r.at[i], left).wait_recv()
        push(at(i, 0, 1, hc, hc), at(i, 0, 2, hc, hc), ag_send, ag_r2.at[i], left).start()
        push(at(i, 0, 3), at(i, 1, 3), ag_send, ag_p.at[i], mate).start()
        push(at(i, 0, 1), at(i, 1, 1), ag_send, ag_p.at[i], mate).start()

    def forward_two(at, j):
        with jax.named_scope("gw2"):
            push(at(j, 0, 3, 0, hc), at(j, 0, 2, 0, hc), ag_send, ag_l2.at[j], right).wait_recv()
            push(at(j, 0, 1, hc, hc), at(j, 0, 2, hc, hc), ag_send, ag_r2.at[j], left).wait_recv()
        push(at(j, 0, 2), at(j, 1, 2), ag_send, ag_p.at[j], mate).start()

    def gather(at, whole, n_use, consume, lags):
        look, lag_b, lag_c = lags

        def step(i, c):
            @pl.when(i < nch)
            def _():
                forward_one(at, i)

            @pl.when(i + look < nch)
            def _():
                send_own(at, i + look)

            @pl.when((i >= lag_b) & (i < nch + lag_b))
            def _():
                forward_two(at, i - lag_b)

            @pl.when(i >= lag_c)
            def _():
                j = i - lag_c
                with jax.named_scope("gwp"):
                    wait_mate(whole, j)
                with jax.named_scope("guse"):
                    consume(j)
            return c

        lax.fori_loop(0, n_use + lag_c, step, 0)

    def gather_drain():
        sent = h_all.at[:, :, pl.ds(0, 7 * hr), :]
        push(sent, sent, ag_send, ag_p.at[0], mate).wait_send()

    tiles = [(t, min(CH, qw - t * CH)) for t in range((qw + CH - 1) // CH)]

    def use_qkv(last):
        @pl.when(last % 2 == 1)
        def _():
            j = last - 1
            for k in (j, last):
                part = u_w.at[k, :, pl.ds(0, qw)]
                pltpu.make_async_copy(part, part, usem.at[k]).wait()
            h = jnp.concatenate([h_all[j].reshape(n_tok, CH), h_all[last].reshape(n_tok, CH)], axis=1)
            for t, n in tiles:
                w = u_w[pl.ds(j, 2), :, t * CH:t * CH + n].reshape(2 * CH, n)
                p = dot(h, w)
                acc[2 * t, :, 0:n] += p[0:st_rows]
                acc[2 * t + 1, :, 0:n] += p[st_rows:]
            load_up(j).start()
            load_up(last).start()

    for v in range(GATHER_QKV[0]):
        send_own(piece_both, v)
    with jax.named_scope("gather1"):
        gather(piece_both, all_both, nch, use_qkv, GATHER_QKV)
    for copy in late:
        copy.wait()
    for s in range(n_slab):
        lo = s * hd
        for st in range(2):
            part = acc[2 * (lo // CH) + st, :, lo % CH:lo % CH + hd]
            qkv[st * st_rows:(st + 1) * st_rows, lo:lo + hd] = bf16(
                part + f32(bqkv_ref[s % heads, s // heads:s // heads + 1, :]))

    def position(i):
        st, s, r, w = i // st_rows, (i // side) % 2, (i // hr) % n_chips, i % hr
        return ((chip + r) % n_chips) * (2 * rows) + (core + s - 2 * core * s) * rows + st * hr + w

    qpos = position(lax.broadcasted_iota(jnp.int32, (n_tok, n_tok), 0))
    kpos = position(lax.broadcasted_iota(jnp.int32, (n_tok, n_tok), 1))
    keep = qpos >= kpos
    for h in range(heads):
        q = qkv[:, h * hd:(h + 1) * hd]
        k = qkv[:, (heads + h) * hd:(heads + h + 1) * hd]
        v = qkv[:, (2 * heads + h) * hd:(2 * heads + h + 1) * hd]
        logits = lax.dot_general(q, k, (((1,), (1,)), ((), ())), preferred_element_type=jnp.float32) * hd ** -0.5
        logits = jnp.where(keep, logits, -1e30)
        e = jnp.exp(logits - jnp.max(logits, axis=1, keepdims=True))
        p = bf16(e / jnp.sum(e, axis=1, keepdims=True))
        ctx[:, h * hd:(h + 1) * hd] = bf16(dot(p, v))

    gather_drain()
    o_all = pool.at[pl.ds(o_base, ng)]
    pltpu.make_async_copy(o_all, o_all, osem).wait()

    def pair_sum(v, st, g):
        for c in range(2):
            j = 2 * g + c
            s = acc[v, c * side:(c + 1) * side, :] + f32(precv[st, j])
            two = bf16(s[2 * hr:3 * hr])
            hop_s[0, st, j] = two[:, 0:hc]
            hop_s[1, st, j] = two[:, hc:]
            acc[v, c * side:(c + 1) * side, :] = s

    def middle_sum(v, st, g):
        for c in range(2):
            j = 2 * g + c
            one = acc[v, c * side + hr:c * side + 2 * hr, :]
            fin_s[0, st, j, :, 0:hc] = bf16(one[:, 0:hc] + f32(hop_r[0, st, j]))
            fin_s[0, st, j, :, hc:] = bf16(one[:, hc:])
            three = acc[v, c * side + 3 * hr:(c + 1) * side, :]
            fin_s[1, st, j, :, 0:hc] = bf16(three[:, 0:hc])
            fin_s[1, st, j, :, hc:] = bf16(three[:, hc:] + f32(hop_r[1, st, j]))

    def fins(st, g, v):
        pair = pl.ds(2 * g, 2)
        return (push(fin_s.at[0, st, pair], fin_r.at[0, st, pair], rs_send, rs_fl.at[v], right),
                push(fin_s.at[1, st, pair], fin_r.at[1, st, pair], rs_send, rs_fr.at[v], left))

    def last_sum(v, st, g, put):
        for copy in fins(st, g, v):
            copy.wait_recv()
        for c in range(2):
            j = 2 * g + c
            total = acc[v, c * side:c * side + hr, :] + f32(fin_r[0, st, j]) + f32(fin_r[1, st, j])
            put(st, j, bf16(xb[st, j] + total))

    def scatter_drain():
        push(psend, precv, rs_send, rs_p.at[0], mate).wait_send()
        push(hop_s, hop_r, rs_send, rs_p.at[0], mate).wait_send()
        push(fin_s, fin_r, rs_send, rs_p.at[0], mate).wait_send()

    bo = f32(bo_ref[...]).reshape(1, dim)
    for j in range(nch):
        cols = slice(j * CH, (j + 1) * CH)
        y = f32(x_ref[:, cols]) + bo[:, cols]
        xb[0, j] = y[0:hr]
        xb[1, j] = y[hr:]

    def pairs_out(g):
        two = pl.ds(2 * g, 2)
        return push(psend.at[:, two], precv.at[:, two], rs_send, rs_p.at[g], mate)

    def hops_out(g):
        two = pl.ds(2 * g, 2)
        return (push(hop_s.at[0, :, two], hop_r.at[0, :, two], rs_send, rs_hl.at[g], right),
                push(hop_s.at[1, :, two], hop_r.at[1, :, two], rs_send, rs_hr.at[g], left))

    def put_x1(st, j, y):
        x1[st, j] = y

    lag_p, lag_h, lag_f = LAGS_OUT

    def out_step(i, carry):
        @pl.when(i < ng)
        def _():
            with jax.named_scope("spart"):
                for c in range(2):
                    j = 2 * i + c
                    p = dot(ctx[...], pool[o_base + i, :, c * CH:(c + 1) * CH])
                    for st in range(2):
                        acc[st * ng + i, c * side:(c + 1) * side, :] = p[st * st_rows:st * st_rows + side]
                        psend[st, j] = bf16(p[st * st_rows + side:(st + 1) * st_rows])
            pairs_out(i).start()

        @pl.when((i >= lag_p) & (i < ng + lag_p))
        def _():
            g = i - lag_p
            with jax.named_scope("swp"):
                pairs_out(g).wait_recv()
            for st in range(2):
                pair_sum(st * ng + g, st, g)
            for copy in hops_out(g):
                copy.start()

        @pl.when((i >= lag_h) & (i < ng + lag_h))
        def _():
            g = i - lag_h
            with jax.named_scope("swh"):
                for copy in hops_out(g):
                    copy.wait_recv()
            for st in range(2):
                middle_sum(st * ng + g, st, g)
            for copy in fins(0, g, g):
                copy.start()

        @pl.when(i == ng + lag_h - 1)
        def _():
            for g in range(ng):
                for copy in fins(1, g, ng + g):
                    copy.start()

        @pl.when(i >= lag_f)
        def _():
            g = i - lag_f
            with jax.named_scope("swf"):
                last_sum(g, 0, g, put_x1)
        return carry

    with jax.named_scope("scatter1"):
        lax.fori_loop(0, ng + lag_f, out_step, 0)

    load_down(N_WD - 1)

    with jax.named_scope("ln2a"):
        norm(lambda j: f32(x1[0, j]), put_stream(0), hr, g2_ref, s2_ref)
    for v in range(GATHER_UP[0]):
        send_own(piece_stream, v)

    def last_out(g, carry):
        last_sum(ng + g, 1, g, put_x1)
        return carry

    with jax.named_scope("last1"):
        lax.fori_loop(0, ng, last_out, 0)
    with jax.named_scope("ln2b"):
        norm(lambda j: f32(x1[1, j]), put_stream(1), hr, g2_ref, s2_ref)
    acc[ng:2 * ng] = jnp.zeros((ng, st_rows, CH), jnp.float32)
    bd = f32(bd_ref[...]).reshape(1, dim)
    for j in range(nch):
        for st in range(2):
            xb[st, j] = f32(x1[st, j]) + bd[:, j * CH:(j + 1) * CH]
    for j in range(nch):
        load_up(j).wait()

    def use_up(v):
        st, g = v // ng, v % ng
        h = jnp.concatenate([h_all[2 * g, st], h_all[2 * g + 1, st]], axis=1)
        for t in range(nt):
            w = u_w[pl.ds(2 * g, 2), :, t * CH:(t + 1) * CH].reshape(2 * CH, CH)
            acc[ng + t] += dot(h, w)

    with jax.named_scope("gather2"):
        gather(piece_stream, all_stream, ng, use_up, GATHER_UP)
    scatter_drain()

    bu = f32(bu_ref[...]).reshape(1, ff)

    def activate(st):
        for t in range(nt):
            cols = slice(t * CH, (t + 1) * CH)
            act[st, :, cols] = bf16(jax.nn.gelu(acc[ng + t] + bu[:, cols], approximate=True))
            acc[ng + t] = jnp.zeros((st_rows, CH), jnp.float32)

    def put_out(st, j, y):
        out_ref[pl.ds(pl.multiple_of(st * hr, hr), hr), pl.ds(pl.multiple_of(j * CH, CH), CH)] = y

    def pairs_down(v, st, g):
        two = pl.ds(2 * g, 2)
        return push(psend.at[st, two], precv.at[st, two], rs_send, rs_p.at[v], mate)

    def hops_down(v, st, g):
        two = pl.ds(2 * g, 2)
        return (push(hop_s.at[0, st, two], hop_r.at[0, st, two], rs_send, rs_hl.at[v], right),
                push(hop_s.at[1, st, two], hop_r.at[1, st, two], rs_send, rs_hr.at[v], left))

    def when_group(k, fn):
        @pl.when(((k >= 0) & (k < ng)) | ((k >= 2 * ng) & (k < 3 * ng)))
        def _():
            st = k // (2 * ng)
            g = k - st * 2 * ng
            fn(st * ng + g, st, g)

    lag_p2, lag_h2, lag_f2 = LAGS_DOWN
    done_two = ng + GATHER_UP[2] - GATHER_UP[1]

    def down_part(v, st, g):
        wait_down(v)
        slot = v % N_WD
        with jax.named_scope("dpart"):
            for c in range(2):
                j = 2 * g + c
                p = dot(act[st], pool[pl.ds(slot * nk, nk), :, c * CH:(c + 1) * CH].reshape(ff, CH))
                acc[v, c * side:(c + 1) * side, :] = p[0:side]
                psend[st, j] = bf16(p[side:])

        @pl.when(v + N_WD < 2 * ng)
        def _():
            load_down(v + N_WD)
        pairs_down(v, st, g).start()

    def down_pair(v, st, g):
        with jax.named_scope("dwp"):
            pairs_down(v, st, g).wait_recv()
        pair_sum(v, st, g)
        for copy in hops_down(v, st, g):
            copy.start()

    def down_middle(v, st, g):
        with jax.named_scope("dwh"):
            for copy in hops_down(v, st, g):
                copy.wait_recv()
        middle_sum(v, st, g)
        for copy in fins(st, g, v):
            copy.start()

    def down_last(v, st, g):
        with jax.named_scope("dwf"):
            last_sum(v, st, g, put_out)

    def mlp_step(w, carry):
        @pl.when((w == 0) | (w == 2 * ng))
        def _():
            with jax.named_scope("gelu"):
                activate(w // (2 * ng))

        when_group(w, down_part)

        @pl.when(w + done_two < nch)
        def _():
            forward_two(piece_stream, w + done_two)

        @pl.when((w >= ng) & (w < 2 * ng))
        def _():
            with jax.named_scope("mwp"):
                wait_mate(all_stream, w)
            with jax.named_scope("muse"):
                use_up(w)

        when_group(w - lag_p2, down_pair)
        when_group(w - lag_h2, down_middle)
        when_group(w - lag_f2, down_last)
        return carry

    with jax.named_scope("mlp"):
        lax.fori_loop(0, 3 * ng + lag_f2, mlp_step, 0)
    scatter_drain()
    gather_drain()


def solution(mesh):
    n_dev = mesh.shape["tp"]

    def body(hidden, g1, s1, w_qkv, b_qkv, w_out, b_out, g2, s2, w_up, b_up, w_down, b_down):
        _, rows, dim = hidden.shape
        _, three, heads, hd = w_qkv.shape
        ff = w_up.shape[1]
        nch = dim // CH
        n_tok, hr = rows * n_dev, rows // 2
        st_rows, side = n_tok // 2, n_tok // 4
        bf, fl = jnp.bfloat16, jnp.float32
        row = lambda v: v.reshape(1, -1)
        hbm = pl.BlockSpec(memory_space=pl.ANY)
        dma = pltpu.SemaphoreType.DMA
        out = pl.pallas_call(
            functools.partial(layer_kernel, n_dev),
            out_shape=pltpu.VMEM((rows, dim), bf),
            in_specs=[hbm] * 13,
            out_specs=pl.BlockSpec(memory_space=pltpu.VMEM),
            scratch_shapes=[
                pltpu.VMEM((rows, dim), bf),
                pltpu.VMEM((1, dim), fl), pltpu.VMEM((1, dim), fl),
                pltpu.VMEM((1, dim), fl), pltpu.VMEM((1, dim), fl),
                pltpu.VMEM((heads, three, hd), bf), pltpu.VMEM((dim,), bf),
                pltpu.VMEM((ff,), bf), pltpu.VMEM((dim,), bf),
                pltpu.VMEM((2, nch, hr, CH), fl),
                pltpu.VMEM((nch, 2, st_rows, CH), bf),
                pltpu.VMEM((nch, CH, ff), bf),
                pltpu.VMEM(((N_WD - 1) * (ff // (heads * hd)) + nch // 2, heads * hd, 2 * CH), bf),
                pltpu.VMEM((nch, st_rows, CH), fl),
                pltpu.VMEM((n_tok, three * heads * hd), bf),
                pltpu.VMEM((n_tok, heads * hd), bf),
                pltpu.VMEM((2, st_rows, ff), bf),
                pltpu.VMEM((2, nch, side, CH), bf),
                pltpu.VMEM((2, nch, side, CH), bf),
                pltpu.VMEM((2, 2, nch, hr, CH // 2), bf),
                pltpu.VMEM((2, 2, nch, hr, CH // 2), bf),
                pltpu.VMEM((2, 2, nch, hr, CH), bf),
                pltpu.VMEM((2, 2, nch, hr, CH), bf),
                pltpu.VMEM((2, nch, hr, CH), bf),
                dma((3,)), dma((6,)), dma((nch,)), dma(()), dma((N_WD,)),
                dma(()), dma((nch,)), dma((nch,)), dma((nch,)), dma((nch,)), dma((nch,)),
                dma(()), dma((nch,)), dma((nch,)), dma((nch,)), dma((nch,)), dma((nch,)),
            ],
            compiler_params=pltpu.CompilerParams(
                collective_id=0, has_side_effects=True, vmem_limit_bytes=61 * 1024 * 1024),
            name="decoder_layer",
        )(
            hidden[0], row(g1), row(s1),
            jnp.transpose(w_qkv, (1, 2, 0, 3)).reshape(three * heads, dim, hd),
            jnp.transpose(b_qkv, (1, 0, 2)),
            w_out.reshape(heads * hd, dim), b_out, row(g2), row(s2), w_up, b_up, w_down, b_down,
        )
        return out[None]

    specs = (P("dp", "tp", None), P(), P(), P(None, None, "tp", None), P(None, "tp", None),
             P("tp", None, None), P(), P(), P(), P(None, "tp"), P("tp"), P("tp", None), P())
    return jax.shard_map(body, mesh=mesh, in_specs=specs, out_specs=P("dp", "tp", None), check_vma=False)
```

```python
import functools

import jax
import jax.numpy as jnp
from jax import lax
from jax.experimental import pallas as pl
from jax.experimental.pallas import tpu as pltpu
from jax.sharding import PartitionSpec as P

LN_EPS = 1e-5
MESH = pl.DeviceIdType.MESH
CH = 512
GATHER_QKV = (5, 4, 5)
GATHER_UP = (5, 4, 5)
LAGS_OUT = (2, 6, 11)
LAGS_DOWN = (2, 6, 10)
N_WD = 4


def f32(v):
    return v.astype(jnp.float32)


def bf16(v):
    return v.astype(jnp.bfloat16)


def dot(a, b):
    return jnp.dot(a, b, preferred_element_type=jnp.float32)


def layer_kernel(
    n_dev,
    x_hbm, g1_hbm, s1_hbm, wqkv, bqkv_hbm, wo, bo_hbm, g2_hbm, s2_hbm, wu, bu_hbm, wd, bd_hbm,
    out_ref,
    x_ref, g1_ref, s1_ref, g2_ref, s2_ref, bqkv_ref, bo_ref, bu_ref, bd_ref,
    xb, h_all, u_w, pool, acc, qkv, ctx, act, psend, precv,
    hop_s, hop_r, fin_s, fin_r, x1,
    xsem, psem, usem, osem, dsem, ag_send, ag_l, ag_r, ag_l2, ag_r2, ag_p,
    rs_send, rs_p, rs_hl, rs_hr, rs_fl, rs_fr,
):
    small = [pltpu.make_async_copy(a, b, xsem.at[i]) for i, (a, b) in enumerate(
        ((x_hbm, x_ref), (g1_hbm, g1_ref), (s1_hbm, s1_ref)))]
    late = [pltpu.make_async_copy(a, b, psem.at[i]) for i, (a, b) in enumerate(
        ((bqkv_hbm, bqkv_ref), (bo_hbm, bo_ref), (g2_hbm, g2_ref), (s2_hbm, s2_ref), (bu_hbm, bu_ref), (bd_hbm, bd_ref)))]
    for copy in small:
        copy.start()
    n_chips = n_dev // 2
    rows, dim = x_ref.shape
    nch = dim // CH
    ng = nch // 2
    hr = rows // 2
    side = hr * n_chips
    st_rows = 2 * side
    n_tok = 2 * st_rows
    hc = CH // 2
    n_slab = wqkv.shape[0]
    hd = wqkv.shape[2]
    heads = n_slab // 3
    qw = n_slab * hd
    ff = wu.shape[1]
    nt = ff // CH
    me = lax.axis_index("tp")
    chip, core = me // 2, me % 2
    right = {"tp": ((chip + 1) % n_chips) * 2 + core}
    left = {"tp": ((chip + n_chips - 1) % n_chips) * 2 + core}
    mate = {"tp": chip * 2 + (1 - core)}

    def push(src, dst, ssem, rsem, dev):
        return pltpu.make_async_remote_copy(
            src_ref=src, dst_ref=dst, send_sem=ssem, recv_sem=rsem, device_id=dev, device_id_type=MESH)

    barrier = pltpu.get_barrier_semaphore()
    for dev in (left, right, mate):
        pl.semaphore_signal(barrier, inc=1, device_id=dev, device_id_type=MESH)

    def load_qkv(j):
        for s in range(n_slab):
            pltpu.make_async_copy(
                wqkv.at[s, pl.ds(pl.multiple_of(j * CH, CH), CH), :],
                u_w.at[j, :, pl.ds(s * hd, hd)], usem.at[j]).start()

    def load_up(j):
        return pltpu.make_async_copy(
            wu.at[pl.ds(pl.multiple_of(j * CH, CH), CH), :], u_w.at[j], usem.at[j])

    kt = heads * hd
    nk = ff // kt
    o_base = (N_WD - 1) * nk

    def load_down(q):
        g, slot = q % ng, q % N_WD
        for k in range(nk):
            pltpu.make_async_copy(
                wd.at[pl.ds(k * kt, kt), pl.ds(pl.multiple_of(g * 2 * CH, 2 * CH), 2 * CH)],
                pool.at[slot * nk + k], dsem.at[slot]).start()

    def wait_down(q):
        slot = q % N_WD
        pltpu.make_async_copy(pool.at[pl.ds(slot * nk, nk)], pool.at[pl.ds(slot * nk, nk)], dsem.at[slot]).wait()

    def init_loads(j, c):
        load_qkv(j)
        return c

    lax.fori_loop(0, nch, init_loads, 0)
    for copy in late:
        copy.start()
    for g in range(ng):
        pltpu.make_async_copy(wo.at[:, pl.ds(g * 2 * CH, 2 * CH)], pool.at[o_base + g], osem).start()
    for q in range(N_WD - 1):
        load_down(q)

    def norm(get, put, n, gain_ref, shift_ref):
        tot = jnp.zeros((n, CH), jnp.float32)
        for j in range(nch):
            tot += get(j)
        mean = jnp.sum(tot, axis=1, keepdims=True) * (1.0 / dim)
        tot = jnp.zeros((n, CH), jnp.float32)
        for j in range(nch):
            cen = get(j) - mean
            tot += cen * cen
        var = jnp.sum(tot, axis=1, keepdims=True) * (1.0 / dim)
        inv = lax.rsqrt(var + LN_EPS)
        for j in range(nch):
            cols = slice(j * CH, (j + 1) * CH)
            put(j, bf16((get(j) - mean) * inv * gain_ref[:, cols] + shift_ref[:, cols]))

    def put_both(j, y):
        h_all[j, 0, 0:hr, :] = y[0:hr]
        h_all[j, 1, 0:hr, :] = y[hr:]

    def put_stream(st):
        def put(j, y):
            h_all[j, st, 0:hr, :] = y
        return put

    for copy in small:
        copy.wait()
    norm(lambda j: f32(x_ref[:, j * CH:(j + 1) * CH]), put_both, rows, g1_ref, s1_ref)
    acc[...] = jnp.zeros_like(acc)
    pl.semaphore_wait(barrier, 3)

    def piece_both(v, s, r, lo=0, n=CH):
        return h_all.at[v, :, pl.ds(s * side + r * hr, hr), pl.ds(lo, n)]

    def all_both(v, s):
        return h_all.at[v, :, pl.ds(s * side, side), :]

    def piece_stream(v, s, r, lo=0, n=CH):
        return h_all.at[pl.ds((v % ng) * 2, 2), v // ng, pl.ds(s * side + r * hr, hr), pl.ds(lo, n)]

    def all_stream(v, s):
        return h_all.at[pl.ds((v % ng) * 2, 2), v // ng, pl.ds(s * side, side), :]

    def send_own(at, v):
        push(at(v, 0, 0), at(v, 0, 3), ag_send, ag_l.at[v], right).start()
        push(at(v, 0, 0), at(v, 0, 1), ag_send, ag_r.at[v], left).start()
        push(at(v, 0, 0), at(v, 1, 0), ag_send, ag_p.at[v], mate).start()

    def wait_mate(whole, v):
        push(whole(v, 0), whole(v, 1), ag_send, ag_p.at[v], mate).wait_recv()

    def forward_one(at, i):
        with jax.named_scope("gw1l"):
            push(at(i, 0, 0), at(i, 0, 3), ag_send, ag_l.at[i], right).wait_recv()
        push(at(i, 0, 3, 0, hc), at(i, 0, 2, 0, hc), ag_send, ag_l2.at[i], right).start()
        with jax.named_scope("gw1r"):
            push(at(i, 0, 0), at(i, 0, 1), ag_send, ag_r.at[i], left).wait_recv()
        push(at(i, 0, 1, hc, hc), at(i, 0, 2, hc, hc), ag_send, ag_r2.at[i], left).start()
        push(at(i, 0, 3), at(i, 1, 3), ag_send, ag_p.at[i], mate).start()
        push(at(i, 0, 1), at(i, 1, 1), ag_send, ag_p.at[i], mate).start()

    def forward_two(at, j):
        with jax.named_scope("gw2"):
            push(at(j, 0, 3, 0, hc), at(j, 0, 2, 0, hc), ag_send, ag_l2.at[j], right).wait_recv()
            push(at(j, 0, 1, hc, hc), at(j, 0, 2, hc, hc), ag_send, ag_r2.at[j], left).wait_recv()
        push(at(j, 0, 2), at(j, 1, 2), ag_send, ag_p.at[j], mate).start()

    def gather(at, whole, n_use, consume, lags):
        look, lag_b, lag_c = lags

        def step(i, c):
            @pl.when(i < nch)
            def _():
                forward_one(at, i)

            @pl.when(i + look < nch)
            def _():
                send_own(at, i + look)

            @pl.when((i >= lag_b) & (i < nch + lag_b))
            def _():
                forward_two(at, i - lag_b)

            @pl.when(i >= lag_c)
            def _():
                j = i - lag_c
                with jax.named_scope("gwp"):
                    wait_mate(whole, j)
                with jax.named_scope("guse"):
                    consume(j)
            return c

        lax.fori_loop(0, n_use + lag_c, step, 0)

    def gather_drain():
        sent = h_all.at[:, :, pl.ds(0, 7 * hr), :]
        push(sent, sent, ag_send, ag_p.at[0], mate).wait_send()

    tiles = [(t, min(CH, qw - t * CH)) for t in range((qw + CH - 1) // CH)]

    def use_qkv(j):
        part = u_w.at[j, :, pl.ds(0, qw)]
        pltpu.make_async_copy(part, part, usem.at[j]).wait()
        h = h_all[j].reshape(n_tok, CH)

        @pl.when(j < nch - 1)
        def _():
            for t, n in tiles:
                p = dot(h, u_w[j, :, t * CH:t * CH + n])
                acc[2 * t, :, 0:n] += p[0:st_rows]
                acc[2 * t + 1, :, 0:n] += p[st_rows:]

        @pl.when(j == nch - 1)
        def _():
            for t, n in tiles:
                p = dot(h, u_w[j, :, t * CH:t * CH + n])
                slabs = range(t * CH // hd, (t * CH + n) // hd)
                b = jnp.concatenate([bqkv_ref[s % heads, s // heads:s // heads + 1, :] for s in slabs], axis=1)
                for st in range(2):
                    y = acc[2 * t + st, :, 0:n] + p[st * st_rows:(st + 1) * st_rows]
                    qkv[st * st_rows:(st + 1) * st_rows, t * CH:t * CH + n] = bf16(y + f32(b))
        load_up(j).start()

    for copy in late:
        copy.wait()
    for v in range(GATHER_QKV[0]):
        send_own(piece_both, v)
    with jax.named_scope("gather1"):
        gather(piece_both, all_both, nch, use_qkv, GATHER_QKV)
    def position(i):
        st, s, r, w = i // st_rows, (i // side) % 2, (i // hr) % n_chips, i % hr
        return ((chip + r) % n_chips) * (2 * rows) + (core + s - 2 * core * s) * rows + st * hr + w

    qpos = position(lax.broadcasted_iota(jnp.int32, (n_tok, n_tok), 0))
    kpos = position(lax.broadcasted_iota(jnp.int32, (n_tok, n_tok), 1))
    keep = qpos >= kpos
    for h in range(heads):
        q = qkv[:, h * hd:(h + 1) * hd]
        k = qkv[:, (heads + h) * hd:(heads + h + 1) * hd]
        v = qkv[:, (2 * heads + h) * hd:(2 * heads + h + 1) * hd]
        logits = lax.dot_general(q, k, (((1,), (1,)), ((), ())), preferred_element_type=jnp.float32) * hd ** -0.5
        logits = jnp.where(keep, logits, -1e30)
        e = jnp.exp(logits - jnp.max(logits, axis=1, keepdims=True))
        p = bf16(e / jnp.sum(e, axis=1, keepdims=True))
        ctx[:, h * hd:(h + 1) * hd] = bf16(dot(p, v))

    gather_drain()
    o_all = pool.at[pl.ds(o_base, ng)]
    pltpu.make_async_copy(o_all, o_all, osem).wait()

    def pair_sum(v, st, g):
        for c in range(2):
            j = 2 * g + c
            s = acc[v, c * side:(c + 1) * side, :] + f32(precv[st, j])
            two = bf16(s[2 * hr:3 * hr])
            hop_s[0, st, j] = two[:, 0:hc]
            hop_s[1, st, j] = two[:, hc:]
            acc[v, c * side:(c + 1) * side, :] = s

    def middle_sum(v, st, g):
        for c in range(2):
            j = 2 * g + c
            one = acc[v, c * side + hr:c * side + 2 * hr, :]
            fin_s[0, st, j, :, 0:hc] = bf16(one[:, 0:hc] + f32(hop_r[0, st, j]))
            fin_s[0, st, j, :, hc:] = bf16(one[:, hc:])
            three = acc[v, c * side + 3 * hr:(c + 1) * side, :]
            fin_s[1, st, j, :, 0:hc] = bf16(three[:, 0:hc])
            fin_s[1, st, j, :, hc:] = bf16(three[:, hc:] + f32(hop_r[1, st, j]))

    def fins(st, g, v):
        pair = pl.ds(2 * g, 2)
        return (push(fin_s.at[0, st, pair], fin_r.at[0, st, pair], rs_send, rs_fl.at[v], right),
                push(fin_s.at[1, st, pair], fin_r.at[1, st, pair], rs_send, rs_fr.at[v], left))

    def last_sum(v, st, g, put):
        for copy in fins(st, g, v):
            copy.wait_recv()
        for c in range(2):
            j = 2 * g + c
            total = acc[v, c * side:c * side + hr, :] + f32(fin_r[0, st, j]) + f32(fin_r[1, st, j])
            put(st, j, bf16(xb[st, j] + total))

    def scatter_drain():
        push(psend, precv, rs_send, rs_p.at[0], mate).wait_send()
        push(hop_s, hop_r, rs_send, rs_p.at[0], mate).wait_send()
        push(fin_s, fin_r, rs_send, rs_p.at[0], mate).wait_send()

    bo = f32(bo_ref[...]).reshape(1, dim)
    for j in range(nch):
        cols = slice(j * CH, (j + 1) * CH)
        y = f32(x_ref[:, cols]) + bo[:, cols]
        xb[0, j] = y[0:hr]
        xb[1, j] = y[hr:]

    def pairs_out(g):
        two = pl.ds(2 * g, 2)
        return push(psend.at[:, two], precv.at[:, two], rs_send, rs_p.at[g], mate)

    def hops_out(g):
        two = pl.ds(2 * g, 2)
        return (push(hop_s.at[0, :, two], hop_r.at[0, :, two], rs_send, rs_hl.at[g], right),
                push(hop_s.at[1, :, two], hop_r.at[1, :, two], rs_send, rs_hr.at[g], left))

    def put_x1(st, j, y):
        x1[st, j] = y

    lag_p, lag_h, lag_f = LAGS_OUT

    def out_step(i, carry):
        @pl.when(i < ng)
        def _():
            with jax.named_scope("spart"):
                for c in range(2):
                    j = 2 * i + c
                    p = dot(ctx[...], pool[o_base + i, :, c * CH:(c + 1) * CH])
                    for st in range(2):
                        acc[st * ng + i, c * side:(c + 1) * side, :] = p[st * st_rows:st * st_rows + side]
                        psend[st, j] = bf16(p[st * st_rows + side:(st + 1) * st_rows])
            pairs_out(i).start()

        @pl.when((i >= lag_p) & (i < ng + lag_p))
        def _():
            g = i - lag_p
            with jax.named_scope("swp"):
                pairs_out(g).wait_recv()
            for st in range(2):
                pair_sum(st * ng + g, st, g)
            for copy in hops_out(g):
                copy.start()

        @pl.when((i >= lag_h) & (i < ng + lag_h))
        def _():
            g = i - lag_h
            with jax.named_scope("swh"):
                for copy in hops_out(g):
                    copy.wait_recv()
            for st in range(2):
                middle_sum(st * ng + g, st, g)
            for copy in fins(0, g, g):
                copy.start()

        @pl.when(i == ng + lag_h - 1)
        def _():
            for g in range(ng):
                for copy in fins(1, g, ng + g):
                    copy.start()

        @pl.when(i >= lag_f)
        def _():
            g = i - lag_f
            with jax.named_scope("swf"):
                last_sum(g, 0, g, put_x1)
        return carry

    with jax.named_scope("scatter1"):
        lax.fori_loop(0, ng + lag_f, out_step, 0)

    load_down(N_WD - 1)

    with jax.named_scope("ln2a"):
        norm(lambda j: f32(x1[0, j]), put_stream(0), hr, g2_ref, s2_ref)
    for v in range(GATHER_UP[0]):
        send_own(piece_stream, v)

    def last_out(g, carry):
        last_sum(ng + g, 1, g, put_x1)
        return carry

    with jax.named_scope("last1"):
        lax.fori_loop(0, ng, last_out, 0)
    with jax.named_scope("ln2b"):
        norm(lambda j: f32(x1[1, j]), put_stream(1), hr, g2_ref, s2_ref)
    acc[ng:2 * ng] = jnp.zeros((ng, st_rows, CH), jnp.float32)
    bd = f32(bd_ref[...]).reshape(1, dim)
    for j in range(nch):
        for st in range(2):
            xb[st, j] = f32(x1[st, j]) + bd[:, j * CH:(j + 1) * CH]
    for j in range(nch):
        load_up(j).wait()

    bu = f32(bu_ref[...]).reshape(1, ff)

    def activate(st, t, a):
        cols = slice(t * CH, (t + 1) * CH)
        act[st, :, cols] = bf16(jax.nn.gelu(a + bu[:, cols], approximate=True))

    def use_up(g):
        h = jnp.concatenate([h_all[2 * g, 0], h_all[2 * g + 1, 0]], axis=1)

        def weight(t):
            return u_w[pl.ds(2 * g, 2), :, t * CH:(t + 1) * CH].reshape(2 * CH, CH)

        @pl.when(g < ng - 1)
        def _():
            for t in range(nt):
                acc[ng + t] += dot(h, weight(t))

        @pl.when(g == ng - 1)
        def _():
            for t in range(nt):
                activate(0, t, acc[ng + t] + dot(h, weight(t)))

    def up_whole():
        for g in range(ng):
            wait_mate(all_stream, ng + g)
        with jax.named_scope("muse"):
            h = jnp.concatenate([h_all[j, 1] for j in range(nch)], axis=1)
            for t in range(nt):
                activate(1, t, dot(h, u_w[:, :, t * CH:(t + 1) * CH].reshape(dim, CH)))

    with jax.named_scope("gather2"):
        gather(piece_stream, all_stream, ng, use_up, GATHER_UP)
    scatter_drain()

    def put_out(st, j, y):
        out_ref[pl.ds(pl.multiple_of(st * hr, hr), hr), pl.ds(pl.multiple_of(j * CH, CH), CH)] = y

    def pairs_down(v, st, g):
        two = pl.ds(2 * g, 2)
        return push(psend.at[st, two], precv.at[st, two], rs_send, rs_p.at[v], mate)

    def hops_down(v, st, g):
        two = pl.ds(2 * g, 2)
        return (push(hop_s.at[0, st, two], hop_r.at[0, st, two], rs_send, rs_hl.at[v], right),
                push(hop_s.at[1, st, two], hop_r.at[1, st, two], rs_send, rs_hr.at[v], left))

    def when_group(k, fn):
        @pl.when((k >= 0) & (k <= 2 * ng) & (k != ng))
        def _():
            st = k // (ng + 1)
            v = k - st
            fn(v, st, v - st * ng)

    lag_p2, lag_h2, lag_f2 = LAGS_DOWN
    done_two = ng + GATHER_UP[2] - GATHER_UP[1]

    def down_part(v, st, g):
        wait_down(v)
        slot = v % N_WD
        with jax.named_scope("dpart"):
            for c in range(2):
                j = 2 * g + c
                p = dot(act[st], pool[pl.ds(slot * nk, nk), :, c * CH:(c + 1) * CH].reshape(ff, CH))
                acc[v, c * side:(c + 1) * side, :] = p[0:side]
                psend[st, j] = bf16(p[side:])

        @pl.when(v + N_WD < 2 * ng)
        def _():
            load_down(v + N_WD)
        pairs_down(v, st, g).start()

    def down_pair(v, st, g):
        with jax.named_scope("dwp"):
            pairs_down(v, st, g).wait_recv()
        pair_sum(v, st, g)
        for copy in hops_down(v, st, g):
            copy.start()

    def down_middle(v, st, g):
        with jax.named_scope("dwh"):
            for copy in hops_down(v, st, g):
                copy.wait_recv()
        middle_sum(v, st, g)
        for copy in fins(st, g, v):
            copy.start()

    def down_last(v, st, g):
        with jax.named_scope("dwf"):
            last_sum(v, st, g, put_out)

    def mlp_step(w, carry):
        when_group(w - lag_p2, down_pair)
        when_group(w - lag_h2, down_middle)
        when_group(w - lag_f2, down_last)

        @pl.when(w + done_two < nch)
        def _():
            forward_two(piece_stream, w + done_two)

        pl.when(w == ng)(up_whole)
        when_group(w, down_part)
        return carry

    with jax.named_scope("mlp"):
        lax.fori_loop(0, 2 * ng + 1 + lag_f2, mlp_step, 0)
    scatter_drain()
    gather_drain()


def solution(mesh):
    n_dev = mesh.shape["tp"]

    def body(hidden, g1, s1, w_qkv, b_qkv, w_out, b_out, g2, s2, w_up, b_up, w_down, b_down):
        _, rows, dim = hidden.shape
        _, three, heads, hd = w_qkv.shape
        ff = w_up.shape[1]
        nch = dim // CH
        n_tok, hr = rows * n_dev, rows // 2
        st_rows, side = n_tok // 2, n_tok // 4
        bf, fl = jnp.bfloat16, jnp.float32
        row = lambda v: v.reshape(1, -1)
        hbm = pl.BlockSpec(memory_space=pl.ANY)
        dma = pltpu.SemaphoreType.DMA
        out = pl.pallas_call(
            functools.partial(layer_kernel, n_dev),
            out_shape=pltpu.VMEM((rows, dim), bf),
            in_specs=[hbm] * 13,
            out_specs=pl.BlockSpec(memory_space=pltpu.VMEM),
            scratch_shapes=[
                pltpu.VMEM((rows, dim), bf),
                pltpu.VMEM((1, dim), fl), pltpu.VMEM((1, dim), fl),
                pltpu.VMEM((1, dim), fl), pltpu.VMEM((1, dim), fl),
                pltpu.VMEM((heads, three, hd), bf), pltpu.VMEM((dim,), bf),
                pltpu.VMEM((ff,), bf), pltpu.VMEM((dim,), bf),
                pltpu.VMEM((2, nch, hr, CH), fl),
                pltpu.VMEM((nch, 2, st_rows, CH), bf),
                pltpu.VMEM((nch, CH, ff), bf),
                pltpu.VMEM(((N_WD - 1) * (ff // (heads * hd)) + nch // 2, heads * hd, 2 * CH), bf),
                pltpu.VMEM((nch, st_rows, CH), fl),
                pltpu.VMEM((n_tok, three * heads * hd), bf),
                pltpu.VMEM((n_tok, heads * hd), bf),
                pltpu.VMEM((2, st_rows, ff), bf),
                pltpu.VMEM((2, nch, side, CH), bf),
                pltpu.VMEM((2, nch, side, CH), bf),
                pltpu.VMEM((2, 2, nch, hr, CH // 2), bf),
                pltpu.VMEM((2, 2, nch, hr, CH // 2), bf),
                pltpu.VMEM((2, 2, nch, hr, CH), bf),
                pltpu.VMEM((2, 2, nch, hr, CH), bf),
                pltpu.VMEM((2, nch, hr, CH), bf),
                dma((3,)), dma((6,)), dma((nch,)), dma(()), dma((N_WD,)),
                dma(()), dma((nch,)), dma((nch,)), dma((nch,)), dma((nch,)), dma((nch,)),
                dma(()), dma((nch,)), dma((nch,)), dma((nch,)), dma((nch,)), dma((nch,)),
            ],
            compiler_params=pltpu.CompilerParams(
                collective_id=0, has_side_effects=True, vmem_limit_bytes=61 * 1024 * 1024),
            name="decoder_layer",
        )(
            hidden[0], row(g1), row(s1),
            jnp.transpose(w_qkv, (1, 2, 0, 3)).reshape(three * heads, dim, hd),
            jnp.transpose(b_qkv, (1, 0, 2)),
            w_out.reshape(heads * hd, dim), b_out, row(g2), row(s2), w_up, b_up, w_down, b_down,
        )
        return out[None]

    specs = (P("dp", "tp", None), P(), P(), P(None, None, "tp", None), P(None, "tp", None),
             P("tp", None, None), P(), P(), P(), P(None, "tp"), P("tp"), P("tp", None), P())
    return jax.shard_map(body, mesh=mesh, in_specs=specs, out_specs=P("dp", "tp", None), check_vma=False)
```

```python
import functools

import jax
import jax.numpy as jnp
from jax import lax
from jax.experimental import pallas as pl
from jax.experimental.pallas import tpu as pltpu
from jax.sharding import PartitionSpec as P

LN_EPS = 1e-5
MESH = pl.DeviceIdType.MESH
CH = 512
GATHER_QKV = (5, 4, 5)
GATHER_UP = (5, 4, 5)
LAGS_OUT = (2, 6, 11)
LAGS_DOWN = (2, 6, 10)
N_FAR = 2
N_WD = 4


def f32(v):
    return v.astype(jnp.float32)


def bf16(v):
    return v.astype(jnp.bfloat16)


def dot(a, b):
    return jnp.dot(a, b, preferred_element_type=jnp.float32)


def layer_kernel(
    n_dev,
    x_hbm, g1_hbm, s1_hbm, wqkv, bqkv_hbm, wo, bo_hbm, g2_hbm, s2_hbm, wu, bu_hbm, wd, bd_hbm,
    out_ref,
    x_ref, g1_ref, s1_ref, g2_ref, s2_ref, bqkv_ref, bo_ref, bu_ref, bd_ref,
    xb, h_all, u_w, pool, acc, qkv, ctx, act, psend, precv,
    hop_s, hop_r, fin_s, fin_r, x1,
    xsem, psem, usem, osem, dsem, ag_send, ag_l, ag_r, ag_l2, ag_r2, ag_p,
    rs_send, rs_p, rs_hl, rs_hr, rs_fl, rs_fr,
):
    small = [pltpu.make_async_copy(a, b, xsem.at[i]) for i, (a, b) in enumerate(
        ((x_hbm, x_ref), (g1_hbm, g1_ref), (s1_hbm, s1_ref)))]
    late = [pltpu.make_async_copy(a, b, psem.at[i]) for i, (a, b) in enumerate(
        ((bqkv_hbm, bqkv_ref), (bo_hbm, bo_ref), (g2_hbm, g2_ref), (s2_hbm, s2_ref), (bu_hbm, bu_ref), (bd_hbm, bd_ref)))]
    for copy in small + late:
        copy.start()
    n_chips = n_dev // 2
    rows, dim = x_ref.shape
    nch = dim // CH
    ng = nch // 2
    hr = rows // 2
    side = hr * n_chips
    st_rows = 2 * side
    n_tok = 2 * st_rows
    hc = CH // 2
    n_slab = wqkv.shape[0]
    hd = wqkv.shape[2]
    heads = n_slab // 3
    qw = n_slab * hd
    ff = wu.shape[1]
    nt = ff // CH
    me = lax.axis_index("tp")
    chip, core = me // 2, me % 2
    right = {"tp": ((chip + 1) % n_chips) * 2 + core}
    left = {"tp": ((chip + n_chips - 1) % n_chips) * 2 + core}
    mate = {"tp": chip * 2 + (1 - core)}
    far = {"tp": ((chip + 2) % n_chips) * 2 + core}

    def push(src, dst, ssem, rsem, dev):
        return pltpu.make_async_remote_copy(
            src_ref=src, dst_ref=dst, send_sem=ssem, recv_sem=rsem, device_id=dev, device_id_type=MESH)

    barrier = pltpu.get_barrier_semaphore()
    for dev in (left, right, mate, far):
        pl.semaphore_signal(barrier, inc=1, device_id=dev, device_id_type=MESH)

    def load_qkv(j):
        for s in range(n_slab):
            pltpu.make_async_copy(
                wqkv.at[s, pl.ds(pl.multiple_of(j * CH, CH), CH), :],
                u_w.at[j, :, pl.ds(s * hd, hd)], usem.at[j]).start()

    def load_up(j):
        return pltpu.make_async_copy(
            wu.at[pl.ds(pl.multiple_of(j * CH, CH), CH), :], u_w.at[j], usem.at[j])

    kt = heads * hd
    nk = ff // kt
    o_base = (N_WD - 1) * nk

    def load_down(q):
        g, slot = q % ng, q % N_WD
        for k in range(nk):
            pltpu.make_async_copy(
                wd.at[pl.ds(k * kt, kt), pl.ds(pl.multiple_of(g * 2 * CH, 2 * CH), 2 * CH)],
                pool.at[slot * nk + k], dsem.at[slot]).start()

    def wait_down(q):
        slot = q % N_WD
        pltpu.make_async_copy(pool.at[pl.ds(slot * nk, nk)], pool.at[pl.ds(slot * nk, nk)], dsem.at[slot]).wait()

    def init_loads(j, c):
        load_qkv(j)
        return c

    lax.fori_loop(0, nch, init_loads, 0)
    for g in range(ng):
        pltpu.make_async_copy(wo.at[:, pl.ds(g * 2 * CH, 2 * CH)], pool.at[o_base + g], osem).start()
    for q in range(N_WD - 1):
        load_down(q)

    def norm(get, put, n, gain_ref, shift_ref):
        tot = jnp.zeros((n, CH), jnp.float32)
        for j in range(nch):
            tot += get(j)
        mean = jnp.sum(tot, axis=1, keepdims=True) * (1.0 / dim)
        tot = jnp.zeros((n, CH), jnp.float32)
        for j in range(nch):
            cen = get(j) - mean
            tot += cen * cen
        var = jnp.sum(tot, axis=1, keepdims=True) * (1.0 / dim)
        inv = lax.rsqrt(var + LN_EPS)
        for j in range(nch):
            cols = slice(j * CH, (j + 1) * CH)
            put(j, bf16((get(j) - mean) * inv * gain_ref[:, cols] + shift_ref[:, cols]))

    def put_both(j, y):
        h_all[j, 0, 0:hr, :] = y[0:hr]
        h_all[j, 1, 0:hr, :] = y[hr:]

    def put_stream(st):
        def put(j, y):
            h_all[j, st, 0:hr, :] = y
        return put

    for copy in small:
        copy.wait()
    norm(lambda j: f32(x_ref[:, j * CH:(j + 1) * CH]), put_both, rows, g1_ref, s1_ref)
    acc[...] = jnp.zeros_like(acc)
    pl.semaphore_wait(barrier, 4)

    def piece_both(v, s, r, lo=0, n=CH):
        return h_all.at[v, :, pl.ds(s * side + r * hr, hr), pl.ds(lo, n)]

    def all_both(v, s):
        return h_all.at[v, :, pl.ds(s * side, side), :]

    def piece_stream(v, s, r, lo=0, n=CH):
        return h_all.at[pl.ds((v % ng) * 2, 2), v // ng, pl.ds(s * side + r * hr, hr), pl.ds(lo, n)]

    def all_stream(v, s):
        return h_all.at[pl.ds((v % ng) * 2, 2), v // ng, pl.ds(s * side, side), :]

    def send_own(at, v):
        push(at(v, 0, 0), at(v, 0, 3), ag_send, ag_l.at[v], right).start()
        push(at(v, 0, 0), at(v, 0, 1), ag_send, ag_r.at[v], left).start()
        push(at(v, 0, 0), at(v, 1, 0), ag_send, ag_p.at[v], mate).start()

    def wait_mate(whole, v):
        push(whole(v, 0), whole(v, 1), ag_send, ag_p.at[v], mate).wait_recv()

    def forward_one(at, i):
        with jax.named_scope("gw1l"):
            push(at(i, 0, 0), at(i, 0, 3), ag_send, ag_l.at[i], right).wait_recv()
        push(at(i, 0, 3, 0, hc), at(i, 0, 2, 0, hc), ag_send, ag_l2.at[i], right).start()
        with jax.named_scope("gw1r"):
            push(at(i, 0, 0), at(i, 0, 1), ag_send, ag_r.at[i], left).wait_recv()
        push(at(i, 0, 1, hc, hc), at(i, 0, 2, hc, hc), ag_send, ag_r2.at[i], left).start()
        push(at(i, 0, 3), at(i, 1, 3), ag_send, ag_p.at[i], mate).start()
        push(at(i, 0, 1), at(i, 1, 1), ag_send, ag_p.at[i], mate).start()

    def forward_two(at, j):
        with jax.named_scope("gw2"):
            push(at(j, 0, 3, 0, hc), at(j, 0, 2, 0, hc), ag_send, ag_l2.at[j], right).wait_recv()
            push(at(j, 0, 1, hc, hc), at(j, 0, 2, hc, hc), ag_send, ag_r2.at[j], left).wait_recv()
        push(at(j, 0, 2), at(j, 1, 2), ag_send, ag_p.at[j], mate).start()

    def gather(at, whole, n_use, consume, lags):
        look, lag_b, lag_c = lags

        def step(i, c):
            @pl.when(i < nch)
            def _():
                forward_one(at, i)

            @pl.when(i + look < nch)
            def _():
                send_own(at, i + look)

            @pl.when((i >= lag_b) & (i < nch + lag_b))
            def _():
                forward_two(at, i - lag_b)

            @pl.when(i >= lag_c)
            def _():
                j = i - lag_c
                with jax.named_scope("gwp"):
                    wait_mate(whole, j)
                with jax.named_scope("guse"):
                    consume(j)
            return c

        lax.fori_loop(0, n_use + lag_c, step, 0)

    def gather_drain():
        sent = h_all.at[:, :, pl.ds(0, 7 * hr), :]
        push(sent, sent, ag_send, ag_p.at[0], mate).wait_send()

    tiles = [(t, min(CH, qw - t * CH)) for t in range((qw + CH - 1) // CH)]

    def use_qkv(j):
        part = u_w.at[j, :, pl.ds(0, qw)]
        pltpu.make_async_copy(part, part, usem.at[j]).wait()
        h = h_all[j].reshape(n_tok, CH)

        @pl.when(j < nch - 1)
        def _():
            for t, n in tiles:
                p = dot(h, u_w[j, :, t * CH:t * CH + n])
                acc[2 * t, :, 0:n] += p[0:st_rows]
                acc[2 * t + 1, :, 0:n] += p[st_rows:]

        @pl.when(j == nch - 1)
        def _():
            for t, n in tiles:
                p = dot(h, u_w[j, :, t * CH:t * CH + n])
                slabs = range(t * CH // hd, (t * CH + n) // hd)
                b = jnp.concatenate([bqkv_ref[s % heads, s // heads:s // heads + 1, :] for s in slabs], axis=1)
                for st in range(2):
                    y = acc[2 * t + st, :, 0:n] + p[st * st_rows:(st + 1) * st_rows]
                    qkv[st * st_rows:(st + 1) * st_rows, t * CH:t * CH + n] = bf16(y + f32(b))
        load_up(j).start()

    for copy in late:
        copy.wait()
    for v in range(GATHER_QKV[0]):
        send_own(piece_both, v)
    with jax.named_scope("gather1"):
        gather(piece_both, all_both, nch, use_qkv, GATHER_QKV)
    def position(i):
        st, s, r, w = i // st_rows, (i // side) % 2, (i // hr) % n_chips, i % hr
        return ((chip + r) % n_chips) * (2 * rows) + (core + s - 2 * core * s) * rows + st * hr + w

    qpos = position(lax.broadcasted_iota(jnp.int32, (n_tok, n_tok), 0))
    kpos = position(lax.broadcasted_iota(jnp.int32, (n_tok, n_tok), 1))
    keep = qpos >= kpos
    for h in range(heads):
        q = qkv[:, h * hd:(h + 1) * hd]
        k = qkv[:, (heads + h) * hd:(heads + h + 1) * hd]
        v = qkv[:, (2 * heads + h) * hd:(2 * heads + h + 1) * hd]
        logits = lax.dot_general(q, k, (((1,), (1,)), ((), ())), preferred_element_type=jnp.float32) * hd ** -0.5
        logits = jnp.where(keep, logits, -1e30)
        e = jnp.exp(logits - jnp.max(logits, axis=1, keepdims=True))
        p = bf16(e / jnp.sum(e, axis=1, keepdims=True))
        ctx[:, h * hd:(h + 1) * hd] = bf16(dot(p, v))

    gather_drain()
    o_all = pool.at[pl.ds(o_base, ng)]
    pltpu.make_async_copy(o_all, o_all, osem).wait()

    def pair_sum(v, st, g):
        for c in range(2):
            j = 2 * g + c
            s = acc[v, c * side:(c + 1) * side, :] + f32(precv[st, j])
            two = bf16(s[2 * hr:3 * hr])
            hop_s[0, st, j] = two[:, 0:hc]
            hop_s[1, st, j] = two[:, hc:]
            acc[v, c * side:(c + 1) * side, :] = s

    def middle_sum(v, st, g):
        for c in range(2):
            j = 2 * g + c
            one = acc[v, c * side + hr:c * side + 2 * hr, :]
            fin_s[0, st, j, :, 0:hc] = bf16(one[:, 0:hc] + f32(hop_r[0, st, j]))
            fin_s[0, st, j, :, hc:] = bf16(one[:, hc:])
            three = acc[v, c * side + 3 * hr:(c + 1) * side, :]
            fin_s[1, st, j, :, 0:hc] = bf16(three[:, 0:hc])
            fin_s[1, st, j, :, hc:] = bf16(three[:, hc:] + f32(hop_r[1, st, j]))

    def fins(st, g, v):
        pair = pl.ds(2 * g, 2)
        return (push(fin_s.at[0, st, pair], fin_r.at[0, st, pair], rs_send, rs_fl.at[v], right),
                push(fin_s.at[1, st, pair], fin_r.at[1, st, pair], rs_send, rs_fr.at[v], left))

    def last_sum(v, st, g, put):
        for copy in fins(st, g, v):
            copy.wait_recv()
        for c in range(2):
            j = 2 * g + c
            total = acc[v, c * side:c * side + hr, :] + f32(fin_r[0, st, j]) + f32(fin_r[1, st, j])
            put(st, j, bf16(xb[st, j] + total))

    def scatter_drain():
        push(psend, precv, rs_send, rs_p.at[0], mate).wait_send()
        push(hop_s, hop_r, rs_send, rs_p.at[0], mate).wait_send()
        push(fin_s, fin_r, rs_send, rs_p.at[0], mate).wait_send()

    bo = f32(bo_ref[...]).reshape(1, dim)
    for j in range(nch):
        cols = slice(j * CH, (j + 1) * CH)
        y = f32(x_ref[:, cols]) + bo[:, cols]
        xb[0, j] = y[0:hr]
        xb[1, j] = y[hr:]

    def pairs_out(g):
        two = pl.ds(2 * g, 2)
        return push(psend.at[:, two], precv.at[:, two], rs_send, rs_p.at[g], mate)

    def hops_out(g):
        two = pl.ds(2 * g, 2)
        return (push(hop_s.at[0, :, two], hop_r.at[0, :, two], rs_send, rs_hl.at[g], right),
                push(hop_s.at[1, :, two], hop_r.at[1, :, two], rs_send, rs_hr.at[g], left))

    def put_x1(st, j, y):
        x1[st, j] = y

    lag_p, lag_h, lag_f = LAGS_OUT

    def out_step(i, carry):
        @pl.when(i < ng)
        def _():
            with jax.named_scope("spart"):
                for c in range(2):
                    j = 2 * i + c
                    p = dot(ctx[...], pool[o_base + i, :, c * CH:(c + 1) * CH])
                    for st in range(2):
                        acc[st * ng + i, c * side:(c + 1) * side, :] = p[st * st_rows:st * st_rows + side]
                        psend[st, j] = bf16(p[st * st_rows + side:(st + 1) * st_rows])
            pairs_out(i).start()

        @pl.when((i >= lag_p) & (i < ng + lag_p))
        def _():
            g = i - lag_p
            with jax.named_scope("swp"):
                pairs_out(g).wait_recv()
            for st in range(2):
                pair_sum(st * ng + g, st, g)
            for copy in hops_out(g):
                copy.start()

        @pl.when((i >= lag_h) & (i < ng + lag_h))
        def _():
            g = i - lag_h
            with jax.named_scope("swh"):
                for copy in hops_out(g):
                    copy.wait_recv()
            for st in range(2):
                middle_sum(st * ng + g, st, g)
            for copy in fins(0, g, g):
                copy.start()

        @pl.when(i == ng + lag_h - 1)
        def _():
            for g in range(ng):
                for copy in fins(1, g, ng + g):
                    copy.start()

        @pl.when(i >= lag_f)
        def _():
            g = i - lag_f
            with jax.named_scope("swf"):
                last_sum(g, 0, g, put_x1)
        return carry

    with jax.named_scope("scatter1"):
        lax.fori_loop(0, ng + lag_f, out_step, 0)

    load_down(N_WD - 1)

    with jax.named_scope("ln2a"):
        norm(lambda j: f32(x1[0, j]), put_stream(0), hr, g2_ref, s2_ref)
    for v in range(GATHER_UP[0]):
        send_own(piece_stream, v)

    def last_out(g, carry):
        last_sum(ng + g, 1, g, put_x1)
        return carry

    with jax.named_scope("last1"):
        lax.fori_loop(0, ng, last_out, 0)
    with jax.named_scope("ln2b"):
        norm(lambda j: f32(x1[1, j]), put_stream(1), hr, g2_ref, s2_ref)
    acc[ng:2 * ng] = jnp.zeros((ng, st_rows, CH), jnp.float32)
    bd = f32(bd_ref[...]).reshape(1, dim)
    for j in range(nch):
        for st in range(2):
            xb[st, j] = f32(x1[st, j]) + bd[:, j * CH:(j + 1) * CH]
    for j in range(nch):
        load_up(j).wait()

    bu = f32(bu_ref[...]).reshape(1, ff)

    def activate(st, t, a):
        cols = slice(t * CH, (t + 1) * CH)
        act[st, :, cols] = bf16(jax.nn.gelu(a + bu[:, cols], approximate=True))

    def use_up(g):
        h = jnp.concatenate([h_all[2 * g, 0], h_all[2 * g + 1, 0]], axis=1)

        def weight(t):
            return u_w[pl.ds(2 * g, 2), :, t * CH:(t + 1) * CH].reshape(2 * CH, CH)

        @pl.when(g < ng - 1)
        def _():
            for t in range(nt):
                acc[ng + t] += dot(h, weight(t))

        @pl.when(g == ng - 1)
        def _():
            for t in range(nt):
                activate(0, t, acc[ng + t] + dot(h, weight(t)))

    def up_whole():
        for g in range(ng):
            wait_mate(all_stream, ng + g)
        with jax.named_scope("muse"):
            h = jnp.concatenate([h_all[j, 1] for j in range(nch)], axis=1)
            for t in range(nt):
                activate(1, t, dot(h, u_w[:, :, t * CH:(t + 1) * CH].reshape(dim, CH)))

    with jax.named_scope("gather2"):
        gather(piece_stream, all_stream, ng, use_up, GATHER_UP)
    scatter_drain()

    def put_out(st, j, y):
        out_ref[pl.ds(pl.multiple_of(st * hr, hr), hr), pl.ds(pl.multiple_of(j * CH, CH), CH)] = y

    def pairs_down(v, st, g):
        two = pl.ds(2 * g, 2)
        return push(psend.at[st, two], precv.at[st, two], rs_send, rs_p.at[v], mate)

    def hops_down(v, st, g):
        two = pl.ds(2 * g, 2)
        return (push(hop_s.at[0, st, two], hop_r.at[0, st, two], rs_send, rs_hl.at[v], right),
                push(hop_s.at[1, st, two], hop_r.at[1, st, two], rs_send, rs_hr.at[v], left))

    def far_down(v, st, g):
        two = pl.ds(2 * g, 2)
        return push(hop_s.at[:, st, two], hop_r.at[:, st, two], rs_send, rs_hl.at[v], far)

    first_far = 2 * ng - N_FAR

    def when_group(k, fn):
        @pl.when((k >= 0) & (k <= 2 * ng) & (k != ng))
        def _():
            st = k // (ng + 1)
            v = k - st
            fn(v, st, v - st * ng)

    lag_p2, lag_h2, lag_f2 = LAGS_DOWN
    done_two = ng + GATHER_UP[2] - GATHER_UP[1]

    def down_part(v, st, g):
        wait_down(v)
        slot = v % N_WD
        with jax.named_scope("dpart"):
            for c in range(2):
                j = 2 * g + c
                p = dot(act[st], pool[pl.ds(slot * nk, nk), :, c * CH:(c + 1) * CH].reshape(ff, CH))
                acc[v, c * side:(c + 1) * side, :] = p[0:side]
                psend[st, j] = bf16(p[side:])

        @pl.when(v + N_WD < 2 * ng)
        def _():
            load_down(v + N_WD)
        pairs_down(v, st, g).start()

    def down_pair(v, st, g):
        with jax.named_scope("dwp"):
            pairs_down(v, st, g).wait_recv()
        pair_sum(v, st, g)

        @pl.when(v < first_far)
        def _():
            for copy in hops_down(v, st, g):
                copy.start()

        @pl.when(v >= first_far)
        def _():
            far_down(v, st, g).start()
            for c in range(2):
                j = 2 * g + c
                fin_s[0, st, j] = bf16(acc[v, c * side + hr:c * side + 2 * hr, :])
                fin_s[1, st, j] = bf16(acc[v, c * side + 3 * hr:(c + 1) * side, :])
            for copy in fins(st, g, v):
                copy.start()

    def down_middle(v, st, g):
        @pl.when(v < first_far)
        def _():
            with jax.named_scope("dwh"):
                for copy in hops_down(v, st, g):
                    copy.wait_recv()
            middle_sum(v, st, g)
            for copy in fins(st, g, v):
                copy.start()

    def down_last(v, st, g):
        @pl.when(v < first_far)
        def _():
            with jax.named_scope("dwf"):
                last_sum(v, st, g, put_out)

        @pl.when(v >= first_far)
        def _():
            with jax.named_scope("dwx"):
                far_down(v, st, g).wait_recv()
                for c in range(2):
                    j = 2 * g + c
                    acc[v, c * side:c * side + hr, 0:hc] += f32(hop_r[0, st, j])
                    acc[v, c * side:c * side + hr, hc:] += f32(hop_r[1, st, j])
                last_sum(v, st, g, put_out)

    def mlp_step(w, carry):
        when_group(w - lag_p2, down_pair)
        when_group(w - lag_h2, down_middle)
        when_group(w - lag_f2, down_last)

        @pl.when(w + done_two < nch)
        def _():
            forward_two(piece_stream, w + done_two)

        pl.when(w == ng)(up_whole)
        when_group(w, down_part)
        return carry

    with jax.named_scope("mlp"):
        lax.fori_loop(0, 2 * ng + 1 + lag_f2, mlp_step, 0)
    scatter_drain()
    gather_drain()


def solution(mesh):
    n_dev = mesh.shape["tp"]

    def body(hidden, g1, s1, w_qkv, b_qkv, w_out, b_out, g2, s2, w_up, b_up, w_down, b_down):
        _, rows, dim = hidden.shape
        _, three, heads, hd = w_qkv.shape
        ff = w_up.shape[1]
        nch = dim // CH
        n_tok, hr = rows * n_dev, rows // 2
        st_rows, side = n_tok // 2, n_tok // 4
        bf, fl = jnp.bfloat16, jnp.float32
        row = lambda v: v.reshape(1, -1)
        hbm = pl.BlockSpec(memory_space=pl.ANY)
        dma = pltpu.SemaphoreType.DMA
        out = pl.pallas_call(
            functools.partial(layer_kernel, n_dev),
            out_shape=pltpu.VMEM((rows, dim), bf),
            in_specs=[hbm] * 13,
            out_specs=pl.BlockSpec(memory_space=pltpu.VMEM),
            scratch_shapes=[
                pltpu.VMEM((rows, dim), bf),
                pltpu.VMEM((1, dim), fl), pltpu.VMEM((1, dim), fl),
                pltpu.VMEM((1, dim), fl), pltpu.VMEM((1, dim), fl),
                pltpu.VMEM((heads, three, hd), bf), pltpu.VMEM((dim,), bf),
                pltpu.VMEM((ff,), bf), pltpu.VMEM((dim,), bf),
                pltpu.VMEM((2, nch, hr, CH), fl),
                pltpu.VMEM((nch, 2, st_rows, CH), bf),
                pltpu.VMEM((nch, CH, ff), bf),
                pltpu.VMEM(((N_WD - 1) * (ff // (heads * hd)) + nch // 2, heads * hd, 2 * CH), bf),
                pltpu.VMEM((nch, st_rows, CH), fl),
                pltpu.VMEM((n_tok, three * heads * hd), bf),
                pltpu.VMEM((n_tok, heads * hd), bf),
                pltpu.VMEM((2, st_rows, ff), bf),
                pltpu.VMEM((2, nch, side, CH), bf),
                pltpu.VMEM((2, nch, side, CH), bf),
                pltpu.VMEM((2, 2, nch, hr, CH // 2), bf),
                pltpu.VMEM((2, 2, nch, hr, CH // 2), bf),
                pltpu.VMEM((2, 2, nch, hr, CH), bf),
                pltpu.VMEM((2, 2, nch, hr, CH), bf),
                pltpu.VMEM((2, nch, hr, CH), bf),
                dma((3,)), dma((6,)), dma((nch,)), dma(()), dma((N_WD,)),
                dma(()), dma((nch,)), dma((nch,)), dma((nch,)), dma((nch,)), dma((nch,)),
                dma(()), dma((nch,)), dma((nch,)), dma((nch,)), dma((nch,)), dma((nch,)),
            ],
            compiler_params=pltpu.CompilerParams(
                collective_id=0, has_side_effects=True, vmem_limit_bytes=61 * 1024 * 1024),
            name="decoder_layer",
        )(
            hidden[0], row(g1), row(s1),
            jnp.transpose(w_qkv, (1, 2, 0, 3)).reshape(three * heads, dim, hd),
            jnp.transpose(b_qkv, (1, 0, 2)),
            w_out.reshape(heads * hd, dim), b_out, row(g2), row(s2), w_up, b_up, w_down, b_down,
        )
        return out[None]

    specs = (P("dp", "tp", None), P(), P(), P(None, None, "tp", None), P(None, "tp", None),
             P("tp", None, None), P(), P(), P(), P(None, "tp"), P("tp"), P("tp", None), P())
    return jax.shard_map(body, mesh=mesh, in_specs=specs, out_specs=P("dp", "tp", None), check_vma=False)
```

```python
import functools

import jax
import jax.numpy as jnp
from jax import lax
from jax.experimental import pallas as pl
from jax.experimental.pallas import tpu as pltpu
from jax.sharding import PartitionSpec as P

LN_EPS = 1e-5
MESH = pl.DeviceIdType.MESH
CH = 512
GATHER_QKV = (5, 4, 5)
GATHER_UP = (5, 4, 5)
LAGS_OUT = (3, 9, 15)
LAGS_DOWN = (2, 6, 10)
UP_TILES = 3
N_FAR = 1
N_WD = 4


def f32(v):
    return v.astype(jnp.float32)


def bf16(v):
    return v.astype(jnp.bfloat16)


def dot(a, b):
    return jnp.dot(a, b, preferred_element_type=jnp.float32)


def layer_kernel(
    n_dev,
    x_hbm, g1_hbm, s1_hbm, wqkv, bqkv_hbm, wo, bo_hbm, g2_hbm, s2_hbm, wu, bu_hbm, wd, bd_hbm,
    out_ref,
    x_ref, g1_ref, s1_ref, g2_ref, s2_ref, bqkv_ref, bo_ref, bu_ref, bd_ref,
    xb, h_all, u_w, pool, acc, qkv, ctx, act, psend, precv,
    hop_s, hop_r, fin_s, fin_r, x1,
    xsem, psem, usem, osem, dsem, ag_send, ag_l, ag_r, ag_l2, ag_r2, ag_p,
    rs_send, rs_p, rs_hl, rs_hr, rs_fl, rs_fr,
):
    small = [pltpu.make_async_copy(a, b, xsem.at[i]) for i, (a, b) in enumerate(
        ((x_hbm, x_ref), (g1_hbm, g1_ref), (s1_hbm, s1_ref)))]
    late = [pltpu.make_async_copy(a, b, psem.at[i]) for i, (a, b) in enumerate(
        ((bqkv_hbm, bqkv_ref), (bo_hbm, bo_ref), (g2_hbm, g2_ref), (s2_hbm, s2_ref), (bu_hbm, bu_ref), (bd_hbm, bd_ref)))]
    for copy in small + late:
        copy.start()
    n_chips = n_dev // 2
    rows, dim = x_ref.shape
    nch = dim // CH
    ng = nch // 2
    hr = rows // 2
    side = hr * n_chips
    st_rows = 2 * side
    n_tok = 2 * st_rows
    hc = CH // 2
    n_slab = wqkv.shape[0]
    hd = wqkv.shape[2]
    heads = n_slab // 3
    qw = n_slab * hd
    ff = wu.shape[1]
    nt = ff // CH
    me = lax.axis_index("tp")
    chip, core = me // 2, me % 2
    right = {"tp": ((chip + 1) % n_chips) * 2 + core}
    left = {"tp": ((chip + n_chips - 1) % n_chips) * 2 + core}
    mate = {"tp": chip * 2 + (1 - core)}
    far = {"tp": ((chip + 2) % n_chips) * 2 + core}

    def push(src, dst, ssem, rsem, dev):
        return pltpu.make_async_remote_copy(
            src_ref=src, dst_ref=dst, send_sem=ssem, recv_sem=rsem, device_id=dev, device_id_type=MESH)

    barrier = pltpu.get_barrier_semaphore()
    for dev in (left, right, mate, far):
        pl.semaphore_signal(barrier, inc=1, device_id=dev, device_id_type=MESH)

    def load_qkv(j):
        for s in range(n_slab):
            pltpu.make_async_copy(
                wqkv.at[s, pl.ds(pl.multiple_of(j * CH, CH), CH), :],
                u_w.at[j, :, pl.ds(s * hd, hd)], usem.at[j]).start()

    def load_up(j):
        return pltpu.make_async_copy(
            wu.at[pl.ds(pl.multiple_of(j * CH, CH), CH), :], u_w.at[j], usem.at[j])

    kt = heads * hd
    nk = ff // kt
    o_base = (N_WD - 1) * nk

    def load_down(q):
        g, slot = q % ng, q % N_WD
        for k in range(nk):
            pltpu.make_async_copy(
                wd.at[pl.ds(k * kt, kt), pl.ds(pl.multiple_of(g * 2 * CH, 2 * CH), 2 * CH)],
                pool.at[slot * nk + k], dsem.at[slot]).start()

    def wait_down(q):
        slot = q % N_WD
        pltpu.make_async_copy(pool.at[pl.ds(slot * nk, nk)], pool.at[pl.ds(slot * nk, nk)], dsem.at[slot]).wait()

    def init_loads(j, c):
        load_qkv(j)
        return c

    lax.fori_loop(0, nch, init_loads, 0)
    for g in range(ng):
        pltpu.make_async_copy(wo.at[:, pl.ds(g * 2 * CH, 2 * CH)], pool.at[o_base + g], osem).start()
    for q in range(N_WD - 1):
        load_down(q)

    def norm(get, put, n, gain_ref, shift_ref):
        tot = jnp.zeros((n, CH), jnp.float32)
        for j in range(nch):
            tot += get(j)
        mean = jnp.sum(tot, axis=1, keepdims=True) * (1.0 / dim)
        tot = jnp.zeros((n, CH), jnp.float32)
        for j in range(nch):
            cen = get(j) - mean
            tot += cen * cen
        var = jnp.sum(tot, axis=1, keepdims=True) * (1.0 / dim)
        inv = lax.rsqrt(var + LN_EPS)
        for j in range(nch):
            cols = slice(j * CH, (j + 1) * CH)
            put(j, bf16((get(j) - mean) * inv * gain_ref[:, cols] + shift_ref[:, cols]))

    def put_both(j, y):
        h_all[j, 0, 0:hr, :] = y[0:hr]
        h_all[j, 1, 0:hr, :] = y[hr:]

    def put_stream(st):
        def put(j, y):
            h_all[j, st, 0:hr, :] = y
        return put

    for copy in small:
        copy.wait()
    norm(lambda j: f32(x_ref[:, j * CH:(j + 1) * CH]), put_both, rows, g1_ref, s1_ref)
    acc[...] = jnp.zeros_like(acc)
    pl.semaphore_wait(barrier, 4)

    def piece_both(v, s, r, lo=0, n=CH):
        return h_all.at[v, :, pl.ds(s * side + r * hr, hr), pl.ds(lo, n)]

    def all_both(v, s):
        return h_all.at[v, :, pl.ds(s * side, side), :]

    def piece_stream(v, s, r, lo=0, n=CH):
        return h_all.at[pl.ds((v % ng) * 2, 2), v // ng, pl.ds(s * side + r * hr, hr), pl.ds(lo, n)]

    def all_stream(v, s):
        return h_all.at[pl.ds((v % ng) * 2, 2), v // ng, pl.ds(s * side, side), :]

    def send_own(at, v):
        push(at(v, 0, 0), at(v, 0, 3), ag_send, ag_l.at[v], right).start()
        push(at(v, 0, 0), at(v, 0, 1), ag_send, ag_r.at[v], left).start()
        push(at(v, 0, 0), at(v, 1, 0), ag_send, ag_p.at[v], mate).start()

    def wait_mate(whole, v):
        push(whole(v, 0), whole(v, 1), ag_send, ag_p.at[v], mate).wait_recv()

    def forward_one(at, i):
        with jax.named_scope("gw1l"):
            push(at(i, 0, 0), at(i, 0, 3), ag_send, ag_l.at[i], right).wait_recv()
        push(at(i, 0, 3, 0, hc), at(i, 0, 2, 0, hc), ag_send, ag_l2.at[i], right).start()
        with jax.named_scope("gw1r"):
            push(at(i, 0, 0), at(i, 0, 1), ag_send, ag_r.at[i], left).wait_recv()
        push(at(i, 0, 1, hc, hc), at(i, 0, 2, hc, hc), ag_send, ag_r2.at[i], left).start()
        push(at(i, 0, 3), at(i, 1, 3), ag_send, ag_p.at[i], mate).start()
        push(at(i, 0, 1), at(i, 1, 1), ag_send, ag_p.at[i], mate).start()

    def forward_two(at, j):
        with jax.named_scope("gw2"):
            push(at(j, 0, 3, 0, hc), at(j, 0, 2, 0, hc), ag_send, ag_l2.at[j], right).wait_recv()
            push(at(j, 0, 1, hc, hc), at(j, 0, 2, hc, hc), ag_send, ag_r2.at[j], left).wait_recv()
        push(at(j, 0, 2), at(j, 1, 2), ag_send, ag_p.at[j], mate).start()

    def gather(at, whole, n_use, consume, lags):
        look, lag_b, lag_c = lags

        def step(i, c):
            @pl.when(i < nch)
            def _():
                forward_one(at, i)

            @pl.when(i + look < nch)
            def _():
                send_own(at, i + look)

            @pl.when((i >= lag_b) & (i < nch + lag_b))
            def _():
                forward_two(at, i - lag_b)

            @pl.when(i >= lag_c)
            def _():
                j = i - lag_c
                with jax.named_scope("gwp"):
                    wait_mate(whole, j)
                with jax.named_scope("guse"):
                    consume(j)
            return c

        lax.fori_loop(0, n_use + lag_c, step, 0)

    def gather_drain():
        sent = h_all.at[:, :, pl.ds(0, 7 * hr), :]
        push(sent, sent, ag_send, ag_p.at[0], mate).wait_send()

    tiles = [(t, min(CH, qw - t * CH)) for t in range((qw + CH - 1) // CH)]

    def use_qkv(j):
        part = u_w.at[j, :, pl.ds(0, qw)]
        pltpu.make_async_copy(part, part, usem.at[j]).wait()
        h = h_all[j].reshape(n_tok, CH)

        @pl.when(j < nch - 1)
        def _():
            for t, n in tiles:
                p = dot(h, u_w[j, :, t * CH:t * CH + n])
                acc[2 * t, :, 0:n] += p[0:st_rows]
                acc[2 * t + 1, :, 0:n] += p[st_rows:]

        @pl.when(j == nch - 1)
        def _():
            for t, n in tiles:
                p = dot(h, u_w[j, :, t * CH:t * CH + n])
                slabs = range(t * CH // hd, (t * CH + n) // hd)
                b = jnp.concatenate([bqkv_ref[s % heads, s // heads:s // heads + 1, :] for s in slabs], axis=1)
                for st in range(2):
                    y = acc[2 * t + st, :, 0:n] + p[st * st_rows:(st + 1) * st_rows]
                    qkv[st * st_rows:(st + 1) * st_rows, t * CH:t * CH + n] = bf16(y + f32(b))
        load_up(j).start()

    for copy in late:
        copy.wait()
    for v in range(GATHER_QKV[0]):
        send_own(piece_both, v)
    with jax.named_scope("gather1"):
        gather(piece_both, all_both, nch, use_qkv, GATHER_QKV)
    def position(i):
        st, s, r, w = i // st_rows, (i // side) % 2, (i // hr) % n_chips, i % hr
        return ((chip + r) % n_chips) * (2 * rows) + (core + s - 2 * core * s) * rows + st * hr + w

    qpos = position(lax.broadcasted_iota(jnp.int32, (n_tok, n_tok), 0))
    kpos = position(lax.broadcasted_iota(jnp.int32, (n_tok, n_tok), 1))
    keep = qpos >= kpos
    for h in range(heads):
        q = qkv[:, h * hd:(h + 1) * hd]
        k = qkv[:, (heads + h) * hd:(heads + h + 1) * hd]
        v = qkv[:, (2 * heads + h) * hd:(2 * heads + h + 1) * hd]
        logits = lax.dot_general(q, k, (((1,), (1,)), ((), ())), preferred_element_type=jnp.float32) * hd ** -0.5
        logits = jnp.where(keep, logits, -1e30)
        e = jnp.exp(logits - jnp.max(logits, axis=1, keepdims=True))
        p = bf16(e / jnp.sum(e, axis=1, keepdims=True))
        o = bf16(dot(p, v))
        for st in range(2):
            ctx[st, :, h * hd:(h + 1) * hd] = o[st * st_rows:(st + 1) * st_rows]

    gather_drain()
    o_all = pool.at[pl.ds(o_base, ng)]
    pltpu.make_async_copy(o_all, o_all, osem).wait()

    def pair_sum(v, st, g):
        for c in range(2):
            j = 2 * g + c
            s = acc[v, c * side:(c + 1) * side, :] + f32(precv[st, j])
            two = bf16(s[2 * hr:3 * hr])
            hop_s[0, st, j] = two[:, 0:hc]
            hop_s[1, st, j] = two[:, hc:]
            acc[v, c * side:(c + 1) * side, :] = s

    def middle_sum(v, st, g):
        for c in range(2):
            j = 2 * g + c
            one = acc[v, c * side + hr:c * side + 2 * hr, :]
            fin_s[0, st, j, :, 0:hc] = bf16(one[:, 0:hc] + f32(hop_r[0, st, j]))
            fin_s[0, st, j, :, hc:] = bf16(one[:, hc:])
            three = acc[v, c * side + 3 * hr:(c + 1) * side, :]
            fin_s[1, st, j, :, 0:hc] = bf16(three[:, 0:hc])
            fin_s[1, st, j, :, hc:] = bf16(three[:, hc:] + f32(hop_r[1, st, j]))

    def fins(st, g, v):
        pair = pl.ds(2 * g, 2)
        return (push(fin_s.at[0, st, pair], fin_r.at[0, st, pair], rs_send, rs_fl.at[v], right),
                push(fin_s.at[1, st, pair], fin_r.at[1, st, pair], rs_send, rs_fr.at[v], left))

    def last_sum(v, st, g, put):
        for copy in fins(st, g, v):
            copy.wait_recv()
        for c in range(2):
            j = 2 * g + c
            total = acc[v, c * side:c * side + hr, :] + f32(fin_r[0, st, j]) + f32(fin_r[1, st, j])
            put(st, j, bf16(xb[st, j] + total))

    def pairs(v, st, g):
        two = pl.ds(2 * g, 2)
        return push(psend.at[st, two], precv.at[st, two], rs_send, rs_p.at[v], mate)

    def hops(v, st, g):
        two = pl.ds(2 * g, 2)
        return (push(hop_s.at[0, st, two], hop_r.at[0, st, two], rs_send, rs_hl.at[v], right),
                push(hop_s.at[1, st, two], hop_r.at[1, st, two], rs_send, rs_hr.at[v], left))

    def scatter_drain():
        push(psend, precv, rs_send, rs_p.at[0], mate).wait_send()
        push(hop_s, hop_r, rs_send, rs_p.at[0], mate).wait_send()
        push(fin_s, fin_r, rs_send, rs_p.at[0], mate).wait_send()

    bo = f32(bo_ref[...]).reshape(1, dim)
    for j in range(nch):
        cols = slice(j * CH, (j + 1) * CH)
        y = f32(x_ref[:, cols]) + bo[:, cols]
        xb[0, j] = y[0:hr]
        xb[1, j] = y[hr:]

    def put_x1(st, j, y):
        x1[st, j] = y

    lag_p, lag_h, lag_f = LAGS_OUT

    def when_v(k, n, fn):
        @pl.when((k >= 0) & (k < n))
        def _():
            st = k // ng
            fn(k, st, k - st * ng)

    def out_part(v, st, g):
        with jax.named_scope("spart"):
            for c in range(2):
                p = dot(ctx[st], pool[o_base + g, :, c * CH:(c + 1) * CH])
                acc[v, c * side:(c + 1) * side, :] = p[0:side]
                psend[st, 2 * g + c] = bf16(p[side:])
        pairs(v, st, g).start()

    def out_pair(v, st, g):
        with jax.named_scope("swp"):
            pairs(v, st, g).wait_recv()
        pair_sum(v, st, g)
        for copy in hops(v, st, g):
            copy.start()

    def out_middle(v, st, g):
        with jax.named_scope("swh"):
            for copy in hops(v, st, g):
                copy.wait_recv()
        middle_sum(v, st, g)
        for copy in fins(st, g, v):
            copy.start()

    def out_last(v, st, g):
        with jax.named_scope("swf"):
            last_sum(v, st, g, put_x1)

    def out_step(i, carry):
        when_v(i, 2 * ng, out_part)
        when_v(i - lag_p, 2 * ng, out_pair)
        when_v(i - lag_h, 2 * ng, out_middle)
        when_v(i - lag_f, ng, out_last)
        return carry

    with jax.named_scope("scatter1"):
        lax.fori_loop(0, max(ng + lag_f, 2 * ng + lag_h), out_step, 0)

    load_down(N_WD - 1)

    with jax.named_scope("ln2a"):
        norm(lambda j: f32(x1[0, j]), put_stream(0), hr, g2_ref, s2_ref)
    for v in range(GATHER_UP[0]):
        send_own(piece_stream, v)

    def last_out(g, carry):
        last_sum(ng + g, 1, g, put_x1)
        return carry

    with jax.named_scope("last1"):
        lax.fori_loop(0, ng, last_out, 0)
    with jax.named_scope("ln2b"):
        norm(lambda j: f32(x1[1, j]), put_stream(1), hr, g2_ref, s2_ref)
    acc[ng:2 * ng] = jnp.zeros((ng, st_rows, CH), jnp.float32)
    bd = f32(bd_ref[...]).reshape(1, dim)
    for j in range(nch):
        for st in range(2):
            xb[st, j] = f32(x1[st, j]) + bd[:, j * CH:(j + 1) * CH]
    for j in range(nch):
        load_up(j).wait()

    bu = f32(bu_ref[...]).reshape(1, ff)

    def activate(st, t, a):
        cols = slice(t * CH, (t + 1) * CH)
        act[st, :, cols] = bf16(jax.nn.gelu(a + bu[:, cols], approximate=True))

    def use_up(g):
        h = jnp.concatenate([h_all[2 * g, 0], h_all[2 * g + 1, 0]], axis=1)

        def weight(t):
            return u_w[pl.ds(2 * g, 2), :, t * CH:(t + 1) * CH].reshape(2 * CH, CH)

        @pl.when(g < ng - 1)
        def _():
            for t in range(nt):
                acc[ng + t] += dot(h, weight(t))

        @pl.when(g == ng - 1)
        def _():
            for t in range(nt):
                activate(0, t, acc[ng + t] + dot(h, weight(t)))

    def up_block(lo, hi):
        with jax.named_scope("muse"):
            h = jnp.concatenate([h_all[j, 1] for j in range(nch)], axis=1)
            for t in range(lo, hi):
                activate(1, t, dot(h, u_w[:, :, t * CH:(t + 1) * CH].reshape(dim, CH)))

    with jax.named_scope("gather2"):
        gather(piece_stream, all_stream, ng, use_up, GATHER_UP)
    scatter_drain()

    def put_out(st, j, y):
        out_ref[pl.ds(pl.multiple_of(st * hr, hr), hr), pl.ds(pl.multiple_of(j * CH, CH), CH)] = y

    def far_down(v, st, g):
        two = pl.ds(2 * g, 2)
        return push(hop_s.at[:, st, two], hop_r.at[:, st, two], rs_send, rs_hl.at[v], far)

    first_far = 2 * ng - N_FAR

    def when_group(k, fn):
        @pl.when(((k >= 0) & (k < ng)) | ((k >= ng + 2) & (k < 2 * ng + 2)))
        def _():
            st = k // (ng + 1)
            v = k - 2 * st
            fn(v, st, v - st * ng)

    lag_p2, lag_h2, lag_f2 = LAGS_DOWN
    done_two = ng + GATHER_UP[2] - GATHER_UP[1]

    def down_part(v, st, g):
        wait_down(v)
        slot = v % N_WD
        with jax.named_scope("dpart"):
            for c in range(2):
                j = 2 * g + c
                p = dot(act[st], pool[pl.ds(slot * nk, nk), :, c * CH:(c + 1) * CH].reshape(ff, CH))
                acc[v, c * side:(c + 1) * side, :] = p[0:side]
                psend[st, j] = bf16(p[side:])

        @pl.when(v + N_WD < 2 * ng)
        def _():
            load_down(v + N_WD)
        pairs(v, st, g).start()

    def down_pair(v, st, g):
        with jax.named_scope("dwp"):
            pairs(v, st, g).wait_recv()
        pair_sum(v, st, g)

        @pl.when(v < first_far)
        def _():
            for copy in hops(v, st, g):
                copy.start()

        @pl.when(v >= first_far)
        def _():
            far_down(v, st, g).start()
            for c in range(2):
                j = 2 * g + c
                fin_s[0, st, j] = bf16(acc[v, c * side + hr:c * side + 2 * hr, :])
                fin_s[1, st, j] = bf16(acc[v, c * side + 3 * hr:(c + 1) * side, :])
            for copy in fins(st, g, v):
                copy.start()

    def down_middle(v, st, g):
        @pl.when(v < first_far)
        def _():
            with jax.named_scope("dwh"):
                for copy in hops(v, st, g):
                    copy.wait_recv()
            middle_sum(v, st, g)
            for copy in fins(st, g, v):
                copy.start()

    def down_last(v, st, g):
        @pl.when(v < first_far)
        def _():
            with jax.named_scope("dwf"):
                last_sum(v, st, g, put_out)

        @pl.when(v >= first_far)
        def _():
            with jax.named_scope("dwx"):
                far_down(v, st, g).wait_recv()
                for c in range(2):
                    j = 2 * g + c
                    acc[v, c * side:c * side + hr, 0:hc] += f32(hop_r[0, st, j])
                    acc[v, c * side:c * side + hr, hc:] += f32(hop_r[1, st, j])
                last_sum(v, st, g, put_out)

    def mlp_step(w, carry):
        @pl.when((w > ng) & (w < ng + 4))
        def _():
            def one(n, c):
                g = 2 * (w - ng - 1) + n

                @pl.when(g < ng)
                def _():
                    down_middle(g, 0, g)
                return c

            lax.fori_loop(0, 2, one, 0)

        @pl.when(w >= ng + 2 + lag_h2)
        def _():
            when_group(w - lag_h2, down_middle)

        when_group(w - lag_p2, down_pair)
        when_group(w - lag_f2, down_last)

        @pl.when(w + done_two < nch)
        def _():
            forward_two(piece_stream, w + done_two)

        @pl.when(w == ng)
        def _():
            for g in range(ng):
                wait_mate(all_stream, ng + g)
            up_block(0, UP_TILES)

        @pl.when(w == ng + 1)
        def _():
            up_block(UP_TILES, nt)

        when_group(w, down_part)
        return carry

    with jax.named_scope("mlp"):
        lax.fori_loop(0, 2 * ng + 2 + lag_f2, mlp_step, 0)
    scatter_drain()
    gather_drain()


def solution(mesh):
    n_dev = mesh.shape["tp"]

    def body(hidden, g1, s1, w_qkv, b_qkv, w_out, b_out, g2, s2, w_up, b_up, w_down, b_down):
        _, rows, dim = hidden.shape
        _, three, heads, hd = w_qkv.shape
        ff = w_up.shape[1]
        nch = dim // CH
        n_tok, hr = rows * n_dev, rows // 2
        st_rows, side = n_tok // 2, n_tok // 4
        bf, fl = jnp.bfloat16, jnp.float32
        row = lambda v: v.reshape(1, -1)
        hbm = pl.BlockSpec(memory_space=pl.ANY)
        dma = pltpu.SemaphoreType.DMA
        out = pl.pallas_call(
            functools.partial(layer_kernel, n_dev),
            out_shape=pltpu.VMEM((rows, dim), bf),
            in_specs=[hbm] * 13,
            out_specs=pl.BlockSpec(memory_space=pltpu.VMEM),
            scratch_shapes=[
                pltpu.VMEM((rows, dim), bf),
                pltpu.VMEM((1, dim), fl), pltpu.VMEM((1, dim), fl),
                pltpu.VMEM((1, dim), fl), pltpu.VMEM((1, dim), fl),
                pltpu.VMEM((heads, three, hd), bf), pltpu.VMEM((dim,), bf),
                pltpu.VMEM((ff,), bf), pltpu.VMEM((dim,), bf),
                pltpu.VMEM((2, nch, hr, CH), fl),
                pltpu.VMEM((nch, 2, st_rows, CH), bf),
                pltpu.VMEM((nch, CH, ff), bf),
                pltpu.VMEM(((N_WD - 1) * (ff // (heads * hd)) + nch // 2, heads * hd, 2 * CH), bf),
                pltpu.VMEM((nch, st_rows, CH), fl),
                pltpu.VMEM((n_tok, three * heads * hd), bf),
                pltpu.VMEM((2, st_rows, heads * hd), bf),
                pltpu.VMEM((2, st_rows, ff), bf),
                pltpu.VMEM((2, nch, side, CH), bf),
                pltpu.VMEM((2, nch, side, CH), bf),
                pltpu.VMEM((2, 2, nch, hr, CH // 2), bf),
                pltpu.VMEM((2, 2, nch, hr, CH // 2), bf),
                pltpu.VMEM((2, 2, nch, hr, CH), bf),
                pltpu.VMEM((2, 2, nch, hr, CH), bf),
                pltpu.VMEM((2, nch, hr, CH), bf),
                dma((3,)), dma((6,)), dma((nch,)), dma(()), dma((N_WD,)),
                dma(()), dma((nch,)), dma((nch,)), dma((nch,)), dma((nch,)), dma((nch,)),
                dma(()), dma((nch,)), dma((nch,)), dma((nch,)), dma((nch,)), dma((nch,)),
            ],
            compiler_params=pltpu.CompilerParams(
                collective_id=0, has_side_effects=True, vmem_limit_bytes=61 * 1024 * 1024),
            name="decoder_layer",
        )(
            hidden[0], row(g1), row(s1),
            jnp.transpose(w_qkv, (1, 2, 0, 3)).reshape(three * heads, dim, hd),
            jnp.transpose(b_qkv, (1, 0, 2)),
            w_out.reshape(heads * hd, dim), b_out, row(g2), row(s2), w_up, b_up, w_down, b_down,
        )
        return out[None]

    specs = (P("dp", "tp", None), P(), P(), P(None, None, "tp", None), P(None, "tp", None),
             P("tp", None, None), P(), P(), P(), P(None, "tp"), P("tp"), P("tp", None), P())
    return jax.shard_map(body, mesh=mesh, in_specs=specs, out_specs=P("dp", "tp", None), check_vma=False)
```

```python
import functools

import jax
import jax.numpy as jnp
from jax import lax
from jax.experimental import pallas as pl
from jax.experimental.pallas import tpu as pltpu
from jax.sharding import PartitionSpec as P

LN_EPS = 1e-5
MESH = pl.DeviceIdType.MESH
CH = 512
GATHER_QKV = (5, 4, 5)
GATHER_UP = (5, 4, 5)
LAGS_OUT = (2, 6, 11)
LAGS_DOWN = (2, 6, 10)
QKV_SINGLE = 4
UP_TILES = 3
N_WD = 4


def f32(v):
    return v.astype(jnp.float32)


def bf16(v):
    return v.astype(jnp.bfloat16)


def dot(a, b):
    return jnp.dot(a, b, preferred_element_type=jnp.float32)


def layer_kernel(
    n_dev,
    x_hbm, g1_hbm, s1_hbm, wqkv, bqkv_hbm, wo, bo_hbm, g2_hbm, s2_hbm, wu, bu_hbm, wd, bd_hbm,
    out_ref,
    x_ref, g1_ref, s1_ref, g2_ref, s2_ref, bqkv_ref, bo_ref, bu_ref, bd_ref,
    xb, h_all, u_w, pool, acc, qkv, ctx, act, psend, precv,
    hop_s, hop_r, fin_s, fin_r, x1,
    xsem, psem, usem, osem, dsem, ag_send, ag_l, ag_r, ag_l2, ag_r2, ag_p,
    rs_send, rs_p, rs_hl, rs_hr, rs_fl, rs_fr,
):
    small = [pltpu.make_async_copy(a, b, xsem.at[i]) for i, (a, b) in enumerate(
        ((x_hbm, x_ref), (g1_hbm, g1_ref), (s1_hbm, s1_ref)))]
    late = [pltpu.make_async_copy(a, b, psem.at[i]) for i, (a, b) in enumerate(
        ((bqkv_hbm, bqkv_ref), (bo_hbm, bo_ref), (g2_hbm, g2_ref), (s2_hbm, s2_ref), (bu_hbm, bu_ref), (bd_hbm, bd_ref)))]
    for copy in small + late:
        copy.start()
    n_chips = n_dev // 2
    rows, dim = x_ref.shape
    nch = dim // CH
    ng = nch // 2
    hr = rows // 2
    side = hr * n_chips
    st_rows = 2 * side
    n_tok = 2 * st_rows
    hc = CH // 2
    n_slab = wqkv.shape[0]
    hd = wqkv.shape[2]
    heads = n_slab // 3
    qw = n_slab * hd
    ff = wu.shape[1]
    nt = ff // CH
    me = lax.axis_index("tp")
    chip, core = me // 2, me % 2
    right = {"tp": ((chip + 1) % n_chips) * 2 + core}
    left = {"tp": ((chip + n_chips - 1) % n_chips) * 2 + core}
    mate = {"tp": chip * 2 + (1 - core)}

    def push(src, dst, ssem, rsem, dev):
        return pltpu.make_async_remote_copy(
            src_ref=src, dst_ref=dst, send_sem=ssem, recv_sem=rsem, device_id=dev, device_id_type=MESH)

    barrier = pltpu.get_barrier_semaphore()
    for dev in (left, right, mate):
        pl.semaphore_signal(barrier, inc=1, device_id=dev, device_id_type=MESH)

    def load_qkv(j):
        for s in range(n_slab):
            pltpu.make_async_copy(
                wqkv.at[s, pl.ds(pl.multiple_of(j * CH, CH), CH), :],
                u_w.at[j, :, pl.ds(s * hd, hd)], usem.at[j]).start()

    def load_up(j):
        return pltpu.make_async_copy(
            wu.at[pl.ds(pl.multiple_of(j * CH, CH), CH), :], u_w.at[j], usem.at[j])

    kt = heads * hd
    nk = ff // kt
    o_base = (N_WD - 1) * nk

    def load_down(q):
        g, slot = q % ng, q % N_WD
        for k in range(nk):
            pltpu.make_async_copy(
                wd.at[pl.ds(k * kt, kt), pl.ds(pl.multiple_of(g * 2 * CH, 2 * CH), 2 * CH)],
                pool.at[slot * nk + k], dsem.at[slot]).start()

    def wait_down(q):
        slot = q % N_WD
        pltpu.make_async_copy(pool.at[pl.ds(slot * nk, nk)], pool.at[pl.ds(slot * nk, nk)], dsem.at[slot]).wait()

    def init_loads(j, c):
        load_qkv(j)
        return c

    lax.fori_loop(0, nch, init_loads, 0)
    for g in range(ng):
        pltpu.make_async_copy(wo.at[:, pl.ds(g * 2 * CH, 2 * CH)], pool.at[o_base + g], osem).start()
    for q in range(N_WD - 1):
        load_down(q)

    def norm(get, put, n, gain_ref, shift_ref):
        tot = jnp.zeros((n, CH), jnp.float32)
        for j in range(nch):
            tot += get(j)
        mean = jnp.sum(tot, axis=1, keepdims=True) * (1.0 / dim)
        tot = jnp.zeros((n, CH), jnp.float32)
        for j in range(nch):
            cen = get(j) - mean
            tot += cen * cen
        var = jnp.sum(tot, axis=1, keepdims=True) * (1.0 / dim)
        inv = lax.rsqrt(var + LN_EPS)
        for j in range(nch):
            cols = slice(j * CH, (j + 1) * CH)
            put(j, bf16((get(j) - mean) * inv * gain_ref[:, cols] + shift_ref[:, cols]))

    def put_both(j, y):
        h_all[j, 0, 0:hr, :] = y[0:hr]
        h_all[j, 1, 0:hr, :] = y[hr:]

    def put_stream(st):
        def put(j, y):
            h_all[j, st, 0:hr, :] = y
        return put

    for copy in small:
        copy.wait()
    norm(lambda j: f32(x_ref[:, j * CH:(j + 1) * CH]), put_both, rows, g1_ref, s1_ref)
    acc[...] = jnp.zeros_like(acc)
    pl.semaphore_wait(barrier, 3)

    def piece_both(v, s, r, lo=0, n=CH):
        return h_all.at[v, :, pl.ds(s * side + r * hr, hr), pl.ds(lo, n)]

    def all_both(v, s):
        return h_all.at[v, :, pl.ds(s * side, side), :]

    def piece_stream(v, s, r, lo=0, n=CH):
        return h_all.at[pl.ds((v % ng) * 2, 2), v // ng, pl.ds(s * side + r * hr, hr), pl.ds(lo, n)]

    def all_stream(v, s):
        return h_all.at[pl.ds((v % ng) * 2, 2), v // ng, pl.ds(s * side, side), :]

    def send_own(at, v):
        push(at(v, 0, 0), at(v, 0, 3), ag_send, ag_l.at[v], right).start()
        push(at(v, 0, 0), at(v, 0, 1), ag_send, ag_r.at[v], left).start()
        push(at(v, 0, 0), at(v, 1, 0), ag_send, ag_p.at[v], mate).start()

    def wait_mate(whole, v):
        push(whole(v, 0), whole(v, 1), ag_send, ag_p.at[v], mate).wait_recv()

    def forward_one(at, i):
        with jax.named_scope("gw1l"):
            push(at(i, 0, 0), at(i, 0, 3), ag_send, ag_l.at[i], right).wait_recv()
        push(at(i, 0, 3, 0, hc), at(i, 0, 2, 0, hc), ag_send, ag_l2.at[i], right).start()
        with jax.named_scope("gw1r"):
            push(at(i, 0, 0), at(i, 0, 1), ag_send, ag_r.at[i], left).wait_recv()
        push(at(i, 0, 1, hc, hc), at(i, 0, 2, hc, hc), ag_send, ag_r2.at[i], left).start()
        push(at(i, 0, 3), at(i, 1, 3), ag_send, ag_p.at[i], mate).start()
        push(at(i, 0, 1), at(i, 1, 1), ag_send, ag_p.at[i], mate).start()

    def forward_two(at, j):
        with jax.named_scope("gw2"):
            push(at(j, 0, 3, 0, hc), at(j, 0, 2, 0, hc), ag_send, ag_l2.at[j], right).wait_recv()
            push(at(j, 0, 1, hc, hc), at(j, 0, 2, hc, hc), ag_send, ag_r2.at[j], left).wait_recv()
        push(at(j, 0, 2), at(j, 1, 2), ag_send, ag_p.at[j], mate).start()

    def gather(at, n_use, consume, lags):
        look, lag_b, lag_c = lags

        def step(i, c):
            @pl.when(i < nch)
            def _():
                forward_one(at, i)

            @pl.when(i + look < nch)
            def _():
                send_own(at, i + look)

            @pl.when((i >= lag_b) & (i < nch + lag_b))
            def _():
                forward_two(at, i - lag_b)

            @pl.when(i >= lag_c)
            def _():
                consume(i - lag_c)
            return c

        lax.fori_loop(0, n_use + lag_c, step, 0)

    def gather_drain():
        sent = h_all.at[:, :, pl.ds(0, 7 * hr), :]
        push(sent, sent, ag_send, ag_p.at[0], mate).wait_send()

    tiles = [(t, min(CH, qw - t * CH)) for t in range((qw + CH - 1) // CH)]

    def have_qkv(j):
        wait_mate(all_both, j)
        part = u_w.at[j, :, pl.ds(0, qw)]
        pltpu.make_async_copy(part, part, usem.at[j]).wait()

    def use_qkv(j):
        @pl.when(j < QKV_SINGLE)
        def _():
            have_qkv(j)
            h = h_all[j].reshape(n_tok, CH)
            with jax.named_scope("guse"):
                for t, n in tiles:
                    p = dot(h, u_w[j, :, t * CH:t * CH + n])
                    acc[2 * t, :, 0:n] += p[0:st_rows]
                    acc[2 * t + 1, :, 0:n] += p[st_rows:]
            load_up(j).start()

        def two(t, n):
            h = jnp.concatenate([h_all[j - 2].reshape(n_tok, CH), h_all[j - 1].reshape(n_tok, CH)], axis=1)
            return dot(h, u_w[pl.ds(j - 2, 2), :, t * CH:t * CH + n].reshape(2 * CH, n))

        @pl.when((j > QKV_SINGLE) & (j % 2 == 0) & (j < nch))
        def _():
            have_qkv(j - 2)
            have_qkv(j - 1)
            with jax.named_scope("guse2"):
                for t, n in tiles:
                    p = two(t, n)
                    acc[2 * t, :, 0:n] += p[0:st_rows]
                    acc[2 * t + 1, :, 0:n] += p[st_rows:]
            load_up(j - 2).start()
            load_up(j - 1).start()

        @pl.when(j == nch)
        def _():
            have_qkv(j - 2)
            have_qkv(j - 1)
            with jax.named_scope("guse3"):
                for t, n in tiles:
                    p = two(t, n)
                    slabs = range(t * CH // hd, (t * CH + n) // hd)
                    b = jnp.concatenate([bqkv_ref[s % heads, s // heads:s // heads + 1, :] for s in slabs], axis=1)
                    for st in range(2):
                        y = acc[2 * t + st, :, 0:n] + p[st * st_rows:(st + 1) * st_rows]
                        qkv[st * st_rows:(st + 1) * st_rows, t * CH:t * CH + n] = bf16(y + f32(b))
            load_up(j - 2).start()
            load_up(j - 1).start()

    for copy in late:
        copy.wait()
    for v in range(GATHER_QKV[0]):
        send_own(piece_both, v)
    with jax.named_scope("gather1"):
        gather(piece_both, nch + 1, use_qkv, GATHER_QKV)
    def position(i):
        st, s, r, w = i // st_rows, (i // side) % 2, (i // hr) % n_chips, i % hr
        return ((chip + r) % n_chips) * (2 * rows) + (core + s - 2 * core * s) * rows + st * hr + w

    qpos = position(lax.broadcasted_iota(jnp.int32, (n_tok, n_tok), 0))
    kpos = position(lax.broadcasted_iota(jnp.int32, (n_tok, n_tok), 1))
    keep = qpos >= kpos
    for h in range(heads):
        q = qkv[:, h * hd:(h + 1) * hd]
        k = qkv[:, (heads + h) * hd:(heads + h + 1) * hd]
        v = qkv[:, (2 * heads + h) * hd:(2 * heads + h + 1) * hd]
        logits = lax.dot_general(q, k, (((1,), (1,)), ((), ())), preferred_element_type=jnp.float32) * hd ** -0.5
        logits = jnp.where(keep, logits, -1e30)
        e = jnp.exp(logits - jnp.max(logits, axis=1, keepdims=True))
        p = bf16(e * (1.0 / jnp.sum(e, axis=1, keepdims=True)))
        o = bf16(dot(p, v))
        for st in range(2):
            ctx[st, :, h * hd:(h + 1) * hd] = o[st * st_rows:(st + 1) * st_rows]

    gather_drain()
    o_all = pool.at[pl.ds(o_base, ng)]
    pltpu.make_async_copy(o_all, o_all, osem).wait()

    def pair_sum(v, st, g):
        for c in range(2):
            j = 2 * g + c
            s = acc[v, c * side:(c + 1) * side, :] + f32(precv[st, j])
            two = bf16(s[2 * hr:3 * hr])
            hop_s[0, st, j] = two[:, 0:hc]
            hop_s[1, st, j] = two[:, hc:]
            acc[v, c * side:(c + 1) * side, :] = s

    def middle_sum(v, st, g):
        for c in range(2):
            j = 2 * g + c
            one = acc[v, c * side + hr:c * side + 2 * hr, :]
            fin_s[0, st, j, :, 0:hc] = bf16(one[:, 0:hc] + f32(hop_r[0, st, j]))
            fin_s[0, st, j, :, hc:] = bf16(one[:, hc:])
            three = acc[v, c * side + 3 * hr:(c + 1) * side, :]
            fin_s[1, st, j, :, 0:hc] = bf16(three[:, 0:hc])
            fin_s[1, st, j, :, hc:] = bf16(three[:, hc:] + f32(hop_r[1, st, j]))

    def fins(st, g, v):
        pair = pl.ds(2 * g, 2)
        return (push(fin_s.at[0, st, pair], fin_r.at[0, st, pair], rs_send, rs_fl.at[v], right),
                push(fin_s.at[1, st, pair], fin_r.at[1, st, pair], rs_send, rs_fr.at[v], left))

    def last_sum(v, st, g, put):
        for copy in fins(st, g, v):
            copy.wait_recv()
        for c in range(2):
            j = 2 * g + c
            total = acc[v, c * side:c * side + hr, :] + f32(fin_r[0, st, j]) + f32(fin_r[1, st, j])
            put(st, j, bf16(xb[st, j] + total))

    def pairs(v, st, g):
        two = pl.ds(2 * g, 2)
        return push(psend.at[st, two], precv.at[st, two], rs_send, rs_p.at[v], mate)

    def hops(v, st, g):
        two = pl.ds(2 * g, 2)
        return (push(hop_s.at[0, st, two], hop_r.at[0, st, two], rs_send, rs_hl.at[v], right),
                push(hop_s.at[1, st, two], hop_r.at[1, st, two], rs_send, rs_hr.at[v], left))

    def scatter_drain():
        push(psend, precv, rs_send, rs_p.at[0], mate).wait_send()
        push(hop_s, hop_r, rs_send, rs_p.at[0], mate).wait_send()
        push(fin_s, fin_r, rs_send, rs_p.at[0], mate).wait_send()

    bo = f32(bo_ref[...]).reshape(1, dim)
    for j in range(nch):
        cols = slice(j * CH, (j + 1) * CH)
        y = f32(x_ref[:, cols]) + bo[:, cols]
        xb[0, j] = y[0:hr]
        xb[1, j] = y[hr:]

    def put_x1(st, j, y):
        x1[st, j] = y

    lag_p, lag_h, lag_f = LAGS_OUT

    def pairs_out(g):
        two = pl.ds(2 * g, 2)
        return push(psend.at[:, two], precv.at[:, two], rs_send, rs_p.at[g], mate)

    def hops_out(g):
        two = pl.ds(2 * g, 2)
        return (push(hop_s.at[0, :, two], hop_r.at[0, :, two], rs_send, rs_hl.at[g], right),
                push(hop_s.at[1, :, two], hop_r.at[1, :, two], rs_send, rs_hr.at[g], left))

    def out_step(i, carry):
        @pl.when(i < ng)
        def _():
            with jax.named_scope("spart"):
                for c in range(2):
                    j = 2 * i + c
                    p = dot(ctx[...].reshape(n_tok, kt), pool[o_base + i, :, c * CH:(c + 1) * CH])
                    for st in range(2):
                        acc[st * ng + i, c * side:(c + 1) * side, :] = p[st * st_rows:st * st_rows + side]
                        psend[st, j] = bf16(p[st * st_rows + side:(st + 1) * st_rows])
            pairs_out(i).start()

        @pl.when((i >= lag_p) & (i < ng + lag_p))
        def _():
            g = i - lag_p
            with jax.named_scope("swp"):
                pairs_out(g).wait_recv()
            for st in range(2):
                pair_sum(st * ng + g, st, g)
            for copy in hops_out(g):
                copy.start()

        @pl.when((i >= lag_h) & (i < ng + lag_h))
        def _():
            g = i - lag_h
            with jax.named_scope("swh"):
                for copy in hops_out(g):
                    copy.wait_recv()
            for st in range(2):
                middle_sum(st * ng + g, st, g)
            for copy in fins(0, g, g):
                copy.start()

        @pl.when(i == ng + lag_h - 1)
        def _():
            for g in range(ng):
                for copy in fins(1, g, ng + g):
                    copy.start()

        @pl.when(i >= lag_f)
        def _():
            g = i - lag_f
            with jax.named_scope("swf"):
                last_sum(g, 0, g, put_x1)
        return carry

    with jax.named_scope("scatter1"):
        lax.fori_loop(0, ng + lag_f, out_step, 0)

    load_down(N_WD - 1)

    with jax.named_scope("ln2a"):
        norm(lambda j: f32(x1[0, j]), put_stream(0), hr, g2_ref, s2_ref)
    for v in range(GATHER_UP[0]):
        send_own(piece_stream, v)

    def last_out(g, carry):
        last_sum(ng + g, 1, g, put_x1)
        return carry

    with jax.named_scope("last1"):
        lax.fori_loop(0, ng, last_out, 0)
    with jax.named_scope("ln2b"):
        norm(lambda j: f32(x1[1, j]), put_stream(1), hr, g2_ref, s2_ref)
    acc[ng:2 * ng] = jnp.zeros((ng, st_rows, CH), jnp.float32)
    bd = f32(bd_ref[...]).reshape(1, dim)
    for j in range(nch):
        for st in range(2):
            xb[st, j] = f32(x1[st, j]) + bd[:, j * CH:(j + 1) * CH]
    for j in range(nch):
        load_up(j).wait()

    bu = f32(bu_ref[...]).reshape(1, ff)

    def activate(st, t, a):
        cols = slice(t * CH, (t + 1) * CH)
        act[st, :, cols] = bf16(jax.nn.gelu(a + bu[:, cols], approximate=True))

    def use_up(g):
        wait_mate(all_stream, g)
        h = jnp.concatenate([h_all[2 * g, 0], h_all[2 * g + 1, 0]], axis=1)

        def weight(t):
            return u_w[pl.ds(2 * g, 2), :, t * CH:(t + 1) * CH].reshape(2 * CH, CH)

        @pl.when(g < ng - 1)
        def _():
            for t in range(nt):
                acc[ng + t] += dot(h, weight(t))

        @pl.when(g == ng - 1)
        def _():
            for t in range(nt):
                activate(0, t, acc[ng + t] + dot(h, weight(t)))

    def up_block(lo, hi):
        with jax.named_scope("muse"):
            h = jnp.concatenate([h_all[j, 1] for j in range(nch)], axis=1)
            for t in range(lo, hi):
                activate(1, t, dot(h, u_w[:, :, t * CH:(t + 1) * CH].reshape(dim, CH)))

    with jax.named_scope("gather2"):
        gather(piece_stream, ng, use_up, GATHER_UP)
    scatter_drain()

    def put_out(st, j, y):
        out_ref[pl.ds(pl.multiple_of(st * hr, hr), hr), pl.ds(pl.multiple_of(j * CH, CH), CH)] = y

    def when_group(k, fn):
        @pl.when(((k >= 0) & (k < ng)) | ((k >= ng + 2) & (k < 2 * ng + 2)))
        def _():
            st = k // (ng + 1)
            v = k - 2 * st
            fn(v, st, v - st * ng)

    lag_p2, lag_h2, lag_f2 = LAGS_DOWN
    done_two = ng + GATHER_UP[2] - GATHER_UP[1]

    def down_part(v, st, g):
        wait_down(v)
        slot = v % N_WD
        with jax.named_scope("dpart"):
            for c in range(2):
                j = 2 * g + c
                p = dot(act[st], pool[pl.ds(slot * nk, nk), :, c * CH:(c + 1) * CH].reshape(ff, CH))
                acc[v, c * side:(c + 1) * side, :] = p[0:side]
                psend[st, j] = bf16(p[side:])

        @pl.when(v + N_WD < 2 * ng)
        def _():
            load_down(v + N_WD)
        pairs(v, st, g).start()

    def down_pair(v, st, g):
        with jax.named_scope("dwp"):
            pairs(v, st, g).wait_recv()
        pair_sum(v, st, g)
        for copy in hops(v, st, g):
            copy.start()

    def down_middle(v, st, g):
        with jax.named_scope("dwh"):
            for copy in hops(v, st, g):
                copy.wait_recv()
        middle_sum(v, st, g)
        for copy in fins(st, g, v):
            copy.start()

    def down_last(v, st, g):
        with jax.named_scope("dwf"):
            last_sum(v, st, g, put_out)

    def mlp_step(w, carry):
        @pl.when((w == ng + 1) | (w == ng + 2) | (w == ng + 4))
        def _():
            def one(n, c):
                g = jnp.minimum(2 * (w - ng - 1), ng - 1) + n

                down_middle(g, 0, g)
                return c

            lax.fori_loop(0, jnp.where(w == ng + 4, 1, 2), one, 0)

        @pl.when(w >= ng + 2 + lag_h2)
        def _():
            when_group(w - lag_h2, down_middle)

        when_group(w - lag_p2, down_pair)
        when_group(w - lag_f2, down_last)

        @pl.when(w + done_two < nch)
        def _():
            forward_two(piece_stream, w + done_two)

        @pl.when(w == ng)
        def _():
            for g in range(ng):
                wait_mate(all_stream, ng + g)
            up_block(0, UP_TILES)

        @pl.when(w == ng + 1)
        def _():
            up_block(UP_TILES, nt)

        when_group(w, down_part)
        return carry

    with jax.named_scope("mlp"):
        lax.fori_loop(0, 2 * ng + 2 + lag_f2, mlp_step, 0)
    scatter_drain()
    gather_drain()


def solution(mesh):
    n_dev = mesh.shape["tp"]

    def body(hidden, g1, s1, w_qkv, b_qkv, w_out, b_out, g2, s2, w_up, b_up, w_down, b_down):
        _, rows, dim = hidden.shape
        _, three, heads, hd = w_qkv.shape
        ff = w_up.shape[1]
        nch = dim // CH
        n_tok, hr = rows * n_dev, rows // 2
        st_rows, side = n_tok // 2, n_tok // 4
        bf, fl = jnp.bfloat16, jnp.float32
        row = lambda v: v.reshape(1, -1)
        hbm = pl.BlockSpec(memory_space=pl.ANY)
        dma = pltpu.SemaphoreType.DMA
        out = pl.pallas_call(
            functools.partial(layer_kernel, n_dev),
            out_shape=pltpu.VMEM((rows, dim), bf),
            in_specs=[hbm] * 13,
            out_specs=pl.BlockSpec(memory_space=pltpu.VMEM),
            scratch_shapes=[
                pltpu.VMEM((rows, dim), bf),
                pltpu.VMEM((1, dim), fl), pltpu.VMEM((1, dim), fl),
                pltpu.VMEM((1, dim), fl), pltpu.VMEM((1, dim), fl),
                pltpu.VMEM((heads, three, hd), bf), pltpu.VMEM((dim,), bf),
                pltpu.VMEM((ff,), bf), pltpu.VMEM((dim,), bf),
                pltpu.VMEM((2, nch, hr, CH), fl),
                pltpu.VMEM((nch, 2, st_rows, CH), bf),
                pltpu.VMEM((nch, CH, ff), bf),
                pltpu.VMEM(((N_WD - 1) * (ff // (heads * hd)) + nch // 2, heads * hd, 2 * CH), bf),
                pltpu.VMEM((nch, st_rows, CH), fl),
                pltpu.VMEM((n_tok, three * heads * hd), bf),
                pltpu.VMEM((2, st_rows, heads * hd), bf),
                pltpu.VMEM((2, st_rows, ff), bf),
                pltpu.VMEM((2, nch, side, CH), bf),
                pltpu.VMEM((2, nch, side, CH), bf),
                pltpu.VMEM((2, 2, nch, hr, CH // 2), bf),
                pltpu.VMEM((2, 2, nch, hr, CH // 2), bf),
                pltpu.VMEM((2, 2, nch, hr, CH), bf),
                pltpu.VMEM((2, 2, nch, hr, CH), bf),
                pltpu.VMEM((2, nch, hr, CH), bf),
                dma((3,)), dma((6,)), dma((nch,)), dma(()), dma((N_WD,)),
                dma(()), dma((nch,)), dma((nch,)), dma((nch,)), dma((nch,)), dma((nch,)),
                dma(()), dma((nch,)), dma((nch,)), dma((nch,)), dma((nch,)), dma((nch,)),
            ],
            compiler_params=pltpu.CompilerParams(
                collective_id=0, has_side_effects=True, vmem_limit_bytes=61 * 1024 * 1024),
            name="decoder_layer",
        )(
            hidden[0], row(g1), row(s1),
            jnp.transpose(w_qkv, (1, 2, 0, 3)).reshape(three * heads, dim, hd),
            jnp.transpose(b_qkv, (1, 0, 2)),
            w_out.reshape(heads * hd, dim), b_out, row(g2), row(s2), w_up, b_up, w_down, b_down,
        )
        return out[None]

    specs = (P("dp", "tp", None), P(), P(), P(None, None, "tp", None), P(None, "tp", None),
             P("tp", None, None), P(), P(), P(), P(None, "tp"), P("tp"), P("tp", None), P())
    return jax.shard_map(body, mesh=mesh, in_specs=specs, out_specs=P("dp", "tp", None), check_vma=False)
```

```python
import functools

import jax
import jax.numpy as jnp
from jax import lax
from jax.experimental import pallas as pl
from jax.experimental.pallas import tpu as pltpu
from jax.sharding import PartitionSpec as P

LN_EPS = 1e-5
MESH = pl.DeviceIdType.MESH
CH = 512
GATHER_QKV = (5, 4, 5)
GATHER_UP = (3, 4, 5)
FIRST_OWN = 5
LAGS_OUT = (2, 6, 11)
LAGS_DOWN = (2, 6, 10)
UP_TILES = 3
N_FAR = 1
N_WD = 4


def f32(v):
    return v.astype(jnp.float32)


def bf16(v):
    return v.astype(jnp.bfloat16)


def dot(a, b):
    return jnp.dot(a, b, preferred_element_type=jnp.float32)


def layer_kernel(
    n_dev,
    x_hbm, g1_hbm, s1_hbm, wqkv, bqkv_hbm, wo, bo_hbm, g2_hbm, s2_hbm, wu, bu_hbm, wd, bd_hbm,
    out_ref,
    x_ref, g1_ref, s1_ref, g2_ref, s2_ref, bqkv_ref, bo_ref, bu_ref, bd_ref,
    xb, h_all, u_w, pool, acc, qkv, ctx, act, psend, precv,
    hop_s, hop_r, fin_s, fin_r, x1,
    xsem, psem, usem, osem, dsem, ag_send, ag_l, ag_r, ag_l2, ag_r2, ag_p,
    rs_send, rs_p, rs_hl, rs_hr, rs_fl, rs_fr,
):
    small = [pltpu.make_async_copy(a, b, xsem.at[i]) for i, (a, b) in enumerate(
        ((x_hbm, x_ref), (g1_hbm, g1_ref), (s1_hbm, s1_ref)))]
    late = [pltpu.make_async_copy(a, b, psem.at[i]) for i, (a, b) in enumerate(
        ((bqkv_hbm, bqkv_ref), (bo_hbm, bo_ref), (g2_hbm, g2_ref), (s2_hbm, s2_ref), (bu_hbm, bu_ref), (bd_hbm, bd_ref)))]
    for copy in small + late:
        copy.start()
    n_chips = n_dev // 2
    rows, dim = x_ref.shape
    nch = dim // CH
    ng = nch // 2
    hr = rows // 2
    side = hr * n_chips
    st_rows = 2 * side
    n_tok = 2 * st_rows
    hc = CH // 2
    n_slab = wqkv.shape[0]
    hd = wqkv.shape[2]
    heads = n_slab // 3
    qw = n_slab * hd
    ff = wu.shape[1]
    nt = ff // CH
    me = lax.axis_index("tp")
    chip, core = me // 2, me % 2
    right = {"tp": ((chip + 1) % n_chips) * 2 + core}
    left = {"tp": ((chip + n_chips - 1) % n_chips) * 2 + core}
    mate = {"tp": chip * 2 + (1 - core)}
    far = {"tp": ((chip + 2) % n_chips) * 2 + core}

    def push(src, dst, ssem, rsem, dev):
        return pltpu.make_async_remote_copy(
            src_ref=src, dst_ref=dst, send_sem=ssem, recv_sem=rsem, device_id=dev, device_id_type=MESH)

    barrier = pltpu.get_barrier_semaphore()
    for dev in (left, right, mate, far):
        pl.semaphore_signal(barrier, inc=1, device_id=dev, device_id_type=MESH)

    def load_qkv(j):
        for s in range(n_slab):
            pltpu.make_async_copy(
                wqkv.at[s, pl.ds(pl.multiple_of(j * CH, CH), CH), :],
                u_w.at[j, :, pl.ds(s * hd, hd)], usem.at[j]).start()

    def load_up(j):
        return pltpu.make_async_copy(
            wu.at[pl.ds(pl.multiple_of(j * CH, CH), CH), :], u_w.at[j], usem.at[j])

    kt = heads * hd
    nk = ff // kt
    o_base = (N_WD - 1) * nk

    def load_down(q):
        g, slot = q % ng, q % N_WD
        for k in range(nk):
            pltpu.make_async_copy(
                wd.at[pl.ds(k * kt, kt), pl.ds(pl.multiple_of(g * 2 * CH, 2 * CH), 2 * CH)],
                pool.at[slot * nk + k], dsem.at[slot]).start()

    def wait_down(q):
        slot = q % N_WD
        pltpu.make_async_copy(pool.at[pl.ds(slot * nk, nk)], pool.at[pl.ds(slot * nk, nk)], dsem.at[slot]).wait()

    def init_loads(j, c):
        load_qkv(j)
        return c

    lax.fori_loop(0, nch, init_loads, 0)
    for g in range(ng):
        pltpu.make_async_copy(wo.at[:, pl.ds(g * 2 * CH, 2 * CH)], pool.at[o_base + g], osem).start()
    for q in range(N_WD - 1):
        load_down(q)

    def norm(get, put, n, gain_ref, shift_ref):
        tot = jnp.zeros((n, CH), jnp.float32)
        for j in range(nch):
            tot += get(j)
        mean = jnp.sum(tot, axis=1, keepdims=True) * (1.0 / dim)
        tot = jnp.zeros((n, CH), jnp.float32)
        for j in range(nch):
            cen = get(j) - mean
            tot += cen * cen
        var = jnp.sum(tot, axis=1, keepdims=True) * (1.0 / dim)
        inv = lax.rsqrt(var + LN_EPS)
        for j in range(nch):
            cols = slice(j * CH, (j + 1) * CH)
            put(j, bf16((get(j) - mean) * inv * gain_ref[:, cols] + shift_ref[:, cols]))

    def put_both(j, y):
        h_all[j, 0, 0:hr, :] = y[0:hr]
        h_all[j, 1, 0:hr, :] = y[hr:]

    def put_stream(st):
        def put(j, y):
            h_all[j, st, 0:hr, :] = y
        return put

    for copy in small:
        copy.wait()
    norm(lambda j: f32(x_ref[:, j * CH:(j + 1) * CH]), put_both, rows, g1_ref, s1_ref)
    acc[...] = jnp.zeros_like(acc)
    pl.semaphore_wait(barrier, 4)

    def piece_both(v, s, r, lo=0, n=CH):
        return h_all.at[v, :, pl.ds(s * side + r * hr, hr), pl.ds(lo, n)]

    def all_both(v, s):
        return h_all.at[v, :, pl.ds(s * side, side), :]

    def piece_stream(v, s, r, lo=0, n=CH):
        return h_all.at[pl.ds((v % ng) * 2, 2), v // ng, pl.ds(s * side + r * hr, hr), pl.ds(lo, n)]

    def all_stream(v, s):
        return h_all.at[pl.ds((v % ng) * 2, 2), v // ng, pl.ds(s * side, side), :]

    def send_own(at, v):
        push(at(v, 0, 0), at(v, 0, 3), ag_send, ag_l.at[v], right).start()
        push(at(v, 0, 0), at(v, 0, 1), ag_send, ag_r.at[v], left).start()
        push(at(v, 0, 0), at(v, 1, 0), ag_send, ag_p.at[v], mate).start()

    def wait_mate(whole, v):
        push(whole(v, 0), whole(v, 1), ag_send, ag_p.at[v], mate).wait_recv()

    def forward_one(at, i):
        with jax.named_scope("gw1l"):
            push(at(i, 0, 0), at(i, 0, 3), ag_send, ag_l.at[i], right).wait_recv()
        push(at(i, 0, 3, 0, hc), at(i, 0, 2, 0, hc), ag_send, ag_l2.at[i], right).start()
        with jax.named_scope("gw1r"):
            push(at(i, 0, 0), at(i, 0, 1), ag_send, ag_r.at[i], left).wait_recv()
        push(at(i, 0, 1, hc, hc), at(i, 0, 2, hc, hc), ag_send, ag_r2.at[i], left).start()
        push(at(i, 0, 3), at(i, 1, 3), ag_send, ag_p.at[i], mate).start()
        push(at(i, 0, 1), at(i, 1, 1), ag_send, ag_p.at[i], mate).start()

    def forward_two(at, j):
        with jax.named_scope("gw2"):
            push(at(j, 0, 3, 0, hc), at(j, 0, 2, 0, hc), ag_send, ag_l2.at[j], right).wait_recv()
            push(at(j, 0, 1, hc, hc), at(j, 0, 2, hc, hc), ag_send, ag_r2.at[j], left).wait_recv()
        push(at(j, 0, 2), at(j, 1, 2), ag_send, ag_p.at[j], mate).start()

    def gather(at, whole, n_use, consume, lags):
        look, lag_b, lag_c = lags

        def step(i, c):
            @pl.when(i < nch)
            def _():
                forward_one(at, i)

            @pl.when((i + look >= FIRST_OWN) & (i + look < nch))
            def _():
                send_own(at, i + look)

            @pl.when((i >= lag_b) & (i < nch + lag_b))
            def _():
                forward_two(at, i - lag_b)

            @pl.when(i >= lag_c)
            def _():
                j = i - lag_c
                with jax.named_scope("gwp"):
                    wait_mate(whole, j)
                with jax.named_scope("guse"):
                    consume(j)
            return c

        lax.fori_loop(0, n_use + lag_c, step, 0)

    def gather_drain():
        sent = h_all.at[:, :, pl.ds(0, 7 * hr), :]
        push(sent, sent, ag_send, ag_p.at[0], mate).wait_send()

    tiles = [(t, min(CH, qw - t * CH)) for t in range((qw + CH - 1) // CH)]

    def use_qkv(j):
        part = u_w.at[j, :, pl.ds(0, qw)]
        pltpu.make_async_copy(part, part, usem.at[j]).wait()
        h = h_all[j].reshape(n_tok, CH)

        @pl.when(j < nch - 1)
        def _():
            for t, n in tiles:
                p = dot(h, u_w[j, :, t * CH:t * CH + n])
                acc[2 * t, :, 0:n] += p[0:st_rows]
                acc[2 * t + 1, :, 0:n] += p[st_rows:]

        @pl.when(j == nch - 1)
        def _():
            for t, n in tiles:
                p = dot(h, u_w[j, :, t * CH:t * CH + n])
                slabs = range(t * CH // hd, (t * CH + n) // hd)
                b = jnp.concatenate([bqkv_ref[s % heads, s // heads:s // heads + 1, :] for s in slabs], axis=1)
                for st in range(2):
                    y = acc[2 * t + st, :, 0:n] + p[st * st_rows:(st + 1) * st_rows]
                    qkv[st * st_rows:(st + 1) * st_rows, t * CH:t * CH + n] = bf16(y + f32(b))
        load_up(j).start()

    for copy in late:
        copy.wait()
    for v in range(FIRST_OWN):
        send_own(piece_both, v)
    with jax.named_scope("gather1"):
        gather(piece_both, all_both, nch, use_qkv, GATHER_QKV)
    def position(i):
        st, s, r, w = i // st_rows, (i // side) % 2, (i // hr) % n_chips, i % hr
        return ((chip + r) % n_chips) * (2 * rows) + (core + s - 2 * core * s) * rows + st * hr + w

    qpos = position(lax.broadcasted_iota(jnp.int32, (n_tok, n_tok), 0))
    kpos = position(lax.broadcasted_iota(jnp.int32, (n_tok, n_tok), 1))
    keep = qpos >= kpos
    for h in range(heads):
        q = qkv[:, h * hd:(h + 1) * hd]
        k = qkv[:, (heads + h) * hd:(heads + h + 1) * hd]
        v = qkv[:, (2 * heads + h) * hd:(2 * heads + h + 1) * hd]
        logits = lax.dot_general(q, k, (((1,), (1,)), ((), ())), preferred_element_type=jnp.float32) * hd ** -0.5
        logits = jnp.where(keep, logits, -1e30)
        e = jnp.exp(logits - jnp.max(logits, axis=1, keepdims=True))
        p = bf16(e / jnp.sum(e, axis=1, keepdims=True))
        o = bf16(dot(p, v))
        for st in range(2):
            ctx[st, :, h * hd:(h + 1) * hd] = o[st * st_rows:(st + 1) * st_rows]

    gather_drain()
    o_all = pool.at[pl.ds(o_base, ng)]
    pltpu.make_async_copy(o_all, o_all, osem).wait()

    def pair_sum(v, st, g):
        for c in range(2):
            j = 2 * g + c
            s = acc[v, c * side:(c + 1) * side, :] + f32(precv[st, j])
            two = bf16(s[2 * hr:3 * hr])
            hop_s[0, st, j] = two[:, 0:hc]
            hop_s[1, st, j] = two[:, hc:]
            acc[v, c * side:(c + 1) * side, :] = s

    def middle_sum(v, st, g):
        for c in range(2):
            j = 2 * g + c
            one = acc[v, c * side + hr:c * side + 2 * hr, :]
            fin_s[0, st, j, :, 0:hc] = bf16(one[:, 0:hc] + f32(hop_r[0, st, j]))
            fin_s[0, st, j, :, hc:] = bf16(one[:, hc:])
            three = acc[v, c * side + 3 * hr:(c + 1) * side, :]
            fin_s[1, st, j, :, 0:hc] = bf16(three[:, 0:hc])
            fin_s[1, st, j, :, hc:] = bf16(three[:, hc:] + f32(hop_r[1, st, j]))

    def fins(st, g, v):
        pair = pl.ds(2 * g, 2)
        return (push(fin_s.at[0, st, pair], fin_r.at[0, st, pair], rs_send, rs_fl.at[v], right),
                push(fin_s.at[1, st, pair], fin_r.at[1, st, pair], rs_send, rs_fr.at[v], left))

    def last_sum(v, st, g, put):
        for copy in fins(st, g, v):
            copy.wait_recv()
        for c in range(2):
            j = 2 * g + c
            total = acc[v, c * side:c * side + hr, :] + f32(fin_r[0, st, j]) + f32(fin_r[1, st, j])
            put(st, j, bf16(xb[st, j] + total))

    def pairs(v, st, g):
        two = pl.ds(2 * g, 2)
        return push(psend.at[st, two], precv.at[st, two], rs_send, rs_p.at[v], mate)

    def hops(v, st, g):
        two = pl.ds(2 * g, 2)
        return (push(hop_s.at[0, st, two], hop_r.at[0, st, two], rs_send, rs_hl.at[v], right),
                push(hop_s.at[1, st, two], hop_r.at[1, st, two], rs_send, rs_hr.at[v], left))

    def scatter_drain():
        push(psend, precv, rs_send, rs_p.at[0], mate).wait_send()
        push(hop_s, hop_r, rs_send, rs_p.at[0], mate).wait_send()
        push(fin_s, fin_r, rs_send, rs_p.at[0], mate).wait_send()

    bo = f32(bo_ref[...]).reshape(1, dim)
    for j in range(nch):
        cols = slice(j * CH, (j + 1) * CH)
        y = f32(x_ref[:, cols]) + bo[:, cols]
        xb[0, j] = y[0:hr]
        xb[1, j] = y[hr:]

    def put_x1(st, j, y):
        x1[st, j] = y

    lag_p, lag_h, lag_f = LAGS_OUT

    def pairs_out(g):
        two = pl.ds(2 * g, 2)
        return push(psend.at[:, two], precv.at[:, two], rs_send, rs_p.at[g], mate)

    def hops_out(g):
        two = pl.ds(2 * g, 2)
        return (push(hop_s.at[0, :, two], hop_r.at[0, :, two], rs_send, rs_hl.at[g], right),
                push(hop_s.at[1, :, two], hop_r.at[1, :, two], rs_send, rs_hr.at[g], left))

    def out_step(i, carry):
        @pl.when(i < ng)
        def _():
            with jax.named_scope("spart"):
                for c in range(2):
                    j = 2 * i + c
                    p = dot(ctx[...].reshape(n_tok, kt), pool[o_base + i, :, c * CH:(c + 1) * CH])
                    for st in range(2):
                        acc[st * ng + i, c * side:(c + 1) * side, :] = p[st * st_rows:st * st_rows + side]
                        psend[st, j] = bf16(p[st * st_rows + side:(st + 1) * st_rows])
            pairs_out(i).start()

        @pl.when((i >= lag_p) & (i < ng + lag_p))
        def _():
            g = i - lag_p
            with jax.named_scope("swp"):
                pairs_out(g).wait_recv()
            for st in range(2):
                pair_sum(st * ng + g, st, g)
            for copy in hops_out(g):
                copy.start()

        @pl.when((i >= lag_h) & (i < ng + lag_h))
        def _():
            g = i - lag_h
            with jax.named_scope("swh"):
                for copy in hops_out(g):
                    copy.wait_recv()
            for st in range(2):
                middle_sum(st * ng + g, st, g)
            for copy in fins(0, g, g):
                copy.start()

        @pl.when(i == ng + lag_h - 1)
        def _():
            for g in range(ng):
                for copy in fins(1, g, ng + g):
                    copy.start()

        @pl.when(i >= lag_f)
        def _():
            g = i - lag_f
            with jax.named_scope("swf"):
                last_sum(g, 0, g, put_x1)
        return carry

    with jax.named_scope("scatter1"):
        lax.fori_loop(0, ng + lag_f, out_step, 0)

    load_down(N_WD - 1)

    with jax.named_scope("ln2a"):
        norm(lambda j: f32(x1[0, j]), put_stream(0), hr, g2_ref, s2_ref)
    for v in range(FIRST_OWN):
        send_own(piece_stream, v)

    def last_out(g, carry):
        last_sum(ng + g, 1, g, put_x1)
        return carry

    with jax.named_scope("last1"):
        lax.fori_loop(0, ng, last_out, 0)
    with jax.named_scope("ln2b"):
        norm(lambda j: f32(x1[1, j]), put_stream(1), hr, g2_ref, s2_ref)
    acc[ng:2 * ng] = jnp.zeros((ng, st_rows, CH), jnp.float32)
    bd = f32(bd_ref[...]).reshape(1, dim)
    for j in range(nch):
        for st in range(2):
            xb[st, j] = f32(x1[st, j]) + bd[:, j * CH:(j + 1) * CH]
    for j in range(nch):
        load_up(j).wait()

    bu = f32(bu_ref[...]).reshape(1, ff)

    def activate(st, t, a):
        cols = slice(t * CH, (t + 1) * CH)
        act[st, :, cols] = bf16(jax.nn.gelu(a + bu[:, cols], approximate=True))

    def use_up(g):
        h = jnp.concatenate([h_all[2 * g, 0], h_all[2 * g + 1, 0]], axis=1)

        def weight(t):
            return u_w[pl.ds(2 * g, 2), :, t * CH:(t + 1) * CH].reshape(2 * CH, CH)

        @pl.when(g < ng - 1)
        def _():
            for t in range(nt):
                acc[ng + t] += dot(h, weight(t))

        @pl.when(g == ng - 1)
        def _():
            for t in range(nt):
                activate(0, t, acc[ng + t] + dot(h, weight(t)))

    def up_block(lo, hi):
        with jax.named_scope("muse"):
            h = jnp.concatenate([h_all[j, 1] for j in range(nch)], axis=1)
            for t in range(lo, hi):
                activate(1, t, dot(h, u_w[:, :, t * CH:(t + 1) * CH].reshape(dim, CH)))

    with jax.named_scope("gather2"):
        gather(piece_stream, all_stream, ng, use_up, GATHER_UP)
    scatter_drain()

    def put_out(st, j, y):
        out_ref[pl.ds(pl.multiple_of(st * hr, hr), hr), pl.ds(pl.multiple_of(j * CH, CH), CH)] = y

    def far_down(v, st, g):
        two = pl.ds(2 * g, 2)
        return push(hop_s.at[:, st, two], hop_r.at[:, st, two], rs_send, rs_hl.at[v], far)

    first_far = 2 * ng - N_FAR

    def when_group(k, fn):
        @pl.when(((k >= 0) & (k < ng)) | ((k >= ng + 2) & (k < 2 * ng + 2)))
        def _():
            st = k // (ng + 1)
            v = k - 2 * st
            fn(v, st, v - st * ng)

    lag_p2, lag_h2, lag_f2 = LAGS_DOWN
    done_two = ng + GATHER_UP[2] - GATHER_UP[1]

    def down_part(v, st, g):
        wait_down(v)
        slot = v % N_WD
        with jax.named_scope("dpart"):
            for c in range(2):
                j = 2 * g + c
                p = dot(act[st], pool[pl.ds(slot * nk, nk), :, c * CH:(c + 1) * CH].reshape(ff, CH))
                acc[v, c * side:(c + 1) * side, :] = p[0:side]
                psend[st, j] = bf16(p[side:])

        @pl.when(v + N_WD < 2 * ng)
        def _():
            load_down(v + N_WD)
        pairs(v, st, g).start()

    def down_pair(v, st, g):
        with jax.named_scope("dwp"):
            pairs(v, st, g).wait_recv()
        pair_sum(v, st, g)

        @pl.when(v < first_far)
        def _():
            for copy in hops(v, st, g):
                copy.start()

        @pl.when(v >= first_far)
        def _():
            far_down(v, st, g).start()
            for c in range(2):
                j = 2 * g + c
                fin_s[0, st, j] = bf16(acc[v, c * side + hr:c * side + 2 * hr, :])
                fin_s[1, st, j] = bf16(acc[v, c * side + 3 * hr:(c + 1) * side, :])
            for copy in fins(st, g, v):
                copy.start()

    def down_middle(v, st, g):
        @pl.when(v < first_far)
        def _():
            with jax.named_scope("dwh"):
                for copy in hops(v, st, g):
                    copy.wait_recv()
            middle_sum(v, st, g)
            for copy in fins(st, g, v):
                copy.start()

    def down_last(v, st, g):
        @pl.when(v < first_far)
        def _():
            with jax.named_scope("dwf"):
                last_sum(v, st, g, put_out)

        @pl.when(v >= first_far)
        def _():
            with jax.named_scope("dwx"):
                far_down(v, st, g).wait_recv()
                for c in range(2):
                    j = 2 * g + c
                    acc[v, c * side:c * side + hr, 0:hc] += f32(hop_r[0, st, j])
                    acc[v, c * side:c * side + hr, hc:] += f32(hop_r[1, st, j])
                last_sum(v, st, g, put_out)

    def mlp_step(w, carry):
        @pl.when(w <= ng + 1)
        def _():
            when_group(w - lag_p2, down_pair)

        @pl.when((w == ng + 1) | (w == ng + 2) | (w == ng + 5))
        def _():
            def one(n, c):
                g = jnp.minimum(2 * (w - ng - 1), ng - 1) + n

                down_middle(g, 0, g)
                return c

            lax.fori_loop(0, jnp.where(w == ng + 5, 1, 2), one, 0)

        @pl.when(w >= ng + 2 + lag_h2)
        def _():
            when_group(w - lag_h2, down_middle)

        @pl.when(w > ng + 1)
        def _():
            when_group(w - lag_p2, down_pair)

        when_group(w - lag_f2, down_last)

        @pl.when(w + done_two < nch)
        def _():
            forward_two(piece_stream, w + done_two)

        @pl.when(w == ng)
        def _():
            for g in range(ng):
                wait_mate(all_stream, ng + g)
            up_block(0, UP_TILES)

        @pl.when(w == ng + 1)
        def _():
            up_block(UP_TILES, nt)

        when_group(w, down_part)
        return carry

    with jax.named_scope("mlp"):
        lax.fori_loop(0, 2 * ng + 2 + lag_f2, mlp_step, 0)
    scatter_drain()
    gather_drain()


def solution(mesh):
    n_dev = mesh.shape["tp"]

    def body(hidden, g1, s1, w_qkv, b_qkv, w_out, b_out, g2, s2, w_up, b_up, w_down, b_down):
        _, rows, dim = hidden.shape
        _, three, heads, hd = w_qkv.shape
        ff = w_up.shape[1]
        nch = dim // CH
        n_tok, hr = rows * n_dev, rows // 2
        st_rows, side = n_tok // 2, n_tok // 4
        bf, fl = jnp.bfloat16, jnp.float32
        row = lambda v: v.reshape(1, -1)
        hbm = pl.BlockSpec(memory_space=pl.ANY)
        dma = pltpu.SemaphoreType.DMA
        out = pl.pallas_call(
            functools.partial(layer_kernel, n_dev),
            out_shape=pltpu.VMEM((rows, dim), bf),
            in_specs=[hbm] * 13,
            out_specs=pl.BlockSpec(memory_space=pltpu.VMEM),
            scratch_shapes=[
                pltpu.VMEM((rows, dim), bf),
                pltpu.VMEM((1, dim), fl), pltpu.VMEM((1, dim), fl),
                pltpu.VMEM((1, dim), fl), pltpu.VMEM((1, dim), fl),
                pltpu.VMEM((heads, three, hd), bf), pltpu.VMEM((dim,), bf),
                pltpu.VMEM((ff,), bf), pltpu.VMEM((dim,), bf),
                pltpu.VMEM((2, nch, hr, CH), fl),
                pltpu.VMEM((nch, 2, st_rows, CH), bf),
                pltpu.VMEM((nch, CH, ff), bf),
                pltpu.VMEM(((N_WD - 1) * (ff // (heads * hd)) + nch // 2, heads * hd, 2 * CH), bf),
                pltpu.VMEM((nch, st_rows, CH), fl),
                pltpu.VMEM((n_tok, three * heads * hd), bf),
                pltpu.VMEM((2, st_rows, heads * hd), bf),
                pltpu.VMEM((2, st_rows, ff), bf),
                pltpu.VMEM((2, nch, side, CH), bf),
                pltpu.VMEM((2, nch, side, CH), bf),
                pltpu.VMEM((2, 2, nch, hr, CH // 2), bf),
                pltpu.VMEM((2, 2, nch, hr, CH // 2), bf),
                pltpu.VMEM((2, 2, nch, hr, CH), bf),
                pltpu.VMEM((2, 2, nch, hr, CH), bf),
                pltpu.VMEM((2, nch, hr, CH), bf),
                dma((3,)), dma((6,)), dma((nch,)), dma(()), dma((N_WD,)),
                dma(()), dma((nch,)), dma((nch,)), dma((nch,)), dma((nch,)), dma((nch,)),
                dma(()), dma((nch,)), dma((nch,)), dma((nch,)), dma((nch,)), dma((nch,)),
            ],
            compiler_params=pltpu.CompilerParams(
                collective_id=0, has_side_effects=True, vmem_limit_bytes=61 * 1024 * 1024),
            name="decoder_layer",
        )(
            hidden[0], row(g1), row(s1),
            jnp.transpose(w_qkv, (1, 2, 0, 3)).reshape(three * heads, dim, hd),
            jnp.transpose(b_qkv, (1, 0, 2)),
            w_out.reshape(heads * hd, dim), b_out, row(g2), row(s2), w_up, b_up, w_down, b_down,
        )
        return out[None]

    specs = (P("dp", "tp", None), P(), P(), P(None, None, "tp", None), P(None, "tp", None),
             P("tp", None, None), P(), P(), P(), P(None, "tp"), P("tp"), P("tp", None), P())
    return jax.shard_map(body, mesh=mesh, in_specs=specs, out_specs=P("dp", "tp", None), check_vma=False)
```

```python
import functools

import jax
import jax.numpy as jnp
from jax import lax
from jax.experimental import pallas as pl
from jax.experimental.pallas import tpu as pltpu
from jax.sharding import PartitionSpec as P

LN_EPS = 1e-5
MESH = pl.DeviceIdType.MESH
CH = 512
GATHER_QKV = (5, 4, 5)
GATHER_UP = (5, 4, 5)
LAGS_OUT = (2, 6, 11)
LAGS_DOWN = (2, 6, 10)
N_FAR = 1
N_WD = 4


def f32(v):
    return v.astype(jnp.float32)


def bf16(v):
    return v.astype(jnp.bfloat16)


def dot(a, b):
    return jnp.dot(a, b, preferred_element_type=jnp.float32)


def layer_kernel(
    n_dev,
    x_hbm, g1_hbm, s1_hbm, wqkv, bqkv_hbm, wo, bo_hbm, g2_hbm, s2_hbm, wu, bu_hbm, wd, bd_hbm,
    out_ref,
    x_ref, g1_ref, s1_ref, g2_ref, s2_ref, bqkv_ref, bo_ref, bu_ref, bd_ref,
    xb, h_all, u_w, pool, acc, qkv, ctx, act, psend, precv,
    hop_s, hop_r, fin_s, fin_r, x1,
    xsem, psem, usem, osem, dsem, ag_send, ag_l, ag_r, ag_l2, ag_r2, ag_p,
    rs_send, rs_p, rs_hl, rs_hr, rs_fl, rs_fr,
):
    small = [pltpu.make_async_copy(a, b, xsem.at[i]) for i, (a, b) in enumerate(
        ((x_hbm, x_ref), (g1_hbm, g1_ref), (s1_hbm, s1_ref)))]
    late = [pltpu.make_async_copy(a, b, psem.at[i]) for i, (a, b) in enumerate(
        ((bqkv_hbm, bqkv_ref), (bo_hbm, bo_ref), (g2_hbm, g2_ref), (s2_hbm, s2_ref), (bu_hbm, bu_ref), (bd_hbm, bd_ref)))]
    for copy in small + late:
        copy.start()
    n_chips = n_dev // 2
    rows, dim = x_ref.shape
    nch = dim // CH
    ng = nch // 2
    hr = rows // 2
    side = hr * n_chips
    st_rows = 2 * side
    n_tok = 2 * st_rows
    hc = CH // 2
    n_slab = wqkv.shape[0]
    hd = wqkv.shape[2]
    heads = n_slab // 3
    qw = n_slab * hd
    ff = wu.shape[1]
    nt = ff // CH
    me = lax.axis_index("tp")
    chip, core = me // 2, me % 2
    right = {"tp": ((chip + 1) % n_chips) * 2 + core}
    left = {"tp": ((chip + n_chips - 1) % n_chips) * 2 + core}
    mate = {"tp": chip * 2 + (1 - core)}
    far = {"tp": ((chip + 2) % n_chips) * 2 + core}

    def push(src, dst, ssem, rsem, dev):
        return pltpu.make_async_remote_copy(
            src_ref=src, dst_ref=dst, send_sem=ssem, recv_sem=rsem, device_id=dev, device_id_type=MESH)

    barrier = pltpu.get_barrier_semaphore()
    for dev in (left, right, mate, far):
        pl.semaphore_signal(barrier, inc=1, device_id=dev, device_id_type=MESH)

    def load_qkv(j):
        for s in range(n_slab):
            pltpu.make_async_copy(
                wqkv.at[s, pl.ds(pl.multiple_of(j * CH, CH), CH), :],
                u_w.at[j, :, pl.ds(s * hd, hd)], usem.at[j]).start()

    def load_up(j):
        return pltpu.make_async_copy(
            wu.at[pl.ds(pl.multiple_of(j * CH, CH), CH), :], u_w.at[j], usem.at[j])

    kt = heads * hd
    nk = ff // kt
    o_base = (N_WD - 1) * nk

    def load_down(q):
        g, slot = q % ng, q % N_WD
        for k in range(nk):
            pltpu.make_async_copy(
                wd.at[pl.ds(k * kt, kt), pl.ds(pl.multiple_of(g * 2 * CH, 2 * CH), 2 * CH)],
                pool.at[slot * nk + k], dsem.at[slot]).start()

    def wait_down(q):
        slot = q % N_WD
        pltpu.make_async_copy(pool.at[pl.ds(slot * nk, nk)], pool.at[pl.ds(slot * nk, nk)], dsem.at[slot]).wait()

    def init_loads(j, c):
        load_qkv(j)
        return c

    lax.fori_loop(0, nch, init_loads, 0)
    for g in range(ng):
        pltpu.make_async_copy(wo.at[:, pl.ds(g * 2 * CH, 2 * CH)], pool.at[o_base + g], osem).start()
    for q in range(N_WD - 1):
        load_down(q)

    def norm(get, put, n, gain_ref, shift_ref):
        tot = jnp.zeros((n, CH), jnp.float32)
        for j in range(nch):
            tot += get(j)
        mean = jnp.sum(tot, axis=1, keepdims=True) * (1.0 / dim)
        tot = jnp.zeros((n, CH), jnp.float32)
        for j in range(nch):
            cen = get(j) - mean
            tot += cen * cen
        var = jnp.sum(tot, axis=1, keepdims=True) * (1.0 / dim)
        inv = lax.rsqrt(var + LN_EPS)
        for j in range(nch):
            cols = slice(j * CH, (j + 1) * CH)
            put(j, bf16((get(j) - mean) * inv * gain_ref[:, cols] + shift_ref[:, cols]))

    def put_both(j, y):
        h_all[j, 0, 0:hr, :] = y[0:hr]
        h_all[j, 1, 0:hr, :] = y[hr:]

    def put_stream(st):
        def put(j, y):
            h_all[j, st, 0:hr, :] = y
        return put

    for copy in small:
        copy.wait()
    norm(lambda j: f32(x_ref[:, j * CH:(j + 1) * CH]), put_both, rows, g1_ref, s1_ref)
    acc[...] = jnp.zeros_like(acc)
    pl.semaphore_wait(barrier, 4)

    def piece_both(v, s, r, lo=0, n=CH):
        return h_all.at[v, :, pl.ds(s * side + r * hr, hr), pl.ds(lo, n)]

    def all_both(v, s):
        return h_all.at[v, :, pl.ds(s * side, side), :]

    def piece_stream(v, s, r, lo=0, n=CH):
        return h_all.at[pl.ds((v % ng) * 2, 2), v // ng, pl.ds(s * side + r * hr, hr), pl.ds(lo, n)]

    def all_stream(v, s):
        return h_all.at[pl.ds((v % ng) * 2, 2), v // ng, pl.ds(s * side, side), :]

    def send_own(at, v):
        push(at(v, 0, 0), at(v, 0, 3), ag_send, ag_l.at[v], right).start()
        push(at(v, 0, 0), at(v, 0, 1), ag_send, ag_r.at[v], left).start()
        push(at(v, 0, 0), at(v, 1, 0), ag_send, ag_p.at[v], mate).start()

    def wait_mate(whole, v):
        push(whole(v, 0), whole(v, 1), ag_send, ag_p.at[v], mate).wait_recv()

    def forward_one(at, i):
        with jax.named_scope("gw1l"):
            push(at(i, 0, 0), at(i, 0, 3), ag_send, ag_l.at[i], right).wait_recv()
        push(at(i, 0, 3, 0, hc), at(i, 0, 2, 0, hc), ag_send, ag_l2.at[i], right).start()
        with jax.named_scope("gw1r"):
            push(at(i, 0, 0), at(i, 0, 1), ag_send, ag_r.at[i], left).wait_recv()
        push(at(i, 0, 1, hc, hc), at(i, 0, 2, hc, hc), ag_send, ag_r2.at[i], left).start()
        push(at(i, 0, 3), at(i, 1, 3), ag_send, ag_p.at[i], mate).start()
        push(at(i, 0, 1), at(i, 1, 1), ag_send, ag_p.at[i], mate).start()

    def forward_two(at, j):
        with jax.named_scope("gw2"):
            push(at(j, 0, 3, 0, hc), at(j, 0, 2, 0, hc), ag_send, ag_l2.at[j], right).wait_recv()
            push(at(j, 0, 1, hc, hc), at(j, 0, 2, hc, hc), ag_send, ag_r2.at[j], left).wait_recv()
        push(at(j, 0, 2), at(j, 1, 2), ag_send, ag_p.at[j], mate).start()

    def gather(at, whole, n_use, consume, lags):
        look, lag_b, lag_c = lags

        def step(i, c):
            @pl.when(i < nch)
            def _():
                forward_one(at, i)

            @pl.when(i + look < nch)
            def _():
                send_own(at, i + look)

            @pl.when((i >= lag_b) & (i < nch + lag_b))
            def _():
                forward_two(at, i - lag_b)

            @pl.when(i >= lag_c)
            def _():
                j = i - lag_c
                with jax.named_scope("gwp"):
                    wait_mate(whole, j)
                with jax.named_scope("guse"):
                    consume(j)
            return c

        lax.fori_loop(0, n_use + lag_c, step, 0)

    def gather_drain():
        sent = h_all.at[:, :, pl.ds(0, 7 * hr), :]
        push(sent, sent, ag_send, ag_p.at[0], mate).wait_send()

    tiles = [(t, min(CH, qw - t * CH)) for t in range((qw + CH - 1) // CH)]

    def use_qkv(j):
        part = u_w.at[j, :, pl.ds(0, qw)]
        pltpu.make_async_copy(part, part, usem.at[j]).wait()
        h = h_all[j].reshape(n_tok, CH)

        @pl.when(j < nch - 1)
        def _():
            for t, n in tiles:
                p = dot(h, u_w[j, :, t * CH:t * CH + n])
                acc[2 * t, :, 0:n] += p[0:st_rows]
                acc[2 * t + 1, :, 0:n] += p[st_rows:]

        @pl.when(j == nch - 1)
        def _():
            for t, n in tiles:
                p = dot(h, u_w[j, :, t * CH:t * CH + n])
                slabs = range(t * CH // hd, (t * CH + n) // hd)
                b = jnp.concatenate([bqkv_ref[s % heads, s // heads:s // heads + 1, :] for s in slabs], axis=1)
                for st in range(2):
                    y = acc[2 * t + st, :, 0:n] + p[st * st_rows:(st + 1) * st_rows]
                    qkv[st * st_rows:(st + 1) * st_rows, t * CH:t * CH + n] = bf16(y + f32(b))
        load_up(j).start()

    for copy in late:
        copy.wait()
    for v in range(GATHER_QKV[0]):
        send_own(piece_both, v)
    with jax.named_scope("gather1"):
        gather(piece_both, all_both, nch, use_qkv, GATHER_QKV)
    def position(i):
        st, s, r, w = i // st_rows, (i // side) % 2, (i // hr) % n_chips, i % hr
        return ((chip + r) % n_chips) * (2 * rows) + (core + s - 2 * core * s) * rows + st * hr + w

    qpos = position(lax.broadcasted_iota(jnp.int32, (n_tok, n_tok), 0))
    kpos = position(lax.broadcasted_iota(jnp.int32, (n_tok, n_tok), 1))
    keep = qpos >= kpos
    for h in range(heads):
        q = qkv[:, h * hd:(h + 1) * hd]
        k = qkv[:, (heads + h) * hd:(heads + h + 1) * hd]
        v = qkv[:, (2 * heads + h) * hd:(2 * heads + h + 1) * hd]
        logits = lax.dot_general(q, k, (((1,), (1,)), ((), ())), preferred_element_type=jnp.float32) * hd ** -0.5
        logits = jnp.where(keep, logits, -1e30)
        e = jnp.exp(logits - jnp.max(logits, axis=1, keepdims=True))
        p = bf16(e / jnp.sum(e, axis=1, keepdims=True))
        ctx[:, h * hd:(h + 1) * hd] = bf16(dot(p, v))

    gather_drain()
    o_all = pool.at[pl.ds(o_base, ng)]
    pltpu.make_async_copy(o_all, o_all, osem).wait()

    def pair_sum(v, st, g):
        for c in range(2):
            j = 2 * g + c
            s = acc[v, c * side:(c + 1) * side, :] + f32(precv[st, j])
            two = bf16(s[2 * hr:3 * hr])
            hop_s[0, st, j] = two[:, 0:hc]
            hop_s[1, st, j] = two[:, hc:]
            acc[v, c * side:(c + 1) * side, :] = s

    def middle_sum(v, st, g):
        for c in range(2):
            j = 2 * g + c
            one = acc[v, c * side + hr:c * side + 2 * hr, :]
            fin_s[0, st, j, :, 0:hc] = bf16(one[:, 0:hc] + f32(hop_r[0, st, j]))
            fin_s[0, st, j, :, hc:] = bf16(one[:, hc:])
            three = acc[v, c * side + 3 * hr:(c + 1) * side, :]
            fin_s[1, st, j, :, 0:hc] = bf16(three[:, 0:hc])
            fin_s[1, st, j, :, hc:] = bf16(three[:, hc:] + f32(hop_r[1, st, j]))

    def fins(st, g, v):
        pair = pl.ds(2 * g, 2)
        return (push(fin_s.at[0, st, pair], fin_r.at[0, st, pair], rs_send, rs_fl.at[v], right),
                push(fin_s.at[1, st, pair], fin_r.at[1, st, pair], rs_send, rs_fr.at[v], left))

    def last_sum(v, st, g, put):
        for copy in fins(st, g, v):
            copy.wait_recv()
        for c in range(2):
            j = 2 * g + c
            total = acc[v, c * side:c * side + hr, :] + f32(fin_r[0, st, j]) + f32(fin_r[1, st, j])
            put(st, j, bf16(xb[st, j] + total))

    def scatter_drain():
        push(psend, precv, rs_send, rs_p.at[0], mate).wait_send()
        push(hop_s, hop_r, rs_send, rs_p.at[0], mate).wait_send()
        push(fin_s, fin_r, rs_send, rs_p.at[0], mate).wait_send()

    bo = f32(bo_ref[...]).reshape(1, dim)
    for j in range(nch):
        cols = slice(j * CH, (j + 1) * CH)
        y = f32(x_ref[:, cols]) + bo[:, cols]
        xb[0, j] = y[0:hr]
        xb[1, j] = y[hr:]

    def pairs_out(g):
        two = pl.ds(2 * g, 2)
        return push(psend.at[:, two], precv.at[:, two], rs_send, rs_p.at[g], mate)

    def hops_out(g):
        two = pl.ds(2 * g, 2)
        return (push(hop_s.at[0, :, two], hop_r.at[0, :, two], rs_send, rs_hl.at[g], right),
                push(hop_s.at[1, :, two], hop_r.at[1, :, two], rs_send, rs_hr.at[g], left))

    def put_x1(st, j, y):
        x1[st, j] = y

    lag_p, lag_h, lag_f = LAGS_OUT

    def out_step(i, carry):
        @pl.when(i < ng)
        def _():
            with jax.named_scope("spart"):
                for c in range(2):
                    j = 2 * i + c
                    p = dot(ctx[...], pool[o_base + i, :, c * CH:(c + 1) * CH])
                    for st in range(2):
                        acc[st * ng + i, c * side:(c + 1) * side, :] = p[st * st_rows:st * st_rows + side]
                        psend[st, j] = bf16(p[st * st_rows + side:(st + 1) * st_rows])
            pairs_out(i).start()

        @pl.when((i >= lag_p) & (i < ng + lag_p))
        def _():
            g = i - lag_p
            with jax.named_scope("swp"):
                pairs_out(g).wait_recv()
            for st in range(2):
                pair_sum(st * ng + g, st, g)
            for copy in hops_out(g):
                copy.start()

        @pl.when((i >= lag_h) & (i < ng + lag_h))
        def _():
            g = i - lag_h
            with jax.named_scope("swh"):
                for copy in hops_out(g):
                    copy.wait_recv()
            for st in range(2):
                middle_sum(st * ng + g, st, g)
            for copy in fins(0, g, g):
                copy.start()

        @pl.when(i == ng + lag_h - 1)
        def _():
            for g in range(ng):
                for copy in fins(1, g, ng + g):
                    copy.start()

        @pl.when(i >= lag_f)
        def _():
            g = i - lag_f
            with jax.named_scope("swf"):
                last_sum(g, 0, g, put_x1)
        return carry

    with jax.named_scope("scatter1"):
        lax.fori_loop(0, ng + lag_f, out_step, 0)

    load_down(N_WD - 1)

    with jax.named_scope("ln2a"):
        norm(lambda j: f32(x1[0, j]), put_stream(0), hr, g2_ref, s2_ref)
    for v in range(GATHER_UP[0]):
        send_own(piece_stream, v)

    def last_out(g, carry):
        last_sum(ng + g, 1, g, put_x1)
        return carry

    with jax.named_scope("last1"):
        lax.fori_loop(0, ng, last_out, 0)
    with jax.named_scope("ln2b"):
        norm(lambda j: f32(x1[1, j]), put_stream(1), hr, g2_ref, s2_ref)
    acc[ng:2 * ng] = jnp.zeros((ng, st_rows, CH), jnp.float32)
    bd = f32(bd_ref[...]).reshape(1, dim)
    for j in range(nch):
        for st in range(2):
            xb[st, j] = f32(x1[st, j]) + bd[:, j * CH:(j + 1) * CH]
    for j in range(nch):
        load_up(j).wait()

    bu = f32(bu_ref[...]).reshape(1, ff)

    def activate(st, t, a):
        cols = slice(t * CH, (t + 1) * CH)
        act[st, :, cols] = bf16(jax.nn.gelu(a + bu[:, cols], approximate=True))

    def use_up(g):
        h = jnp.concatenate([h_all[2 * g, 0], h_all[2 * g + 1, 0]], axis=1)

        def weight(t):
            return u_w[pl.ds(2 * g, 2), :, t * CH:(t + 1) * CH].reshape(2 * CH, CH)

        @pl.when(g < ng - 1)
        def _():
            for t in range(nt):
                acc[ng + t] += dot(h, weight(t))

        @pl.when(g == ng - 1)
        def _():
            for t in range(nt):
                activate(0, t, acc[ng + t] + dot(h, weight(t)))

    def up_whole():
        for g in range(ng):
            wait_mate(all_stream, ng + g)
        with jax.named_scope("muse"):
            h = jnp.concatenate([h_all[j, 1] for j in range(nch)], axis=1)
            for t in range(nt):
                activate(1, t, dot(h, u_w[:, :, t * CH:(t + 1) * CH].reshape(dim, CH)))

    with jax.named_scope("gather2"):
        gather(piece_stream, all_stream, ng, use_up, GATHER_UP)
    scatter_drain()

    def put_out(st, j, y):
        out_ref[pl.ds(pl.multiple_of(st * hr, hr), hr), pl.ds(pl.multiple_of(j * CH, CH), CH)] = y

    def pairs_down(v, st, g):
        two = pl.ds(2 * g, 2)
        return push(psend.at[st, two], precv.at[st, two], rs_send, rs_p.at[v], mate)

    def hops_down(v, st, g):
        two = pl.ds(2 * g, 2)
        return (push(hop_s.at[0, st, two], hop_r.at[0, st, two], rs_send, rs_hl.at[v], right),
                push(hop_s.at[1, st, two], hop_r.at[1, st, two], rs_send, rs_hr.at[v], left))

    def far_down(v, st, g):
        two = pl.ds(2 * g, 2)
        return push(hop_s.at[:, st, two], hop_r.at[:, st, two], rs_send, rs_hl.at[v], far)

    first_far = 2 * ng - N_FAR

    def when_group(k, fn):
        @pl.when((k >= 0) & (k <= 2 * ng) & (k != ng))
        def _():
            st = k // (ng + 1)
            v = k - st
            fn(v, st, v - st * ng)

    lag_p2, lag_h2, lag_f2 = LAGS_DOWN
    done_two = ng + GATHER_UP[2] - GATHER_UP[1]

    def down_part(v, st, g):
        wait_down(v)
        slot = v % N_WD
        with jax.named_scope("dpart"):
            for c in range(2):
                j = 2 * g + c
                p = dot(act[st], pool[pl.ds(slot * nk, nk), :, c * CH:(c + 1) * CH].reshape(ff, CH))
                acc[v, c * side:(c + 1) * side, :] = p[0:side]
                psend[st, j] = bf16(p[side:])

        @pl.when(v + N_WD < 2 * ng)
        def _():
            load_down(v + N_WD)
        pairs_down(v, st, g).start()

    def down_pair(v, st, g):
        with jax.named_scope("dwp"):
            pairs_down(v, st, g).wait_recv()
        pair_sum(v, st, g)

        @pl.when(v < first_far)
        def _():
            for copy in hops_down(v, st, g):
                copy.start()

        @pl.when(v >= first_far)
        def _():
            far_down(v, st, g).start()
            for c in range(2):
                j = 2 * g + c
                fin_s[0, st, j] = bf16(acc[v, c * side + hr:c * side + 2 * hr, :])
                fin_s[1, st, j] = bf16(acc[v, c * side + 3 * hr:(c + 1) * side, :])
            for copy in fins(st, g, v):
                copy.start()

    def down_middle(v, st, g):
        @pl.when(v < first_far)
        def _():
            with jax.named_scope("dwh"):
                for copy in hops_down(v, st, g):
                    copy.wait_recv()
            middle_sum(v, st, g)
            for copy in fins(st, g, v):
                copy.start()

    def down_last(v, st, g):
        @pl.when(v < first_far)
        def _():
            with jax.named_scope("dwf"):
                last_sum(v, st, g, put_out)

        @pl.when(v >= first_far)
        def _():
            with jax.named_scope("dwx"):
                far_down(v, st, g).wait_recv()
                for c in range(2):
                    j = 2 * g + c
                    acc[v, c * side:c * side + hr, 0:hc] += f32(hop_r[0, st, j])
                    acc[v, c * side:c * side + hr, hc:] += f32(hop_r[1, st, j])
                last_sum(v, st, g, put_out)

    def mlp_step(w, carry):
        tail = w >= ng + 1 + lag_h2

        @pl.when(tail)
        def _():
            when_group(w - lag_h2, down_middle)

        when_group(w - lag_p2, down_pair)

        @pl.when(jnp.logical_not(tail))
        def _():
            when_group(w - lag_h2, down_middle)

        when_group(w - lag_f2, down_last)

        @pl.when(w + done_two < nch)
        def _():
            forward_two(piece_stream, w + done_two)

        pl.when(w == ng)(up_whole)
        when_group(w, down_part)
        return carry

    with jax.named_scope("mlp"):
        lax.fori_loop(0, 2 * ng + 1 + lag_f2, mlp_step, 0)
    scatter_drain()
    gather_drain()


def solution(mesh):
    n_dev = mesh.shape["tp"]

    def body(hidden, g1, s1, w_qkv, b_qkv, w_out, b_out, g2, s2, w_up, b_up, w_down, b_down):
        _, rows, dim = hidden.shape
        _, three, heads, hd = w_qkv.shape
        ff = w_up.shape[1]
        nch = dim // CH
        n_tok, hr = rows * n_dev, rows // 2
        st_rows, side = n_tok // 2, n_tok // 4
        bf, fl = jnp.bfloat16, jnp.float32
        row = lambda v: v.reshape(1, -1)
        hbm = pl.BlockSpec(memory_space=pl.ANY)
        dma = pltpu.SemaphoreType.DMA
        out = pl.pallas_call(
            functools.partial(layer_kernel, n_dev),
            out_shape=pltpu.VMEM((rows, dim), bf),
            in_specs=[hbm] * 13,
            out_specs=pl.BlockSpec(memory_space=pltpu.VMEM),
            scratch_shapes=[
                pltpu.VMEM((rows, dim), bf),
                pltpu.VMEM((1, dim), fl), pltpu.VMEM((1, dim), fl),
                pltpu.VMEM((1, dim), fl), pltpu.VMEM((1, dim), fl),
                pltpu.VMEM((heads, three, hd), bf), pltpu.VMEM((dim,), bf),
                pltpu.VMEM((ff,), bf), pltpu.VMEM((dim,), bf),
                pltpu.VMEM((2, nch, hr, CH), fl),
                pltpu.VMEM((nch, 2, st_rows, CH), bf),
                pltpu.VMEM((nch, CH, ff), bf),
                pltpu.VMEM(((N_WD - 1) * (ff // (heads * hd)) + nch // 2, heads * hd, 2 * CH), bf),
                pltpu.VMEM((nch, st_rows, CH), fl),
                pltpu.VMEM((n_tok, three * heads * hd), bf),
                pltpu.VMEM((n_tok, heads * hd), bf),
                pltpu.VMEM((2, st_rows, ff), bf),
                pltpu.VMEM((2, nch, side, CH), bf),
                pltpu.VMEM((2, nch, side, CH), bf),
                pltpu.VMEM((2, 2, nch, hr, CH // 2), bf),
                pltpu.VMEM((2, 2, nch, hr, CH // 2), bf),
                pltpu.VMEM((2, 2, nch, hr, CH), bf),
                pltpu.VMEM((2, 2, nch, hr, CH), bf),
                pltpu.VMEM((2, nch, hr, CH), bf),
                dma((3,)), dma((6,)), dma((nch,)), dma(()), dma((N_WD,)),
                dma(()), dma((nch,)), dma((nch,)), dma((nch,)), dma((nch,)), dma((nch,)),
                dma(()), dma((nch,)), dma((nch,)), dma((nch,)), dma((nch,)), dma((nch,)),
            ],
            compiler_params=pltpu.CompilerParams(
                collective_id=0, has_side_effects=True, vmem_limit_bytes=61 * 1024 * 1024),
            name="decoder_layer",
        )(
            hidden[0], row(g1), row(s1),
            jnp.transpose(w_qkv, (1, 2, 0, 3)).reshape(three * heads, dim, hd),
            jnp.transpose(b_qkv, (1, 0, 2)),
            w_out.reshape(heads * hd, dim), b_out, row(g2), row(s2), w_up, b_up, w_down, b_down,
        )
        return out[None]

    specs = (P("dp", "tp", None), P(), P(), P(None, None, "tp", None), P(None, "tp", None),
             P("tp", None, None), P(), P(), P(), P(None, "tp"), P("tp"), P("tp", None), P())
    return jax.shard_map(body, mesh=mesh, in_specs=specs, out_specs=P("dp", "tp", None), check_vma=False)
```

```python
import functools

import jax
import jax.numpy as jnp
from jax import lax
from jax.experimental import pallas as pl
from jax.experimental.pallas import tpu as pltpu
from jax.sharding import PartitionSpec as P

LN_EPS = 1e-5
MESH = pl.DeviceIdType.MESH
CH = 512
GATHER_QKV = (5, 4, 5)
GATHER_UP = (5, 4, 5)
LAGS_OUT = (2, 6, 11)
LAGS_DOWN = (2, 6, 10)
N_FAR = 1
N_WD = 4


def f32(v):
    return v.astype(jnp.float32)


def bf16(v):
    return v.astype(jnp.bfloat16)


def dot(a, b):
    return jnp.dot(a, b, preferred_element_type=jnp.float32)


def layer_kernel(
    n_dev,
    x_hbm, g1_hbm, s1_hbm, wqkv, bqkv_hbm, wo, bo_hbm, g2_hbm, s2_hbm, wu, bu_hbm, wd, bd_hbm,
    out_ref,
    x_ref, g1_ref, s1_ref, g2_ref, s2_ref, bqkv_ref, bo_ref, bu_ref, bd_ref,
    xb, h_all, u_w, pool, acc, qkv, ctx, act, psend, precv,
    hop_s, hop_r, fin_s, fin_r, x1,
    xsem, psem, usem, osem, dsem, ag_send, ag_l, ag_r, ag_l2, ag_r2, ag_p,
    rs_send, rs_p, rs_hl, rs_hr, rs_fl, rs_fr,
):
    small = [pltpu.make_async_copy(a, b, xsem.at[i]) for i, (a, b) in enumerate(
        ((x_hbm, x_ref), (g1_hbm, g1_ref), (s1_hbm, s1_ref)))]
    late = [pltpu.make_async_copy(a, b, psem.at[i]) for i, (a, b) in enumerate(
        ((bqkv_hbm, bqkv_ref), (bo_hbm, bo_ref), (g2_hbm, g2_ref), (s2_hbm, s2_ref), (bu_hbm, bu_ref), (bd_hbm, bd_ref)))]
    for copy in small + late:
        copy.start()
    n_chips = n_dev // 2
    rows, dim = x_ref.shape
    nch = dim // CH
    ng = nch // 2
    hr = rows // 2
    side = hr * n_chips
    st_rows = 2 * side
    n_tok = 2 * st_rows
    hc = CH // 2
    n_slab = wqkv.shape[0]
    hd = wqkv.shape[2]
    heads = n_slab // 3
    qw = n_slab * hd
    ff = wu.shape[1]
    nt = ff // CH
    me = lax.axis_index("tp")
    chip, core = me // 2, me % 2
    right = {"tp": ((chip + 1) % n_chips) * 2 + core}
    left = {"tp": ((chip + n_chips - 1) % n_chips) * 2 + core}
    mate = {"tp": chip * 2 + (1 - core)}
    far = {"tp": ((chip + 2) % n_chips) * 2 + core}

    def push(src, dst, ssem, rsem, dev):
        return pltpu.make_async_remote_copy(
            src_ref=src, dst_ref=dst, send_sem=ssem, recv_sem=rsem, device_id=dev, device_id_type=MESH)

    barrier = pltpu.get_barrier_semaphore()
    for dev in (left, right, mate, far):
        pl.semaphore_signal(barrier, inc=1, device_id=dev, device_id_type=MESH)

    def load_qkv(j):
        for s in range(n_slab):
            pltpu.make_async_copy(
                wqkv.at[s, pl.ds(pl.multiple_of(j * CH, CH), CH), :],
                u_w.at[j, :, pl.ds(s * hd, hd)], usem.at[j]).start()

    def load_up(j):
        return pltpu.make_async_copy(
            wu.at[pl.ds(pl.multiple_of(j * CH, CH), CH), :], u_w.at[j], usem.at[j])

    kt = heads * hd
    nk = ff // kt
    o_base = (N_WD - 1) * nk

    def load_down(q):
        g, slot = q % ng, q % N_WD
        for k in range(nk):
            pltpu.make_async_copy(
                wd.at[pl.ds(k * kt, kt), pl.ds(pl.multiple_of(g * 2 * CH, 2 * CH), 2 * CH)],
                pool.at[slot * nk + k], dsem.at[slot]).start()

    def wait_down(q):
        slot = q % N_WD
        pltpu.make_async_copy(pool.at[pl.ds(slot * nk, nk)], pool.at[pl.ds(slot * nk, nk)], dsem.at[slot]).wait()

    def init_loads(j, c):
        load_qkv(j)
        return c

    lax.fori_loop(0, nch, init_loads, 0)
    for g in range(ng):
        pltpu.make_async_copy(wo.at[:, pl.ds(g * 2 * CH, 2 * CH)], pool.at[o_base + g], osem).start()
    for q in range(N_WD - 1):
        load_down(q)

    def norm(get, put, n, gain_ref, shift_ref):
        tot = jnp.zeros((n, CH), jnp.float32)
        for j in range(nch):
            tot += get(j)
        mean = jnp.sum(tot, axis=1, keepdims=True) * (1.0 / dim)
        tot = jnp.zeros((n, CH), jnp.float32)
        for j in range(nch):
            cen = get(j) - mean
            tot += cen * cen
        var = jnp.sum(tot, axis=1, keepdims=True) * (1.0 / dim)
        inv = lax.rsqrt(var + LN_EPS)
        for j in range(nch):
            cols = slice(j * CH, (j + 1) * CH)
            put(j, bf16((get(j) - mean) * inv * gain_ref[:, cols] + shift_ref[:, cols]))

    def put_both(j, y):
        h_all[j, 0, 0:hr, :] = y[0:hr]
        h_all[j, 1, 0:hr, :] = y[hr:]

    def put_stream(st):
        def put(j, y):
            h_all[j, st, 0:hr, :] = y
        return put

    for copy in small:
        copy.wait()
    norm(lambda j: f32(x_ref[:, j * CH:(j + 1) * CH]), put_both, rows, g1_ref, s1_ref)
    acc[...] = jnp.zeros_like(acc)
    pl.semaphore_wait(barrier, 4)

    def piece_both(v, s, r, lo=0, n=CH):
        return h_all.at[v, :, pl.ds(s * side + r * hr, hr), pl.ds(lo, n)]

    def all_both(v, s):
        return h_all.at[v, :, pl.ds(s * side, side), :]

    def piece_stream(v, s, r, lo=0, n=CH):
        return h_all.at[pl.ds((v % ng) * 2, 2), v // ng, pl.ds(s * side + r * hr, hr), pl.ds(lo, n)]

    def all_stream(v, s):
        return h_all.at[pl.ds((v % ng) * 2, 2), v // ng, pl.ds(s * side, side), :]

    def send_own(at, v):
        push(at(v, 0, 0), at(v, 0, 3), ag_send, ag_l.at[v], right).start()
        push(at(v, 0, 0), at(v, 0, 1), ag_send, ag_r.at[v], left).start()
        push(at(v, 0, 0), at(v, 1, 0), ag_send, ag_p.at[v], mate).start()

    def wait_mate(whole, v):
        push(whole(v, 0), whole(v, 1), ag_send, ag_p.at[v], mate).wait_recv()

    def forward_one(at, i):
        with jax.named_scope("gw1l"):
            push(at(i, 0, 0), at(i, 0, 3), ag_send, ag_l.at[i], right).wait_recv()
        push(at(i, 0, 3, 0, hc), at(i, 0, 2, 0, hc), ag_send, ag_l2.at[i], right).start()
        with jax.named_scope("gw1r"):
            push(at(i, 0, 0), at(i, 0, 1), ag_send, ag_r.at[i], left).wait_recv()
        push(at(i, 0, 1, hc, hc), at(i, 0, 2, hc, hc), ag_send, ag_r2.at[i], left).start()
        push(at(i, 0, 3), at(i, 1, 3), ag_send, ag_p.at[i], mate).start()
        push(at(i, 0, 1), at(i, 1, 1), ag_send, ag_p.at[i], mate).start()

    def forward_two(at, j):
        with jax.named_scope("gw2"):
            push(at(j, 0, 3, 0, hc), at(j, 0, 2, 0, hc), ag_send, ag_l2.at[j], right).wait_recv()
            push(at(j, 0, 1, hc, hc), at(j, 0, 2, hc, hc), ag_send, ag_r2.at[j], left).wait_recv()
        push(at(j, 0, 2), at(j, 1, 2), ag_send, ag_p.at[j], mate).start()

    def gather(at, whole, n_use, consume, lags):
        look, lag_b, lag_c = lags

        def step(i, c):
            @pl.when(i < nch)
            def _():
                forward_one(at, i)

            @pl.when(i + look < nch)
            def _():
                send_own(at, i + look)

            @pl.when((i >= lag_b) & (i < nch + lag_b))
            def _():
                forward_two(at, i - lag_b)

            @pl.when(i >= lag_c)
            def _():
                j = i - lag_c
                with jax.named_scope("gwp"):
                    wait_mate(whole, j)
                with jax.named_scope("guse"):
                    consume(j)
            return c

        lax.fori_loop(0, n_use + lag_c, step, 0)

    def gather_drain():
        sent = h_all.at[:, :, pl.ds(0, 7 * hr), :]
        push(sent, sent, ag_send, ag_p.at[0], mate).wait_send()

    tiles = [(t, min(CH, qw - t * CH)) for t in range((qw + CH - 1) // CH)]

    def use_qkv(j):
        part = u_w.at[j, :, pl.ds(0, qw)]
        pltpu.make_async_copy(part, part, usem.at[j]).wait()
        h = h_all[j].reshape(n_tok, CH)

        @pl.when(j < nch - 1)
        def _():
            for t, n in tiles:
                p = dot(h, u_w[j, :, t * CH:t * CH + n])
                acc[2 * t, :, 0:n] += p[0:st_rows]
                acc[2 * t + 1, :, 0:n] += p[st_rows:]

        @pl.when(j == nch - 1)
        def _():
            for t, n in tiles:
                p = dot(h, u_w[j, :, t * CH:t * CH + n])
                slabs = range(t * CH // hd, (t * CH + n) // hd)
                b = jnp.concatenate([bqkv_ref[s % heads, s // heads:s // heads + 1, :] for s in slabs], axis=1)
                for st in range(2):
                    y = acc[2 * t + st, :, 0:n] + p[st * st_rows:(st + 1) * st_rows]
                    qkv[st * st_rows:(st + 1) * st_rows, t * CH:t * CH + n] = bf16(y + f32(b))
        load_up(j).start()

    for copy in late:
        copy.wait()
    for v in range(GATHER_QKV[0]):
        send_own(piece_both, v)
    with jax.named_scope("gather1"):
        gather(piece_both, all_both, nch, use_qkv, GATHER_QKV)
    def position(i):
        st, s, r, w = i // st_rows, (i // side) % 2, (i // hr) % n_chips, i % hr
        return ((chip + r) % n_chips) * (2 * rows) + (core + s - 2 * core * s) * rows + st * hr + w

    qpos = position(lax.broadcasted_iota(jnp.int32, (n_tok, n_tok), 0))
    kpos = position(lax.broadcasted_iota(jnp.int32, (n_tok, n_tok), 1))
    keep = qpos >= kpos
    for h in range(heads):
        q = qkv[:, h * hd:(h + 1) * hd]
        k = qkv[:, (heads + h) * hd:(heads + h + 1) * hd]
        v = qkv[:, (2 * heads + h) * hd:(2 * heads + h + 1) * hd]
        logits = lax.dot_general(q, k, (((1,), (1,)), ((), ())), preferred_element_type=jnp.float32) * hd ** -0.5
        logits = jnp.where(keep, logits, -1e30)
        e = jnp.exp(logits - jnp.max(logits, axis=1, keepdims=True))
        p = bf16(e / jnp.sum(e, axis=1, keepdims=True))
        ctx[:, h * hd:(h + 1) * hd] = bf16(dot(p, v))

    gather_drain()
    o_all = pool.at[pl.ds(o_base, ng)]
    pltpu.make_async_copy(o_all, o_all, osem).wait()

    def pair_sum(v, st, g):
        for c in range(2):
            j = 2 * g + c
            s = acc[v, c * side:(c + 1) * side, :] + f32(precv[st, j])
            two = bf16(s[2 * hr:3 * hr])
            hop_s[0, st, j] = two[:, 0:hc]
            hop_s[1, st, j] = two[:, hc:]
            acc[v, c * side:(c + 1) * side, :] = s

    def middle_sum(v, st, g):
        for c in range(2):
            j = 2 * g + c
            one = acc[v, c * side + hr:c * side + 2 * hr, :]
            fin_s[0, st, j, :, 0:hc] = bf16(one[:, 0:hc] + f32(hop_r[0, st, j]))
            fin_s[0, st, j, :, hc:] = bf16(one[:, hc:])
            three = acc[v, c * side + 3 * hr:(c + 1) * side, :]
            fin_s[1, st, j, :, 0:hc] = bf16(three[:, 0:hc])
            fin_s[1, st, j, :, hc:] = bf16(three[:, hc:] + f32(hop_r[1, st, j]))

    def fins(st, g, v):
        pair = pl.ds(2 * g, 2)
        return (push(fin_s.at[0, st, pair], fin_r.at[0, st, pair], rs_send, rs_fl.at[v], right),
                push(fin_s.at[1, st, pair], fin_r.at[1, st, pair], rs_send, rs_fr.at[v], left))

    def last_sum(v, st, g, put):
        for copy in fins(st, g, v):
            copy.wait_recv()
        for c in range(2):
            j = 2 * g + c
            total = acc[v, c * side:c * side + hr, :] + f32(fin_r[0, st, j]) + f32(fin_r[1, st, j])
            put(st, j, bf16(xb[st, j] + total))

    def pairs_down(v, st, g):
        two = pl.ds(2 * g, 2)
        return push(psend.at[st, two], precv.at[st, two], rs_send, rs_p.at[v], mate)

    def hops_down(v, st, g):
        two = pl.ds(2 * g, 2)
        return (push(hop_s.at[0, st, two], hop_r.at[0, st, two], rs_send, rs_hl.at[v], right),
                push(hop_s.at[1, st, two], hop_r.at[1, st, two], rs_send, rs_hr.at[v], left))

    def scatter_drain():
        push(psend, precv, rs_send, rs_p.at[0], mate).wait_send()
        push(hop_s, hop_r, rs_send, rs_p.at[0], mate).wait_send()
        push(fin_s, fin_r, rs_send, rs_p.at[0], mate).wait_send()

    bo = f32(bo_ref[...]).reshape(1, dim)
    for j in range(nch):
        cols = slice(j * CH, (j + 1) * CH)
        y = f32(x_ref[:, cols]) + bo[:, cols]
        xb[0, j] = y[0:hr]
        xb[1, j] = y[hr:]

    def pairs_out(g):
        two = pl.ds(2 * g, 2)
        return push(psend.at[:, two], precv.at[:, two], rs_send, rs_p.at[g], mate)

    def put_x1(st, j, y):
        x1[st, j] = y

    lag_p, lag_h, lag_f = LAGS_OUT

    def out_step(i, carry):
        @pl.when(i < ng)
        def _():
            with jax.named_scope("spart"):
                for c in range(2):
                    j = 2 * i + c
                    p = dot(ctx[...], pool[o_base + i, :, c * CH:(c + 1) * CH])
                    for st in range(2):
                        acc[st * ng + i, c * side:(c + 1) * side, :] = p[st * st_rows:st * st_rows + side]
                        psend[st, j] = bf16(p[st * st_rows + side:(st + 1) * st_rows])
            pairs_out(i).start()

        @pl.when((i >= lag_p) & (i < ng + lag_p))
        def _():
            g = i - lag_p
            with jax.named_scope("swp"):
                pairs_out(g).wait_recv()
            for st in range(2):
                pair_sum(st * ng + g, st, g)
            for copy in hops_down(g, 0, g):
                copy.start()

        @pl.when((i >= lag_h) & (i < ng + lag_h))
        def _():
            g = i - lag_h
            with jax.named_scope("swh"):
                for copy in hops_down(g, 0, g):
                    copy.wait_recv()
            middle_sum(g, 0, g)
            for copy in fins(0, g, g) + hops_down(ng + g, 1, g):
                copy.start()

        @pl.when((i >= lag_h + ng) & (i < lag_h + 2 * ng))
        def _():
            g = i - lag_h - ng
            with jax.named_scope("swg"):
                for copy in hops_down(ng + g, 1, g):
                    copy.wait_recv()
            middle_sum(ng + g, 1, g)
            for copy in fins(1, g, ng + g):
                copy.start()

        @pl.when(i >= lag_f)
        def _():
            g = i - lag_f
            with jax.named_scope("swf"):
                last_sum(g, 0, g, put_x1)
        return carry

    with jax.named_scope("scatter1"):
        lax.fori_loop(0, ng + lag_f, out_step, 0)

    load_down(N_WD - 1)

    with jax.named_scope("ln2a"):
        norm(lambda j: f32(x1[0, j]), put_stream(0), hr, g2_ref, s2_ref)
    for v in range(GATHER_UP[0]):
        send_own(piece_stream, v)

    def last_out(g, carry):
        last_sum(ng + g, 1, g, put_x1)
        return carry

    with jax.named_scope("last1"):
        lax.fori_loop(0, ng, last_out, 0)
    with jax.named_scope("ln2b"):
        norm(lambda j: f32(x1[1, j]), put_stream(1), hr, g2_ref, s2_ref)
    acc[ng:2 * ng] = jnp.zeros((ng, st_rows, CH), jnp.float32)
    bd = f32(bd_ref[...]).reshape(1, dim)
    for j in range(nch):
        for st in range(2):
            xb[st, j] = f32(x1[st, j]) + bd[:, j * CH:(j + 1) * CH]
    for j in range(nch):
        load_up(j).wait()

    bu = f32(bu_ref[...]).reshape(1, ff)

    def activate(st, t, a):
        cols = slice(t * CH, (t + 1) * CH)
        act[st, :, cols] = bf16(jax.nn.gelu(a + bu[:, cols], approximate=True))

    def use_up(g):
        h = jnp.concatenate([h_all[2 * g, 0], h_all[2 * g + 1, 0]], axis=1)

        def weight(t):
            return u_w[pl.ds(2 * g, 2), :, t * CH:(t + 1) * CH].reshape(2 * CH, CH)

        @pl.when(g < ng - 1)
        def _():
            for t in range(nt):
                acc[ng + t] += dot(h, weight(t))

        @pl.when(g == ng - 1)
        def _():
            for t in range(nt):
                activate(0, t, acc[ng + t] + dot(h, weight(t)))

    def up_whole():
        for g in range(ng):
            wait_mate(all_stream, ng + g)
        with jax.named_scope("muse"):
            h = jnp.concatenate([h_all[j, 1] for j in range(nch)], axis=1)
            for t in range(nt):
                activate(1, t, dot(h, u_w[:, :, t * CH:(t + 1) * CH].reshape(dim, CH)))

    with jax.named_scope("gather2"):
        gather(piece_stream, all_stream, ng, use_up, GATHER_UP)
    scatter_drain()

    def put_out(st, j, y):
        out_ref[pl.ds(pl.multiple_of(st * hr, hr), hr), pl.ds(pl.multiple_of(j * CH, CH), CH)] = y

    def far_down(v, st, g):
        two = pl.ds(2 * g, 2)
        return push(hop_s.at[:, st, two], hop_r.at[:, st, two], rs_send, rs_hl.at[v], far)

    first_far = 2 * ng - N_FAR

    def when_group(k, fn):
        @pl.when((k >= 0) & (k <= 2 * ng) & (k != ng))
        def _():
            st = k // (ng + 1)
            v = k - st
            fn(v, st, v - st * ng)

    lag_p2, lag_h2, lag_f2 = LAGS_DOWN
    done_two = ng + GATHER_UP[2] - GATHER_UP[1]

    def down_part(v, st, g):
        wait_down(v)
        slot = v % N_WD
        with jax.named_scope("dpart"):
            for c in range(2):
                j = 2 * g + c
                p = dot(act[st], pool[pl.ds(slot * nk, nk), :, c * CH:(c + 1) * CH].reshape(ff, CH))
                acc[v, c * side:(c + 1) * side, :] = p[0:side]
                psend[st, j] = bf16(p[side:])

        @pl.when(v + N_WD < 2 * ng)
        def _():
            load_down(v + N_WD)
        pairs_down(v, st, g).start()

    def down_pair(v, st, g):
        with jax.named_scope("dwp"):
            pairs_down(v, st, g).wait_recv()
        pair_sum(v, st, g)

        @pl.when(v < first_far)
        def _():
            for copy in hops_down(v, st, g):
                copy.start()

        @pl.when(v >= first_far)
        def _():
            far_down(v, st, g).start()
            for c in range(2):
                j = 2 * g + c
                fin_s[0, st, j] = bf16(acc[v, c * side + hr:c * side + 2 * hr, :])
                fin_s[1, st, j] = bf16(acc[v, c * side + 3 * hr:(c + 1) * side, :])
            for copy in fins(st, g, v):
                copy.start()

    def down_middle(v, st, g):
        @pl.when(v < first_far)
        def _():
            with jax.named_scope("dwh"):
                for copy in hops_down(v, st, g):
                    copy.wait_recv()
            middle_sum(v, st, g)
            for copy in fins(st, g, v):
                copy.start()

    def down_last(v, st, g):
        @pl.when(v < first_far)
        def _():
            with jax.named_scope("dwf"):
                last_sum(v, st, g, put_out)

        @pl.when(v >= first_far)
        def _():
            with jax.named_scope("dwx"):
                far_down(v, st, g).wait_recv()
                for c in range(2):
                    j = 2 * g + c
                    acc[v, c * side:c * side + hr, 0:hc] += f32(hop_r[0, st, j])
                    acc[v, c * side:c * side + hr, hc:] += f32(hop_r[1, st, j])
                last_sum(v, st, g, put_out)

    def mlp_step(w, carry):
        tail = w >= ng + 1 + lag_h2

        @pl.when(tail)
        def _():
            when_group(w - lag_h2, down_middle)

        when_group(w - lag_p2, down_pair)

        @pl.when(jnp.logical_not(tail))
        def _():
            when_group(w - lag_h2, down_middle)

        when_group(w - lag_f2, down_last)

        @pl.when(w + done_two < nch)
        def _():
            forward_two(piece_stream, w + done_two)

        pl.when(w == ng)(up_whole)
        when_group(w, down_part)
        return carry

    with jax.named_scope("mlp"):
        lax.fori_loop(0, 2 * ng + 1 + lag_f2, mlp_step, 0)
    scatter_drain()
    gather_drain()


def solution(mesh):
    n_dev = mesh.shape["tp"]

    def body(hidden, g1, s1, w_qkv, b_qkv, w_out, b_out, g2, s2, w_up, b_up, w_down, b_down):
        _, rows, dim = hidden.shape
        _, three, heads, hd = w_qkv.shape
        ff = w_up.shape[1]
        nch = dim // CH
        n_tok, hr = rows * n_dev, rows // 2
        st_rows, side = n_tok // 2, n_tok // 4
        bf, fl = jnp.bfloat16, jnp.float32
        row = lambda v: v.reshape(1, -1)
        hbm = pl.BlockSpec(memory_space=pl.ANY)
        dma = pltpu.SemaphoreType.DMA
        out = pl.pallas_call(
            functools.partial(layer_kernel, n_dev),
            out_shape=pltpu.VMEM((rows, dim), bf),
            in_specs=[hbm] * 13,
            out_specs=pl.BlockSpec(memory_space=pltpu.VMEM),
            scratch_shapes=[
                pltpu.VMEM((rows, dim), bf),
                pltpu.VMEM((1, dim), fl), pltpu.VMEM((1, dim), fl),
                pltpu.VMEM((1, dim), fl), pltpu.VMEM((1, dim), fl),
                pltpu.VMEM((heads, three, hd), bf), pltpu.VMEM((dim,), bf),
                pltpu.VMEM((ff,), bf), pltpu.VMEM((dim,), bf),
                pltpu.VMEM((2, nch, hr, CH), fl),
                pltpu.VMEM((nch, 2, st_rows, CH), bf),
                pltpu.VMEM((nch, CH, ff), bf),
                pltpu.VMEM(((N_WD - 1) * (ff // (heads * hd)) + nch // 2, heads * hd, 2 * CH), bf),
                pltpu.VMEM((nch, st_rows, CH), fl),
                pltpu.VMEM((n_tok, three * heads * hd), bf),
                pltpu.VMEM((n_tok, heads * hd), bf),
                pltpu.VMEM((2, st_rows, ff), bf),
                pltpu.VMEM((2, nch, side, CH), bf),
                pltpu.VMEM((2, nch, side, CH), bf),
                pltpu.VMEM((2, 2, nch, hr, CH // 2), bf),
                pltpu.VMEM((2, 2, nch, hr, CH // 2), bf),
                pltpu.VMEM((2, 2, nch, hr, CH), bf),
                pltpu.VMEM((2, 2, nch, hr, CH), bf),
                pltpu.VMEM((2, nch, hr, CH), bf),
                dma((3,)), dma((6,)), dma((nch,)), dma(()), dma((N_WD,)),
                dma(()), dma((nch,)), dma((nch,)), dma((nch,)), dma((nch,)), dma((nch,)),
                dma(()), dma((nch,)), dma((nch,)), dma((nch,)), dma((nch,)), dma((nch,)),
            ],
            compiler_params=pltpu.CompilerParams(
                collective_id=0, has_side_effects=True, vmem_limit_bytes=61 * 1024 * 1024),
            name="decoder_layer",
        )(
            hidden[0], row(g1), row(s1),
            jnp.transpose(w_qkv, (1, 2, 0, 3)).reshape(three * heads, dim, hd),
            jnp.transpose(b_qkv, (1, 0, 2)),
            w_out.reshape(heads * hd, dim), b_out, row(g2), row(s2), w_up, b_up, w_down, b_down,
        )
        return out[None]

    specs = (P("dp", "tp", None), P(), P(), P(None, None, "tp", None), P(None, "tp", None),
             P("tp", None, None), P(), P(), P(), P(None, "tp"), P("tp"), P("tp", None), P())
    return jax.shard_map(body, mesh=mesh, in_specs=specs, out_specs=P("dp", "tp", None), check_vma=False)
```

```python
import functools

import jax
import jax.numpy as jnp
from jax import lax
from jax.experimental import pallas as pl
from jax.experimental.pallas import tpu as pltpu
from jax.sharding import PartitionSpec as P

LN_EPS = 1e-5
MESH = pl.DeviceIdType.MESH
CH = 512
GATHER_QKV = (5, 4, 5)
GATHER_UP = (2, 4, 5)
FIRST_OWN = 5
LAGS_OUT = (2, 6, 11)
LAGS_DOWN = (2, 6, 10)
N_FAR = 1
N_WD = 4


def f32(v):
    return v.astype(jnp.float32)


def bf16(v):
    return v.astype(jnp.bfloat16)


def dot(a, b):
    return jnp.dot(a, b, preferred_element_type=jnp.float32)


def layer_kernel(
    n_dev,
    x_hbm, g1_hbm, s1_hbm, wqkv, bqkv_hbm, wo, bo_hbm, g2_hbm, s2_hbm, wu, bu_hbm, wd, bd_hbm,
    out_ref,
    x_ref, g1_ref, s1_ref, g2_ref, s2_ref, bqkv_ref, bo_ref, bu_ref, bd_ref,
    xb, h_all, u_w, pool, acc, qkv, ctx, act, psend, precv,
    hop_s, hop_r, fin_s, fin_r, x1,
    xsem, psem, usem, osem, dsem, ag_send, ag_l, ag_r, ag_l2, ag_r2, ag_p,
    rs_send, rs_p, rs_hl, rs_hr, rs_fl, rs_fr,
):
    small = [pltpu.make_async_copy(a, b, xsem.at[i]) for i, (a, b) in enumerate(
        ((x_hbm, x_ref), (g1_hbm, g1_ref), (s1_hbm, s1_ref)))]
    late = [pltpu.make_async_copy(a, b, psem.at[i]) for i, (a, b) in enumerate(
        ((bqkv_hbm, bqkv_ref), (bo_hbm, bo_ref), (g2_hbm, g2_ref), (s2_hbm, s2_ref), (bu_hbm, bu_ref), (bd_hbm, bd_ref)))]
    for copy in small + late:
        copy.start()
    n_chips = n_dev // 2
    rows, dim = x_ref.shape
    nch = dim // CH
    ng = nch // 2
    hr = rows // 2
    side = hr * n_chips
    st_rows = 2 * side
    n_tok = 2 * st_rows
    hc = CH // 2
    n_slab = wqkv.shape[0]
    hd = wqkv.shape[2]
    heads = n_slab // 3
    qw = n_slab * hd
    ff = wu.shape[1]
    nt = ff // CH
    me = lax.axis_index("tp")
    chip, core = me // 2, me % 2
    right = {"tp": ((chip + 1) % n_chips) * 2 + core}
    left = {"tp": ((chip + n_chips - 1) % n_chips) * 2 + core}
    mate = {"tp": chip * 2 + (1 - core)}
    far = {"tp": ((chip + 2) % n_chips) * 2 + core}

    def push(src, dst, ssem, rsem, dev):
        return pltpu.make_async_remote_copy(
            src_ref=src, dst_ref=dst, send_sem=ssem, recv_sem=rsem, device_id=dev, device_id_type=MESH)

    barrier = pltpu.get_barrier_semaphore()
    for dev in (left, right, mate, far):
        pl.semaphore_signal(barrier, inc=1, device_id=dev, device_id_type=MESH)

    def load_qkv(j):
        for s in range(n_slab):
            pltpu.make_async_copy(
                wqkv.at[s, pl.ds(pl.multiple_of(j * CH, CH), CH), :],
                u_w.at[j, :, pl.ds(s * hd, hd)], usem.at[j]).start()

    def load_up(j):
        return pltpu.make_async_copy(
            wu.at[pl.ds(pl.multiple_of(j * CH, CH), CH), :], u_w.at[j], usem.at[j])

    kt = heads * hd
    nk = ff // kt
    o_base = (N_WD - 1) * nk

    def load_down(q):
        g, slot = q % ng, q % N_WD
        for k in range(nk):
            pltpu.make_async_copy(
                wd.at[pl.ds(k * kt, kt), pl.ds(pl.multiple_of(g * 2 * CH, 2 * CH), 2 * CH)],
                pool.at[slot * nk + k], dsem.at[slot]).start()

    def wait_down(q):
        slot = q % N_WD
        pltpu.make_async_copy(pool.at[pl.ds(slot * nk, nk)], pool.at[pl.ds(slot * nk, nk)], dsem.at[slot]).wait()

    def init_loads(j, c):
        load_qkv(j)
        return c

    lax.fori_loop(0, nch, init_loads, 0)
    for g in range(ng):
        pltpu.make_async_copy(wo.at[:, pl.ds(g * 2 * CH, 2 * CH)], pool.at[o_base + g], osem).start()
    for q in range(N_WD - 1):
        load_down(q)

    def norm(get, put, n, gain_ref, shift_ref):
        tot = jnp.zeros((n, CH), jnp.float32)
        for j in range(nch):
            tot += get(j)
        mean = jnp.sum(tot, axis=1, keepdims=True) * (1.0 / dim)
        tot = jnp.zeros((n, CH), jnp.float32)
        for j in range(nch):
            cen = get(j) - mean
            tot += cen * cen
        var = jnp.sum(tot, axis=1, keepdims=True) * (1.0 / dim)
        inv = lax.rsqrt(var + LN_EPS)
        for j in range(nch):
            cols = slice(j * CH, (j + 1) * CH)
            put(j, bf16((get(j) - mean) * inv * gain_ref[:, cols] + shift_ref[:, cols]))

    def put_both(j, y):
        h_all[j, 0, 0:hr, :] = y[0:hr]
        h_all[j, 1, 0:hr, :] = y[hr:]

    def put_stream(st):
        def put(j, y):
            h_all[j, st, 0:hr, :] = y
        return put

    for copy in small:
        copy.wait()
    norm(lambda j: f32(x_ref[:, j * CH:(j + 1) * CH]), put_both, rows, g1_ref, s1_ref)
    acc[...] = jnp.zeros_like(acc)
    pl.semaphore_wait(barrier, 4)

    def piece_both(v, s, r, lo=0, n=CH):
        return h_all.at[v, :, pl.ds(s * side + r * hr, hr), pl.ds(lo, n)]

    def all_both(v, s):
        return h_all.at[v, :, pl.ds(s * side, side), :]

    def piece_stream(v, s, r, lo=0, n=CH):
        return h_all.at[pl.ds((v % ng) * 2, 2), v // ng, pl.ds(s * side + r * hr, hr), pl.ds(lo, n)]

    def all_stream(v, s):
        return h_all.at[pl.ds((v % ng) * 2, 2), v // ng, pl.ds(s * side, side), :]

    def send_own(at, v):
        push(at(v, 0, 0), at(v, 0, 3), ag_send, ag_l.at[v], right).start()
        push(at(v, 0, 0), at(v, 0, 1), ag_send, ag_r.at[v], left).start()
        push(at(v, 0, 0), at(v, 1, 0), ag_send, ag_p.at[v], mate).start()

    def wait_mate(whole, v):
        push(whole(v, 0), whole(v, 1), ag_send, ag_p.at[v], mate).wait_recv()

    def forward_one(at, i):
        with jax.named_scope("gw1l"):
            push(at(i, 0, 0), at(i, 0, 3), ag_send, ag_l.at[i], right).wait_recv()
        push(at(i, 0, 3, 0, hc), at(i, 0, 2, 0, hc), ag_send, ag_l2.at[i], right).start()
        with jax.named_scope("gw1r"):
            push(at(i, 0, 0), at(i, 0, 1), ag_send, ag_r.at[i], left).wait_recv()
        push(at(i, 0, 1, hc, hc), at(i, 0, 2, hc, hc), ag_send, ag_r2.at[i], left).start()
        push(at(i, 0, 3), at(i, 1, 3), ag_send, ag_p.at[i], mate).start()
        push(at(i, 0, 1), at(i, 1, 1), ag_send, ag_p.at[i], mate).start()

    def forward_two(at, j):
        with jax.named_scope("gw2"):
            push(at(j, 0, 3, 0, hc), at(j, 0, 2, 0, hc), ag_send, ag_l2.at[j], right).wait_recv()
            push(at(j, 0, 1, hc, hc), at(j, 0, 2, hc, hc), ag_send, ag_r2.at[j], left).wait_recv()
        push(at(j, 0, 2), at(j, 1, 2), ag_send, ag_p.at[j], mate).start()

    def gather(at, whole, n_use, consume, lags, between=None):
        look, lag_b, lag_c = lags

        def step(i, c):
            if between is not None:
                pl.when(i == FIRST_OWN - look)(between)

            @pl.when(i < nch)
            def _():
                forward_one(at, i)

            @pl.when((i + look >= FIRST_OWN) & (i + look < nch))
            def _():
                send_own(at, i + look)

            @pl.when((i >= lag_b) & (i < nch + lag_b))
            def _():
                forward_two(at, i - lag_b)

            @pl.when(i >= lag_c)
            def _():
                j = i - lag_c
                with jax.named_scope("gwp"):
                    wait_mate(whole, j)
                with jax.named_scope("guse"):
                    consume(j)
            return c

        lax.fori_loop(0, n_use + lag_c, step, 0)

    def gather_drain():
        sent = h_all.at[:, :, pl.ds(0, 7 * hr), :]
        push(sent, sent, ag_send, ag_p.at[0], mate).wait_send()

    tiles = [(t, min(CH, qw - t * CH)) for t in range((qw + CH - 1) // CH)]

    def use_qkv(j):
        part = u_w.at[j, :, pl.ds(0, qw)]
        pltpu.make_async_copy(part, part, usem.at[j]).wait()
        h = h_all[j].reshape(n_tok, CH)

        @pl.when(j < nch - 1)
        def _():
            for t, n in tiles:
                p = dot(h, u_w[j, :, t * CH:t * CH + n])
                acc[2 * t, :, 0:n] += p[0:st_rows]
                acc[2 * t + 1, :, 0:n] += p[st_rows:]

        @pl.when(j == nch - 1)
        def _():
            for t, n in tiles:
                p = dot(h, u_w[j, :, t * CH:t * CH + n])
                slabs = range(t * CH // hd, (t * CH + n) // hd)
                b = jnp.concatenate([bqkv_ref[s % heads, s // heads:s // heads + 1, :] for s in slabs], axis=1)
                for st in range(2):
                    y = acc[2 * t + st, :, 0:n] + p[st * st_rows:(st + 1) * st_rows]
                    qkv[st * st_rows:(st + 1) * st_rows, t * CH:t * CH + n] = bf16(y + f32(b))
        load_up(j).start()

    for copy in late:
        copy.wait()
    for v in range(FIRST_OWN):
        send_own(piece_both, v)
    with jax.named_scope("gather1"):
        gather(piece_both, all_both, nch, use_qkv, GATHER_QKV)
    def position(i):
        st, s, r, w = i // st_rows, (i // side) % 2, (i // hr) % n_chips, i % hr
        return ((chip + r) % n_chips) * (2 * rows) + (core + s - 2 * core * s) * rows + st * hr + w

    qpos = position(lax.broadcasted_iota(jnp.int32, (n_tok, n_tok), 0))
    kpos = position(lax.broadcasted_iota(jnp.int32, (n_tok, n_tok), 1))
    keep = qpos >= kpos
    for h in range(heads):
        q = qkv[:, h * hd:(h + 1) * hd]
        k = qkv[:, (heads + h) * hd:(heads + h + 1) * hd]
        v = qkv[:, (2 * heads + h) * hd:(2 * heads + h + 1) * hd]
        logits = lax.dot_general(q, k, (((1,), (1,)), ((), ())), preferred_element_type=jnp.float32) * hd ** -0.5
        logits = jnp.where(keep, logits, -1e30)
        e = jnp.exp(logits - jnp.max(logits, axis=1, keepdims=True))
        p = bf16(e / jnp.sum(e, axis=1, keepdims=True))
        ctx[:, h * hd:(h + 1) * hd] = bf16(dot(p, v))

    gather_drain()
    o_all = pool.at[pl.ds(o_base, ng)]
    pltpu.make_async_copy(o_all, o_all, osem).wait()

    def pair_sum(v, st, g):
        for c in range(2):
            j = 2 * g + c
            s = acc[v, c * side:(c + 1) * side, :] + f32(precv[st, j])
            two = bf16(s[2 * hr:3 * hr])
            hop_s[0, st, j] = two[:, 0:hc]
            hop_s[1, st, j] = two[:, hc:]
            acc[v, c * side:(c + 1) * side, :] = s

    def middle_sum(v, st, g):
        for c in range(2):
            j = 2 * g + c
            one = acc[v, c * side + hr:c * side + 2 * hr, :]
            fin_s[0, st, j, :, 0:hc] = bf16(one[:, 0:hc] + f32(hop_r[0, st, j]))
            fin_s[0, st, j, :, hc:] = bf16(one[:, hc:])
            three = acc[v, c * side + 3 * hr:(c + 1) * side, :]
            fin_s[1, st, j, :, 0:hc] = bf16(three[:, 0:hc])
            fin_s[1, st, j, :, hc:] = bf16(three[:, hc:] + f32(hop_r[1, st, j]))

    def fins(st, g, v):
        pair = pl.ds(2 * g, 2)
        return (push(fin_s.at[0, st, pair], fin_r.at[0, st, pair], rs_send, rs_fl.at[v], right),
                push(fin_s.at[1, st, pair], fin_r.at[1, st, pair], rs_send, rs_fr.at[v], left))

    def last_sum(v, st, g, put):
        for copy in fins(st, g, v):
            copy.wait_recv()
        for c in range(2):
            j = 2 * g + c
            total = acc[v, c * side:c * side + hr, :] + f32(fin_r[0, st, j]) + f32(fin_r[1, st, j])
            put(st, j, bf16(xb[st, j] + total))

    def pairs_down(v, st, g):
        two = pl.ds(2 * g, 2)
        return push(psend.at[st, two], precv.at[st, two], rs_send, rs_p.at[v], mate)

    def hops_down(v, st, g):
        two = pl.ds(2 * g, 2)
        return (push(hop_s.at[0, st, two], hop_r.at[0, st, two], rs_send, rs_hl.at[v], right),
                push(hop_s.at[1, st, two], hop_r.at[1, st, two], rs_send, rs_hr.at[v], left))

    def scatter_drain():
        push(psend, precv, rs_send, rs_p.at[0], mate).wait_send()
        push(hop_s, hop_r, rs_send, rs_p.at[0], mate).wait_send()
        push(fin_s, fin_r, rs_send, rs_p.at[0], mate).wait_send()

    bo = f32(bo_ref[...]).reshape(1, dim)
    for j in range(nch):
        cols = slice(j * CH, (j + 1) * CH)
        y = f32(x_ref[:, cols]) + bo[:, cols]
        xb[0, j] = y[0:hr]
        xb[1, j] = y[hr:]

    def pairs_out(g):
        two = pl.ds(2 * g, 2)
        return push(psend.at[:, two], precv.at[:, two], rs_send, rs_p.at[g], mate)

    def put_x1(st, j, y):
        x1[st, j] = y

    lag_p, lag_h, lag_f = LAGS_OUT

    def out_step(i, carry):
        @pl.when(i < ng)
        def _():
            with jax.named_scope("spart"):
                for c in range(2):
                    j = 2 * i + c
                    p = dot(ctx[...], pool[o_base + i, :, c * CH:(c + 1) * CH])
                    for st in range(2):
                        acc[st * ng + i, c * side:(c + 1) * side, :] = p[st * st_rows:st * st_rows + side]
                        psend[st, j] = bf16(p[st * st_rows + side:(st + 1) * st_rows])
            pairs_out(i).start()

        @pl.when((i >= lag_p) & (i < ng + lag_p))
        def _():
            g = i - lag_p
            with jax.named_scope("swp"):
                pairs_out(g).wait_recv()
            for st in range(2):
                pair_sum(st * ng + g, st, g)
            for copy in hops_down(g, 0, g):
                copy.start()

        @pl.when((i >= lag_h) & (i < ng + lag_h))
        def _():
            g = i - lag_h
            with jax.named_scope("swh"):
                for copy in hops_down(g, 0, g):
                    copy.wait_recv()
            middle_sum(g, 0, g)
            for copy in fins(0, g, g) + hops_down(ng + g, 1, g):
                copy.start()

        @pl.when((i >= lag_h + ng) & (i < lag_h + 2 * ng))
        def _():
            g = i - lag_h - ng
            with jax.named_scope("swg"):
                for copy in hops_down(ng + g, 1, g):
                    copy.wait_recv()
            middle_sum(ng + g, 1, g)
            for copy in fins(1, g, ng + g):
                copy.start()

        @pl.when(i >= lag_f)
        def _():
            g = i - lag_f
            with jax.named_scope("swf"):
                last_sum(g, 0, g, put_x1)
        return carry

    with jax.named_scope("scatter1"):
        lax.fori_loop(0, ng + lag_f, out_step, 0)

    load_down(N_WD - 1)

    with jax.named_scope("ln2a"):
        norm(lambda j: f32(x1[0, j]), put_stream(0), hr, g2_ref, s2_ref)
    for v in range(FIRST_OWN):
        send_own(piece_stream, v)

    def last_out(g, carry):
        last_sum(ng + g, 1, g, put_x1)
        return carry

    def second_stream():
        with jax.named_scope("last1"):
            lax.fori_loop(0, ng, last_out, 0)
        with jax.named_scope("ln2b"):
            norm(lambda j: f32(x1[1, j]), put_stream(1), hr, g2_ref, s2_ref)
        acc[ng:2 * ng] = jnp.zeros((ng, st_rows, CH), jnp.float32)
        bd = f32(bd_ref[...]).reshape(1, dim)
        for j in range(nch):
            for st in range(2):
                xb[st, j] = f32(x1[st, j]) + bd[:, j * CH:(j + 1) * CH]
        for j in range(nch):
            load_up(j).wait()

    bu = f32(bu_ref[...]).reshape(1, ff)

    def activate(st, t, a):
        cols = slice(t * CH, (t + 1) * CH)
        act[st, :, cols] = bf16(jax.nn.gelu(a + bu[:, cols], approximate=True))

    def use_up(g):
        h = jnp.concatenate([h_all[2 * g, 0], h_all[2 * g + 1, 0]], axis=1)

        def weight(t):
            return u_w[pl.ds(2 * g, 2), :, t * CH:(t + 1) * CH].reshape(2 * CH, CH)

        @pl.when(g < ng - 1)
        def _():
            for t in range(nt):
                acc[ng + t] += dot(h, weight(t))

        @pl.when(g == ng - 1)
        def _():
            for t in range(nt):
                activate(0, t, acc[ng + t] + dot(h, weight(t)))

    def up_whole():
        for g in range(ng):
            wait_mate(all_stream, ng + g)
        with jax.named_scope("muse"):
            h = jnp.concatenate([h_all[j, 1] for j in range(nch)], axis=1)
            for t in range(nt):
                activate(1, t, dot(h, u_w[:, :, t * CH:(t + 1) * CH].reshape(dim, CH)))

    with jax.named_scope("gather2"):
        gather(piece_stream, all_stream, ng, use_up, GATHER_UP, second_stream)
    scatter_drain()

    def put_out(st, j, y):
        out_ref[pl.ds(pl.multiple_of(st * hr, hr), hr), pl.ds(pl.multiple_of(j * CH, CH), CH)] = y

    def far_down(v, st, g):
        two = pl.ds(2 * g, 2)
        return push(hop_s.at[:, st, two], hop_r.at[:, st, two], rs_send, rs_hl.at[v], far)

    first_far = 2 * ng - N_FAR

    def when_group(k, fn):
        @pl.when((k >= 0) & (k <= 2 * ng) & (k != ng))
        def _():
            st = k // (ng + 1)
            v = k - st
            fn(v, st, v - st * ng)

    lag_p2, lag_h2, lag_f2 = LAGS_DOWN
    done_two = ng + GATHER_UP[2] - GATHER_UP[1]

    def down_part(v, st, g):
        wait_down(v)
        slot = v % N_WD
        with jax.named_scope("dpart"):
            for c in range(2):
                j = 2 * g + c
                p = dot(act[st], pool[pl.ds(slot * nk, nk), :, c * CH:(c + 1) * CH].reshape(ff, CH))
                acc[v, c * side:(c + 1) * side, :] = p[0:side]
                psend[st, j] = bf16(p[side:])

        @pl.when(v + N_WD < 2 * ng)
        def _():
            load_down(v + N_WD)
        pairs_down(v, st, g).start()

    def down_pair(v, st, g):
        with jax.named_scope("dwp"):
            pairs_down(v, st, g).wait_recv()
        pair_sum(v, st, g)

        @pl.when(v < first_far)
        def _():
            for copy in hops_down(v, st, g):
                copy.start()

        @pl.when(v >= first_far)
        def _():
            far_down(v, st, g).start()
            for c in range(2):
                j = 2 * g + c
                fin_s[0, st, j] = bf16(acc[v, c * side + hr:c * side + 2 * hr, :])
                fin_s[1, st, j] = bf16(acc[v, c * side + 3 * hr:(c + 1) * side, :])
            for copy in fins(st, g, v):
                copy.start()

    def down_middle(v, st, g):
        @pl.when(v < first_far)
        def _():
            with jax.named_scope("dwh"):
                for copy in hops_down(v, st, g):
                    copy.wait_recv()
            middle_sum(v, st, g)
            for copy in fins(st, g, v):
                copy.start()

    def down_last(v, st, g):
        @pl.when(v < first_far)
        def _():
            with jax.named_scope("dwf"):
                last_sum(v, st, g, put_out)

        @pl.when(v >= first_far)
        def _():
            with jax.named_scope("dwx"):
                far_down(v, st, g).wait_recv()
                for c in range(2):
                    j = 2 * g + c
                    acc[v, c * side:c * side + hr, 0:hc] += f32(hop_r[0, st, j])
                    acc[v, c * side:c * side + hr, hc:] += f32(hop_r[1, st, j])
                last_sum(v, st, g, put_out)

    def mlp_step(w, carry):
        tail = w >= ng + 1 + lag_h2

        @pl.when(tail)
        def _():
            when_group(w - lag_h2, down_middle)

        when_group(w - lag_p2, down_pair)

        @pl.when(jnp.logical_not(tail))
        def _():
            when_group(w - lag_h2, down_middle)

        when_group(w - lag_f2, down_last)

        @pl.when(w + done_two < nch)
        def _():
            forward_two(piece_stream, w + done_two)

        pl.when(w == ng)(up_whole)
        when_group(w, down_part)
        return carry

    with jax.named_scope("mlp"):
        lax.fori_loop(0, 2 * ng + 1 + lag_f2, mlp_step, 0)
    scatter_drain()
    gather_drain()


def solution(mesh):
    n_dev = mesh.shape["tp"]

    def body(hidden, g1, s1, w_qkv, b_qkv, w_out, b_out, g2, s2, w_up, b_up, w_down, b_down):
        _, rows, dim = hidden.shape
        _, three, heads, hd = w_qkv.shape
        ff = w_up.shape[1]
        nch = dim // CH
        n_tok, hr = rows * n_dev, rows // 2
        st_rows, side = n_tok // 2, n_tok // 4
        bf, fl = jnp.bfloat16, jnp.float32
        row = lambda v: v.reshape(1, -1)
        hbm = pl.BlockSpec(memory_space=pl.ANY)
        dma = pltpu.SemaphoreType.DMA
        out = pl.pallas_call(
            functools.partial(layer_kernel, n_dev),
            out_shape=pltpu.VMEM((rows, dim), bf),
            in_specs=[hbm] * 13,
            out_specs=pl.BlockSpec(memory_space=pltpu.VMEM),
            scratch_shapes=[
                pltpu.VMEM((rows, dim), bf),
                pltpu.VMEM((1, dim), fl), pltpu.VMEM((1, dim), fl),
                pltpu.VMEM((1, dim), fl), pltpu.VMEM((1, dim), fl),
                pltpu.VMEM((heads, three, hd), bf), pltpu.VMEM((dim,), bf),
                pltpu.VMEM((ff,), bf), pltpu.VMEM((dim,), bf),
                pltpu.VMEM((2, nch, hr, CH), fl),
                pltpu.VMEM((nch, 2, st_rows, CH), bf),
                pltpu.VMEM((nch, CH, ff), bf),
                pltpu.VMEM(((N_WD - 1) * (ff // (heads * hd)) + nch // 2, heads * hd, 2 * CH), bf),
                pltpu.VMEM((nch, st_rows, CH), fl),
                pltpu.VMEM((n_tok, three * heads * hd), bf),
                pltpu.VMEM((n_tok, heads * hd), bf),
                pltpu.VMEM((2, st_rows, ff), bf),
                pltpu.VMEM((2, nch, side, CH), bf),
                pltpu.VMEM((2, nch, side, CH), bf),
                pltpu.VMEM((2, 2, nch, hr, CH // 2), bf),
                pltpu.VMEM((2, 2, nch, hr, CH // 2), bf),
                pltpu.VMEM((2, 2, nch, hr, CH), bf),
                pltpu.VMEM((2, 2, nch, hr, CH), bf),
                pltpu.VMEM((2, nch, hr, CH), bf),
                dma((3,)), dma((6,)), dma((nch,)), dma(()), dma((N_WD,)),
                dma(()), dma((nch,)), dma((nch,)), dma((nch,)), dma((nch,)), dma((nch,)),
                dma(()), dma((nch,)), dma((nch,)), dma((nch,)), dma((nch,)), dma((nch,)),
            ],
            compiler_params=pltpu.CompilerParams(
                collective_id=0, has_side_effects=True, vmem_limit_bytes=61 * 1024 * 1024),
            name="decoder_layer",
        )(
            hidden[0], row(g1), row(s1),
            jnp.transpose(w_qkv, (1, 2, 0, 3)).reshape(three * heads, dim, hd),
            jnp.transpose(b_qkv, (1, 0, 2)),
            w_out.reshape(heads * hd, dim), b_out, row(g2), row(s2), w_up, b_up, w_down, b_down,
        )
        return out[None]

    specs = (P("dp", "tp", None), P(), P(), P(None, None, "tp", None), P(None, "tp", None),
             P("tp", None, None), P(), P(), P(), P(None, "tp"), P("tp"), P("tp", None), P())
    return jax.shard_map(body, mesh=mesh, in_specs=specs, out_specs=P("dp", "tp", None), check_vma=False)
```

```python
import functools

import jax
import jax.numpy as jnp
from jax import lax
from jax.experimental import pallas as pl
from jax.experimental.pallas import tpu as pltpu
from jax.sharding import PartitionSpec as P

LN_EPS = 1e-5
MESH = pl.DeviceIdType.MESH
CH = 512
GATHER_QKV = (5, 4, 5)
GATHER_UP = (5, 4, 5)
LAGS_OUT = (2, 6, 11)
LAGS_DOWN = (2, 6, 10)
N_FAR = 2
N_WD = 4


def f32(v):
    return v.astype(jnp.float32)


def bf16(v):
    return v.astype(jnp.bfloat16)


def dot(a, b):
    return jnp.dot(a, b, preferred_element_type=jnp.float32)


def layer_kernel(
    n_dev,
    x_hbm, g1_hbm, s1_hbm, wqkv, bqkv_hbm, wo, bo_hbm, g2_hbm, s2_hbm, wu, bu_hbm, wd, bd_hbm,
    out_ref,
    x_ref, g1_ref, s1_ref, g2_ref, s2_ref, bqkv_ref, bo_ref, bu_ref, bd_ref,
    xb, h_all, u_w, pool, acc, qkv, ctx, act, psend, precv,
    hop_s, hop_r, fin_s, fin_r, x1,
    xsem, psem, usem, osem, dsem, ag_send, ag_l, ag_r, ag_l2, ag_r2, ag_p,
    rs_send, rs_p, rs_hl, rs_hr, rs_fl, rs_fr,
):
    small = [pltpu.make_async_copy(a, b, xsem.at[i]) for i, (a, b) in enumerate(
        ((x_hbm, x_ref), (g1_hbm, g1_ref), (s1_hbm, s1_ref)))]
    late = [pltpu.make_async_copy(a, b, psem.at[i]) for i, (a, b) in enumerate(
        ((bqkv_hbm, bqkv_ref), (bo_hbm, bo_ref), (g2_hbm, g2_ref), (s2_hbm, s2_ref), (bu_hbm, bu_ref), (bd_hbm, bd_ref)))]
    for copy in small + late:
        copy.start()
    n_chips = n_dev // 2
    rows, dim = x_ref.shape
    nch = dim // CH
    ng = nch // 2
    hr = rows // 2
    side = hr * n_chips
    st_rows = 2 * side
    n_tok = 2 * st_rows
    hc = CH // 2
    n_slab = wqkv.shape[0]
    hd = wqkv.shape[2]
    heads = n_slab // 3
    qw = n_slab * hd
    ff = wu.shape[1]
    nt = ff // CH
    me = lax.axis_index("tp")
    chip, core = me // 2, me % 2
    right = {"tp": ((chip + 1) % n_chips) * 2 + core}
    left = {"tp": ((chip + n_chips - 1) % n_chips) * 2 + core}
    mate = {"tp": chip * 2 + (1 - core)}
    far = {"tp": ((chip + 2) % n_chips) * 2 + core}

    def push(src, dst, ssem, rsem, dev):
        return pltpu.make_async_remote_copy(
            src_ref=src, dst_ref=dst, send_sem=ssem, recv_sem=rsem, device_id=dev, device_id_type=MESH)

    barrier = pltpu.get_barrier_semaphore()
    for dev in (left, right, mate, far):
        pl.semaphore_signal(barrier, inc=1, device_id=dev, device_id_type=MESH)

    def load_qkv(j):
        for s in range(n_slab):
            pltpu.make_async_copy(
                wqkv.at[s, pl.ds(pl.multiple_of(j * CH, CH), CH), :],
                u_w.at[j, :, pl.ds(s * hd, hd)], usem.at[j]).start()

    def load_up(j):
        return pltpu.make_async_copy(
            wu.at[pl.ds(pl.multiple_of(j * CH, CH), CH), :], u_w.at[j], usem.at[j])

    kt = heads * hd
    nk = ff // kt
    o_base = (N_WD - 1) * nk

    def load_down(q):
        g, slot = q % ng, q % N_WD
        for k in range(nk):
            pltpu.make_async_copy(
                wd.at[pl.ds(k * kt, kt), pl.ds(pl.multiple_of(g * 2 * CH, 2 * CH), 2 * CH)],
                pool.at[slot * nk + k], dsem.at[slot]).start()

    def wait_down(q):
        slot = q % N_WD
        pltpu.make_async_copy(pool.at[pl.ds(slot * nk, nk)], pool.at[pl.ds(slot * nk, nk)], dsem.at[slot]).wait()

    def init_loads(j, c):
        load_qkv(j)
        return c

    lax.fori_loop(0, nch, init_loads, 0)
    for g in range(ng):
        pltpu.make_async_copy(wo.at[:, pl.ds(g * 2 * CH, 2 * CH)], pool.at[o_base + g], osem).start()
    for q in range(N_WD - 1):
        load_down(q)

    def norm(get, put, n, gain_ref, shift_ref):
        tot = jnp.zeros((n, CH), jnp.float32)
        for j in range(nch):
            tot += get(j)
        mean = jnp.sum(tot, axis=1, keepdims=True) * (1.0 / dim)
        tot = jnp.zeros((n, CH), jnp.float32)
        for j in range(nch):
            cen = get(j) - mean
            tot += cen * cen
        var = jnp.sum(tot, axis=1, keepdims=True) * (1.0 / dim)
        inv = lax.rsqrt(var + LN_EPS)
        for j in range(nch):
            cols = slice(j * CH, (j + 1) * CH)
            put(j, bf16((get(j) - mean) * inv * gain_ref[:, cols] + shift_ref[:, cols]))

    def put_both(j, y):
        h_all[j, 0, 0:hr, :] = y[0:hr]
        h_all[j, 1, 0:hr, :] = y[hr:]

    def put_stream(st):
        def put(j, y):
            h_all[j, st, 0:hr, :] = y
        return put

    for copy in small:
        copy.wait()
    norm(lambda j: f32(x_ref[:, j * CH:(j + 1) * CH]), put_both, rows, g1_ref, s1_ref)
    acc[...] = jnp.zeros_like(acc)
    pl.semaphore_wait(barrier, 4)

    def piece_both(v, s, r, lo=0, n=CH):
        return h_all.at[v, :, pl.ds(s * side + r * hr, hr), pl.ds(lo, n)]

    def all_both(v, s):
        return h_all.at[v, :, pl.ds(s * side, side), :]

    def piece_stream(v, s, r, lo=0, n=CH):
        return h_all.at[pl.ds((v % ng) * 2, 2), v // ng, pl.ds(s * side + r * hr, hr), pl.ds(lo, n)]

    def all_stream(v, s):
        return h_all.at[pl.ds((v % ng) * 2, 2), v // ng, pl.ds(s * side, side), :]

    def send_own(at, v):
        push(at(v, 0, 0), at(v, 0, 3), ag_send, ag_l.at[v], right).start()
        push(at(v, 0, 0), at(v, 0, 1), ag_send, ag_r.at[v], left).start()
        push(at(v, 0, 0), at(v, 1, 0), ag_send, ag_p.at[v], mate).start()

    def wait_mate(whole, v):
        push(whole(v, 0), whole(v, 1), ag_send, ag_p.at[v], mate).wait_recv()

    def forward_one(at, i):
        with jax.named_scope("gw1l"):
            push(at(i, 0, 0), at(i, 0, 3), ag_send, ag_l.at[i], right).wait_recv()
        push(at(i, 0, 3, 0, hc), at(i, 0, 2, 0, hc), ag_send, ag_l2.at[i], right).start()
        with jax.named_scope("gw1r"):
            push(at(i, 0, 0), at(i, 0, 1), ag_send, ag_r.at[i], left).wait_recv()
        push(at(i, 0, 1, hc, hc), at(i, 0, 2, hc, hc), ag_send, ag_r2.at[i], left).start()
        push(at(i, 0, 3), at(i, 1, 3), ag_send, ag_p.at[i], mate).start()
        push(at(i, 0, 1), at(i, 1, 1), ag_send, ag_p.at[i], mate).start()

    def forward_two(at, j):
        with jax.named_scope("gw2"):
            push(at(j, 0, 3, 0, hc), at(j, 0, 2, 0, hc), ag_send, ag_l2.at[j], right).wait_recv()
            push(at(j, 0, 1, hc, hc), at(j, 0, 2, hc, hc), ag_send, ag_r2.at[j], left).wait_recv()
        push(at(j, 0, 2), at(j, 1, 2), ag_send, ag_p.at[j], mate).start()

    def gather(at, whole, n_use, consume, lags):
        look, lag_b, lag_c = lags

        def step(i, c):
            @pl.when(i < nch)
            def _():
                forward_one(at, i)

            @pl.when(i + look < nch)
            def _():
                send_own(at, i + look)

            @pl.when((i >= lag_b) & (i < nch + lag_b))
            def _():
                forward_two(at, i - lag_b)

            @pl.when(i >= lag_c)
            def _():
                j = i - lag_c
                with jax.named_scope("gwp"):
                    wait_mate(whole, j)
                with jax.named_scope("guse"):
                    consume(j)
            return c

        lax.fori_loop(0, n_use + lag_c, step, 0)

    def gather_drain():
        sent = h_all.at[:, :, pl.ds(0, 7 * hr), :]
        push(sent, sent, ag_send, ag_p.at[0], mate).wait_send()

    tiles = [(t, min(CH, qw - t * CH)) for t in range((qw + CH - 1) // CH)]

    def use_qkv(j):
        part = u_w.at[j, :, pl.ds(0, qw)]
        pltpu.make_async_copy(part, part, usem.at[j]).wait()
        h = h_all[j].reshape(n_tok, CH)

        @pl.when(j < nch - 1)
        def _():
            for t, n in tiles:
                p = dot(h, u_w[j, :, t * CH:t * CH + n])
                acc[2 * t, :, 0:n] += p[0:st_rows]
                acc[2 * t + 1, :, 0:n] += p[st_rows:]

        @pl.when(j == nch - 1)
        def _():
            for t, n in tiles:
                p = dot(h, u_w[j, :, t * CH:t * CH + n])
                slabs = range(t * CH // hd, (t * CH + n) // hd)
                b = jnp.concatenate([bqkv_ref[s % heads, s // heads:s // heads + 1, :] for s in slabs], axis=1)
                for st in range(2):
                    y = acc[2 * t + st, :, 0:n] + p[st * st_rows:(st + 1) * st_rows]
                    qkv[st * st_rows:(st + 1) * st_rows, t * CH:t * CH + n] = bf16(y + f32(b))
        load_up(j).start()

    for copy in late:
        copy.wait()
    for v in range(GATHER_QKV[0]):
        send_own(piece_both, v)
    with jax.named_scope("gather1"):
        gather(piece_both, all_both, nch, use_qkv, GATHER_QKV)
    def position(i):
        st, s, r, w = i // st_rows, (i // side) % 2, (i // hr) % n_chips, i % hr
        return ((chip + r) % n_chips) * (2 * rows) + (core + s - 2 * core * s) * rows + st * hr + w

    qpos = position(lax.broadcasted_iota(jnp.int32, (n_tok, n_tok), 0))
    kpos = position(lax.broadcasted_iota(jnp.int32, (n_tok, n_tok), 1))
    keep = qpos >= kpos
    for h in range(heads):
        q = qkv[:, h * hd:(h + 1) * hd]
        k = qkv[:, (heads + h) * hd:(heads + h + 1) * hd]
        v = qkv[:, (2 * heads + h) * hd:(2 * heads + h + 1) * hd]
        logits = lax.dot_general(q, k, (((1,), (1,)), ((), ())), preferred_element_type=jnp.float32) * hd ** -0.5
        logits = jnp.where(keep, logits, -1e30)
        e = jnp.exp(logits - jnp.max(logits, axis=1, keepdims=True))
        p = bf16(e / jnp.sum(e, axis=1, keepdims=True))
        ctx[:, h * hd:(h + 1) * hd] = bf16(dot(p, v))

    gather_drain()
    o_all = pool.at[pl.ds(o_base, ng)]
    pltpu.make_async_copy(o_all, o_all, osem).wait()

    def pair_sum(v, st, g):
        for c in range(2):
            j = 2 * g + c
            s = acc[v, c * side:(c + 1) * side, :] + f32(precv[st, j])
            two = bf16(s[2 * hr:3 * hr])
            hop_s[0, st, j] = two[:, 0:hc]
            hop_s[1, st, j] = two[:, hc:]
            acc[v, c * side:(c + 1) * side, :] = s

    def middle_sum(v, st, g):
        for c in range(2):
            j = 2 * g + c
            one = acc[v, c * side + hr:c * side + 2 * hr, :]
            fin_s[0, st, j, :, 0:hc] = bf16(one[:, 0:hc] + f32(hop_r[0, st, j]))
            fin_s[0, st, j, :, hc:] = bf16(one[:, hc:])
            three = acc[v, c * side + 3 * hr:(c + 1) * side, :]
            fin_s[1, st, j, :, 0:hc] = bf16(three[:, 0:hc])
            fin_s[1, st, j, :, hc:] = bf16(three[:, hc:] + f32(hop_r[1, st, j]))

    def fins(st, g, v):
        pair = pl.ds(2 * g, 2)
        return (push(fin_s.at[0, st, pair], fin_r.at[0, st, pair], rs_send, rs_fl.at[v], right),
                push(fin_s.at[1, st, pair], fin_r.at[1, st, pair], rs_send, rs_fr.at[v], left))

    def last_sum(v, st, g, put):
        for copy in fins(st, g, v):
            copy.wait_recv()
        for c in range(2):
            j = 2 * g + c
            total = acc[v, c * side:c * side + hr, :] + f32(fin_r[0, st, j]) + f32(fin_r[1, st, j])
            put(st, j, bf16(xb[st, j] + total))

    def scatter_drain():
        push(psend, precv, rs_send, rs_p.at[0], mate).wait_send()
        push(hop_s, hop_r, rs_send, rs_p.at[0], mate).wait_send()
        push(fin_s, fin_r, rs_send, rs_p.at[0], mate).wait_send()

    bo = f32(bo_ref[...]).reshape(1, dim)
    for j in range(nch):
        cols = slice(j * CH, (j + 1) * CH)
        y = f32(x_ref[:, cols]) + bo[:, cols]
        xb[0, j] = y[0:hr]
        xb[1, j] = y[hr:]

    def pairs_out(g):
        two = pl.ds(2 * g, 2)
        return push(psend.at[:, two], precv.at[:, two], rs_send, rs_p.at[g], mate)

    def hops_out(g):
        two = pl.ds(2 * g, 2)
        return (push(hop_s.at[0, :, two], hop_r.at[0, :, two], rs_send, rs_hl.at[g], right),
                push(hop_s.at[1, :, two], hop_r.at[1, :, two], rs_send, rs_hr.at[g], left))

    def put_x1(st, j, y):
        x1[st, j] = y

    lag_p, lag_h, lag_f = LAGS_OUT

    def out_step(i, carry):
        @pl.when(i < ng)
        def _():
            with jax.named_scope("spart"):
                for c in range(2):
                    j = 2 * i + c
                    p = dot(ctx[...], pool[o_base + i, :, c * CH:(c + 1) * CH])
                    for st in range(2):
                        acc[st * ng + i, c * side:(c + 1) * side, :] = p[st * st_rows:st * st_rows + side]
                        psend[st, j] = bf16(p[st * st_rows + side:(st + 1) * st_rows])
            pairs_out(i).start()

        @pl.when((i >= lag_p) & (i < ng + lag_p))
        def _():
            g = i - lag_p
            with jax.named_scope("swp"):
                pairs_out(g).wait_recv()
            for st in range(2):
                pair_sum(st * ng + g, st, g)
            for copy in hops_out(g):
                copy.start()

        @pl.when((i >= lag_h) & (i < ng + lag_h))
        def _():
            g = i - lag_h
            with jax.named_scope("swh"):
                for copy in hops_out(g):
                    copy.wait_recv()
            for st in range(2):
                middle_sum(st * ng + g, st, g)
            for copy in fins(0, g, g):
                copy.start()

        @pl.when(i == ng + lag_h - 1)
        def _():
            for g in range(ng):
                for copy in fins(1, g, ng + g):
                    copy.start()

        @pl.when(i >= lag_f)
        def _():
            g = i - lag_f
            with jax.named_scope("swf"):
                last_sum(g, 0, g, put_x1)
        return carry

    with jax.named_scope("scatter1"):
        lax.fori_loop(0, ng + lag_f, out_step, 0)

    load_down(N_WD - 1)

    with jax.named_scope("ln2a"):
        norm(lambda j: f32(x1[0, j]), put_stream(0), hr, g2_ref, s2_ref)
    for v in range(GATHER_UP[0]):
        send_own(piece_stream, v)

    def last_out(g, carry):
        last_sum(ng + g, 1, g, put_x1)
        return carry

    with jax.named_scope("last1"):
        lax.fori_loop(0, ng, last_out, 0)
    with jax.named_scope("ln2b"):
        norm(lambda j: f32(x1[1, j]), put_stream(1), hr, g2_ref, s2_ref)
    acc[ng:2 * ng] = jnp.zeros((ng, st_rows, CH), jnp.float32)
    bd = f32(bd_ref[...]).reshape(1, dim)
    for j in range(nch):
        for st in range(2):
            xb[st, j] = f32(x1[st, j]) + bd[:, j * CH:(j + 1) * CH]
    for j in range(nch):
        load_up(j).wait()

    bu = f32(bu_ref[...]).reshape(1, ff)

    def activate(st, t, a):
        cols = slice(t * CH, (t + 1) * CH)
        act[st, :, cols] = bf16(jax.nn.gelu(a + bu[:, cols], approximate=True))

    def use_up(g):
        h = jnp.concatenate([h_all[2 * g, 0], h_all[2 * g + 1, 0]], axis=1)

        def weight(t):
            return u_w[pl.ds(2 * g, 2), :, t * CH:(t + 1) * CH].reshape(2 * CH, CH)

        @pl.when(g < ng - 1)
        def _():
            for t in range(nt):
                acc[ng + t] += dot(h, weight(t))

        @pl.when(g == ng - 1)
        def _():
            for t in range(nt):
                activate(0, t, acc[ng + t] + dot(h, weight(t)))

    def up_whole():
        for g in range(ng):
            wait_mate(all_stream, ng + g)
        with jax.named_scope("muse"):
            h = jnp.concatenate([h_all[j, 1] for j in range(nch)], axis=1)
            for t in range(nt):
                activate(1, t, dot(h, u_w[:, :, t * CH:(t + 1) * CH].reshape(dim, CH)))

    with jax.named_scope("gather2"):
        gather(piece_stream, all_stream, ng, use_up, GATHER_UP)
    scatter_drain()

    def put_out(st, j, y):
        out_ref[pl.ds(pl.multiple_of(st * hr, hr), hr), pl.ds(pl.multiple_of(j * CH, CH), CH)] = y

    def pairs_down(v, st, g):
        two = pl.ds(2 * g, 2)
        return push(psend.at[st, two], precv.at[st, two], rs_send, rs_p.at[v], mate)

    def hops_down(v, st, g):
        two = pl.ds(2 * g, 2)
        return (push(hop_s.at[0, st, two], hop_r.at[0, st, two], rs_send, rs_hl.at[v], right),
                push(hop_s.at[1, st, two], hop_r.at[1, st, two], rs_send, rs_hr.at[v], left))

    def far_down(v, st, g):
        two = pl.ds(2 * g, 2)
        return push(hop_s.at[:, st, two], hop_r.at[:, st, two], rs_send, rs_hl.at[v], far)

    first_far = 2 * ng - N_FAR

    def when_group(k, fn):
        @pl.when((k >= 0) & (k <= 2 * ng) & (k != ng))
        def _():
            st = k // (ng + 1)
            v = k - st
            fn(v, st, v - st * ng)

    lag_p2, lag_h2, lag_f2 = LAGS_DOWN
    done_two = ng + GATHER_UP[2] - GATHER_UP[1]

    def down_part(v, st, g):
        wait_down(v)
        slot = v % N_WD
        with jax.named_scope("dpart"):
            for c in range(2):
                j = 2 * g + c
                p = dot(act[st], pool[pl.ds(slot * nk, nk), :, c * CH:(c + 1) * CH].reshape(ff, CH))
                acc[v, c * side:(c + 1) * side, :] = p[0:side]
                psend[st, j] = bf16(p[side:])

        @pl.when(v + N_WD < 2 * ng)
        def _():
            load_down(v + N_WD)
        pairs_down(v, st, g).start()

    def down_pair(v, st, g):
        with jax.named_scope("dwp"):
            pairs_down(v, st, g).wait_recv()
        pair_sum(v, st, g)

        @pl.when(v < first_far)
        def _():
            for copy in hops_down(v, st, g):
                copy.start()

        @pl.when(v >= first_far)
        def _():
            far_down(v, st, g).start()
            for c in range(2):
                j = 2 * g + c
                fin_s[0, st, j] = bf16(acc[v, c * side + hr:c * side + 2 * hr, :])
                fin_s[1, st, j] = bf16(acc[v, c * side + 3 * hr:(c + 1) * side, :])
            for copy in fins(st, g, v):
                copy.start()

    def down_middle(v, st, g):
        @pl.when(v < first_far)
        def _():
            with jax.named_scope("dwh"):
                for copy in hops_down(v, st, g):
                    copy.wait_recv()
            middle_sum(v, st, g)
            for copy in fins(st, g, v):
                copy.start()

    def down_last(v, st, g):
        @pl.when(v < first_far)
        def _():
            with jax.named_scope("dwf"):
                last_sum(v, st, g, put_out)

        @pl.when(v >= first_far)
        def _():
            with jax.named_scope("dwx"):
                far_down(v, st, g).wait_recv()
                for c in range(2):
                    j = 2 * g + c
                    acc[v, c * side:c * side + hr, 0:hc] += f32(hop_r[0, st, j])
                    acc[v, c * side:c * side + hr, hc:] += f32(hop_r[1, st, j])
                last_sum(v, st, g, put_out)

    def mlp_step(w, carry):
        tail = w >= ng + 1 + lag_h2

        @pl.when(tail)
        def _():
            when_group(w - lag_h2, down_middle)

        when_group(w - lag_p2, down_pair)

        @pl.when(jnp.logical_not(tail))
        def _():
            when_group(w - lag_h2, down_middle)

        when_group(w - lag_f2, down_last)

        @pl.when(w + done_two < nch)
        def _():
            forward_two(piece_stream, w + done_two)

        pl.when(w == ng)(up_whole)
        when_group(w, down_part)
        return carry

    with jax.named_scope("mlp"):
        lax.fori_loop(0, 2 * ng + 1 + lag_f2, mlp_step, 0)
    scatter_drain()
    gather_drain()


def solution(mesh):
    n_dev = mesh.shape["tp"]

    def body(hidden, g1, s1, w_qkv, b_qkv, w_out, b_out, g2, s2, w_up, b_up, w_down, b_down):
        _, rows, dim = hidden.shape
        _, three, heads, hd = w_qkv.shape
        ff = w_up.shape[1]
        nch = dim // CH
        n_tok, hr = rows * n_dev, rows // 2
        st_rows, side = n_tok // 2, n_tok // 4
        bf, fl = jnp.bfloat16, jnp.float32
        row = lambda v: v.reshape(1, -1)
        hbm = pl.BlockSpec(memory_space=pl.ANY)
        dma = pltpu.SemaphoreType.DMA
        out = pl.pallas_call(
            functools.partial(layer_kernel, n_dev),
            out_shape=pltpu.VMEM((rows, dim), bf),
            in_specs=[hbm] * 13,
            out_specs=pl.BlockSpec(memory_space=pltpu.VMEM),
            scratch_shapes=[
                pltpu.VMEM((rows, dim), bf),
                pltpu.VMEM((1, dim), fl), pltpu.VMEM((1, dim), fl),
                pltpu.VMEM((1, dim), fl), pltpu.VMEM((1, dim), fl),
                pltpu.VMEM((heads, three, hd), bf), pltpu.VMEM((dim,), bf),
                pltpu.VMEM((ff,), bf), pltpu.VMEM((dim,), bf),
                pltpu.VMEM((2, nch, hr, CH), fl),
                pltpu.VMEM((nch, 2, st_rows, CH), bf),
                pltpu.VMEM((nch, CH, ff), bf),
                pltpu.VMEM(((N_WD - 1) * (ff // (heads * hd)) + nch // 2, heads * hd, 2 * CH), bf),
                pltpu.VMEM((nch, st_rows, CH), fl),
                pltpu.VMEM((n_tok, three * heads * hd), bf),
                pltpu.VMEM((n_tok, heads * hd), bf),
                pltpu.VMEM((2, st_rows, ff), bf),
                pltpu.VMEM((2, nch, side, CH), bf),
                pltpu.VMEM((2, nch, side, CH), bf),
                pltpu.VMEM((2, 2, nch, hr, CH // 2), bf),
                pltpu.VMEM((2, 2, nch, hr, CH // 2), bf),
                pltpu.VMEM((2, 2, nch, hr, CH), bf),
                pltpu.VMEM((2, 2, nch, hr, CH), bf),
                pltpu.VMEM((2, nch, hr, CH), bf),
                dma((3,)), dma((6,)), dma((nch,)), dma(()), dma((N_WD,)),
                dma(()), dma((nch,)), dma((nch,)), dma((nch,)), dma((nch,)), dma((nch,)),
                dma(()), dma((nch,)), dma((nch,)), dma((nch,)), dma((nch,)), dma((nch,)),
            ],
            compiler_params=pltpu.CompilerParams(
                collective_id=0, has_side_effects=True, vmem_limit_bytes=61 * 1024 * 1024),
            name="decoder_layer",
        )(
            hidden[0], row(g1), row(s1),
            jnp.transpose(w_qkv, (1, 2, 0, 3)).reshape(three * heads, dim, hd),
            jnp.transpose(b_qkv, (1, 0, 2)),
            w_out.reshape(heads * hd, dim), b_out, row(g2), row(s2), w_up, b_up, w_down, b_down,
        )
        return out[None]

    specs = (P("dp", "tp", None), P(), P(), P(None, None, "tp", None), P(None, "tp", None),
             P("tp", None, None), P(), P(), P(), P(None, "tp"), P("tp"), P("tp", None), P())
    return jax.shard_map(body, mesh=mesh, in_specs=specs, out_specs=P("dp", "tp", None), check_vma=False)
```
